128 devices in a mesh: gz: 16 (over z, x_lo, core), pair: 8 (over x_hi, y).
Axes of the slice: x: 4 (x_hi: 2, x_lo: 2; x = x_hi * 2 + x_lo), y: 4, z: 4, core: 2. Of those that a mesh axis runs over, the one named last changes fastest.
Arguments:
- orbitals: bfloat16 [8, 128, 256, 256], P(None, 'gz'), may hold values from -6 to 6
- pair_index: int32 [8, 2], P('pair'), may hold values from 0 to 7
- pair_weight: float32 [8], P('pair'), may hold values from 0.5 to 2
Outputs:
- potential: float32 [8, 128, 256, 256], P('pair', 'gz')
- residual_norm: float32 [8], P('pair')
- energy: float32 [1], replicated
The draws below stay inside these ranges and needn't reach their ends.
Inputs may be any that keep to these rules, and one draw needn't show every extreme that they name: `pair_index`: A pair may name one orbital twice.
All inputs are finite; a program needn't handle non-finite values.
Results may differ from the reference program's by a relative error of at most 0.0003.
Values sent between devices are 32-bit elements; how exact they have to be, the bound alone decides.
A program may use at most 320 MiB of HBM per device.

```python
import math
import jax
import jax.numpy as jnp
from jax import lax

NX = 256
NY = 256
NORB = 8
LEVELS = 4
NU = 2
COARSE = 8
CYCLES = 1
NZ = 128
PAIRS = 8


def plant(entries, rng, least, largest):
    shape = entries.shape
    place = [jax.random.randint(jax.random.fold_in(rng, axis), (), 0, shape[axis]) for axis in range(len(shape))]
    entries = entries.at[tuple(place)].set(least)
    longest = shape.index(max(shape))
    place[longest] = (place[longest] + 1) % shape[longest]
    return entries.at[tuple(place)].set(largest)


def levels(rng, shape, split, least, high):
    def one(axis_at, blocks):
        steps = jax.random.uniform(jax.random.fold_in(jax.random.fold_in(rng, 6), axis_at), (blocks,), jnp.float32, least / len(split), high / len(split))
        return jnp.repeat(jnp.exp(steps), shape[axis_at] // blocks).reshape((-1,) + (1,) * (len(shape) - axis_at - 1))

    level = one(*split[0])
    for cut in split[1:]:
        level = level * one(*cut)
    return level


def noise(key, shape, scale, most, split=(), dtype=jnp.bfloat16):
    gain = levels(key, shape, split, -0.22, 0.18) if split else 1.0
    entries = jax.random.normal(key, shape, jnp.float32) * scale * gain
    return jnp.minimum(jnp.maximum(entries, -most), most).astype(dtype)


def setup_inputs(seed: int = 0) -> dict:
    seeds = jax.random.split(jax.random.key(seed), 4)
    orbitals = noise(seeds[0], (NORB, NZ, NY, NX), 1.0, 6.0, ((1, 16),))
    pair_index = plant(jax.random.randint(seeds[1], (PAIRS, 2), 0, NORB), jax.random.fold_in(seeds[1], 1), 0, NORB - 1).astype(jnp.int32)
    pair_weight = jnp.clip(jnp.exp(math.log(2.0) - 1.3862944 * jax.random.uniform(seeds[2], (PAIRS,), jnp.float32) ** levels(seeds[2], (PAIRS,), ((0, 8),), -0.2, 0.2)), 0.5, 2.0)
    return {"orbitals": orbitals, "pair_index": pair_index, "pair_weight": pair_weight}


relax = 2.0 / 3.0

def laplace(field, level):
    padded = jnp.pad(field, 1)
    beside = padded[2:, 1:-1, 1:-1] + padded[:-2, 1:-1, 1:-1]
    beside = beside + padded[1:-1, 2:, 1:-1] + padded[1:-1, :-2, 1:-1]
    beside = beside + padded[1:-1, 1:-1, 2:] + padded[1:-1, 1:-1, :-2]
    return (6.0 * field - beside) * 0.25 ** level

def sweep(field, source, level):
    return field + (source - laplace(field, level)) * (relax * 4.0 ** level / 6.0)

def restrict(field):
    zsize, ysize, xsize = field.shape
    return field.reshape(zsize // 2, 2, ysize // 2, 2, xsize // 2, 2).mean(axis=(1, 3, 5))

def prolong(field):
    return jnp.repeat(jnp.repeat(jnp.repeat(field, 2, axis=0), 2, axis=1), 2, axis=2)

def vcycle(field, source, level):
    if level == LEVELS - 1:
        for _ in range(COARSE):
            field = sweep(field, source, level)
        return field
    for _ in range(NU):
        field = sweep(field, source, level)
    remain = source - laplace(field, level)
    coarse_source = restrict(remain)
    correction = vcycle(jnp.zeros_like(coarse_source), coarse_source, level + 1)
    field = field + prolong(correction)
    for _ in range(NU):
        field = sweep(field, source, level)
    return field

def reference(orbitals, pair_index, pair_weight):

    def solve_pair(pair_row):
        left_orbital = orbitals[pair_row[0]].astype(jnp.float32)
        right_orbital = orbitals[pair_row[1]].astype(jnp.float32)
        density = left_orbital * right_orbital
        field = jnp.zeros_like(density)
        for _ in range(CYCLES):
            field = vcycle(field, density, 0)
        final = density - laplace(field, 0)
        return (field, jnp.sum(final * final), jnp.sum(density * field))
    potential, squares, products = lax.map(solve_pair, pair_index)
    cell_count = NZ * NY * NX
    residual_norm = jnp.sqrt(squares / cell_count)
    energy = (-0.5 * jnp.sum(pair_weight * products) / cell_count).reshape(1)
    return (potential, residual_norm, energy)
```

```python
import functools

import jax
import jax.numpy as jnp
from jax import lax
from jax.experimental import pallas as pl
from jax.experimental.pallas import tpu as pltpu
from jax.sharding import PartitionSpec as P

MESH = pl.DeviceIdType.MESH
F32, BF16 = jnp.float32, jnp.bfloat16
PAD = 8
CH = 32
NINTH = 1.0 / 9.0
N81 = 1.0 / 81.0


def lane_iota(shape):
    return lax.broadcasted_iota(jnp.int32, shape, len(shape) - 1)


def roll(x, shift):
    return pltpu.roll(x, shift % x.shape[-1], x.ndim - 1)


def from_left(x, width=128):
    return jnp.where(lane_iota(x.shape) % width == 0, 0.0, roll(x, 1))


def from_right(x, width=128):
    return jnp.where(lane_iota(x.shape) % width == width - 1, 0.0, roll(x, -1))


def split_dot(x, m):
    hi = x.astype(BF16)
    rest = x - hi.astype(F32)
    mid = rest.astype(BF16)
    low = (rest - mid.astype(F32)).astype(BF16)
    dot = functools.partial(jnp.dot, preferred_element_type=F32)
    return dot(hi, m) + dot(mid, m) + dot(low, m)


def selection(shape, test):
    a = lax.broadcasted_iota(jnp.int32, shape, 0)
    b = lax.broadcasted_iota(jnp.int32, shape, 1)
    return jnp.where(test(a, b), 1.0, 0.0).astype(BF16)


def fold(x):
    return x.reshape(x.shape[0] // 8, 8, x.shape[1]).sum(axis=0)


def rows(ref, z, ph, r, n, dr=0):
    return ref[z, ph, pl.ds(PAD + r + dr, n), :]


def nbxy0(ref, z, r, n, c):
    out = []
    for yp in range(2):
        for xp in range(2):
            side = c[2 * yp + 1 - xp]
            x = side + (from_right(side) if xp else from_left(side))
            other = 2 * (1 - yp) + xp
            y = c[other] + rows(ref, z, other, r, n, 1 if yp else -1)
            out.append(x + y)
    return out


def phase_sums(ref, z, r, n, c):
    total = (c[0] + c[1]) + (c[2] + c[3])
    shifts = from_left(c[1] + c[3]) + from_right(c[0] + c[2])
    shifts = shifts + (rows(ref, z, 2, r, n, -1) + rows(ref, z, 3, r, n, -1))
    shifts = shifts + (rows(ref, z, 0, r, n, 1) + rows(ref, z, 1, r, n, 1))
    return total, shifts


def center(ref, z, r, n):
    return [rows(ref, z, ph, r, n) for ph in range(4)]


def crow(ref, z, r, n, dr=0):
    return ref[z, pl.ds(PAD + r + dr, n), :]


def nbxy(ref, z, r, n, c, width):
    y = crow(ref, z, r, n, -1) + crow(ref, z, r, n, 1)
    return y + (from_left(c, width) + from_right(c, width))


def kernel(
    gz, pairs,
    pidx, pweight, orbitals, pot, res_out, en_out,
    orb0, orb1, orb2, orb3, orb4, orb5, orb6, orb7, px, tmp, f, a, b, g0, g0o, s1, a1, b1, t1, g1, g1o, pe1,
    s2, a2, b2, t2, pe2, t3, s3, a3, b3, sums, ens, obuf,
    orb_sem, fs, fr, g0s, g0r, h1s, h1r, g1s, g1r, h2s, h2r, t3s, t3r, ss, sr, es, er, out_sem,
):
    d = lax.axis_index("gz")
    me = lax.axis_index("pair")
    has_lo, has_hi = d > 0, d < gz - 1
    flo, fhi = has_lo.astype(F32), has_hi.astype(F32)

    def remote(src, dst, s_sem, r_sem, **to):
        return pltpu.make_async_remote_copy(
            src_ref=src, dst_ref=dst, send_sem=s_sem, recv_sem=r_sem, device_id=to, device_id_type=MESH
        )

    orb = (orb0, orb1, orb2, orb3, orb4, orb5, orb6, orb7)

    def orb_copy(z):
        return pltpu.make_async_copy(orbitals.at[:, z], orb[z], orb_sem.at[z])

    for z in (0, 7, 1, 6, 2, 5, 3, 4):
        orb_copy(z).start()
    barrier = pltpu.get_barrier_semaphore()

    @pl.loop(1, gz)
    def _(o):
        pl.semaphore_signal(barrier, inc=1, device_id={"gz": lax.rem(d + o, gz)}, device_id_type=MESH)

    @pl.loop(1, pairs)
    def _(o):
        pl.semaphore_signal(barrier, inc=1, device_id={"pair": lax.rem(me + o, pairs)}, device_id_type=MESH)

    px[...] = selection((256, 256), lambda i, j: j == (i & 1) * 128 + (i >> 1))
    pad0 = jnp.zeros((4, PAD, 128), F32)

    @pl.loop(0, 16)
    def _(z):
        for ref in (f, a, b):
            ref[z, :, pl.ds(0, PAD), :] = pad0
            ref[z, :, pl.ds(PAD + 128, PAD), :] = pad0

    def clear_outside(first):
        @pl.loop(first, first + 4)
        def _(z):
            for ref in (f, a, b):
                for ph in range(4):
                    ref[z, ph, pl.ds(PAD, 128), :] = jnp.zeros((128, 128), F32)

        @pl.when(first == 0)
        def _():
            @pl.loop(0, 5)
            def _(z):
                s1[z, pl.ds(PAD, 128), :] = jnp.zeros((128, 128), F32)

        @pl.when(first > 0)
        def _():
            @pl.loop(9, 14)
            def _(z):
                s1[z, pl.ds(PAD, 128), :] = jnp.zeros((128, 128), F32)

    @pl.when(d == 0)
    def _():
        clear_outside(0)
        g0[0] = jnp.zeros((128, 128), F32)
        g1[0] = jnp.zeros((64, 128), F32)

    @pl.when(d == gz - 1)
    def _():
        clear_outside(12)
        g0[1] = jnp.zeros((128, 128), F32)
        g1[1] = jnp.zeros((64, 128), F32)

    @pl.when(d == 1)
    def _():
        s1[0, pl.ds(PAD, 128), :] = jnp.zeros((128, 128), F32)

    @pl.when(d == gz - 2)
    def _():
        s1[13, pl.ds(PAD, 128), :] = jnp.zeros((128, 128), F32)

    @pl.loop(0, 14)
    def _(z):
        s1[z, pl.ds(0, PAD), :] = jnp.zeros((PAD, 128), F32)
        s1[z, pl.ds(PAD + 128, PAD), :] = jnp.zeros((PAD, 128), F32)
        a1[z] = jnp.zeros((144, 128), F32)
        b1[z] = jnp.zeros((144, 128), F32)

    @pl.loop(0, 7)
    def _(p):
        s2[p, pl.ds(0, PAD), :] = jnp.zeros((PAD, 128), F32)
        s2[p, pl.ds(PAD + 64, PAD), :] = jnp.zeros((PAD, 128), F32)
        a2[p] = jnp.zeros((80, 128), F32)
        b2[p] = jnp.zeros((80, 128), F32)
        at = d + p - 3

        @pl.when(jnp.logical_or(at < 0, at >= gz))
        def _():
            s2[p, pl.ds(PAD, 64), :] = jnp.zeros((64, 128), F32)

    for q in range(4):
        a3[q] = jnp.zeros((48, 128), F32)
        b3[q] = jnp.zeros((48, 128), F32)

    i0, i1 = pidx[0, 0], pidx[0, 1]

    for i, z in enumerate((0, 7, 1, 6, 2, 5, 3, 4)):
        orb_copy(z).wait()
        slot = i % 2
        left = jnp.dot(orb[z][i0], px[...], preferred_element_type=F32)
        right = jnp.dot(orb[z][i1], px[...], preferred_element_type=F32)
        both = left * right
        tmp[slot, 0] = both[:, :128]
        tmp[slot, 1] = both[:, 128:]
        for yp in range(2):
            for xp in range(2):
                f[z + 4, 2 * yp + xp, pl.ds(PAD, 128), :] = tmp[slot, xp, pl.ds(yp, 128, stride=2), :]

    def w_plane(z, lo, hi):
        for r in range(0, 128, CH):
            c = center(f, z, r, CH)
            nb = nbxy0(f, z, r, CH, c)
            for ph in range(4):
                t = 12.0 * c[ph] + nb[ph]
                if lo:
                    t = t + rows(f, z - 1, ph, r, CH)
                if hi:
                    t = t + rows(f, z + 1, ph, r, CH)
                a[z, ph, pl.ds(PAD + r, CH), :] = t

    w_plane(4, False, True)
    w_plane(11, True, False)

    pl.semaphore_wait(barrier, gz - 1 + pairs - 1)

    for side, z in ((0, 4), (1, 11)):
        for r in range(0, 128, CH):
            total, shifts = phase_sums(f, z, r, CH, center(f, z, r, CH))
            w = center(a, z, r, CH)
            g0o[side, pl.ds(r, CH), :] = (0.5 * N81) * (
                shifts - 3.0 * total + ((w[0] + w[1]) + (w[2] + w[3]))
            )

    def exchange(out, landed, s_sems, r_sems):
        lo = remote(out.at[0], landed.at[1], s_sems.at[0], r_sems.at[1], gz=jnp.maximum(d - 1, 0))
        hi = remote(out.at[1], landed.at[0], s_sems.at[1], r_sems.at[0], gz=jnp.minimum(d + 1, gz - 1))
        return lo, hi

    g0_lo, g0_hi = exchange(g0o, g0, g0s, g0r)

    @pl.when(has_lo)
    def _():
        g0_lo.start()

    @pl.when(has_hi)
    def _():
        g0_hi.start()

    def f_copy(side, k):
        if side == 0:
            return remote(
                f.at[4 + k, :, pl.ds(PAD, 128), :], f.at[12 + k, :, pl.ds(PAD, 128), :],
                fs.at[0, k], fr.at[1, k], gz=jnp.maximum(d - 1, 0),
            )
        return remote(
            f.at[8 + k, :, pl.ds(PAD, 128), :], f.at[k, :, pl.ds(PAD, 128), :],
            fs.at[1, k], fr.at[0, k], gz=jnp.minimum(d + 1, gz - 1),
        )

    def f_start(*which):
        @pl.when(has_lo)
        def _():
            for k in which:
                f_copy(0, k).start()

        @pl.when(has_hi)
        def _():
            for k in which:
                f_copy(1, 3 - k).start()

    f_start(0)

    @pl.loop(5, 11)
    def _(z):
        w_plane(z, True, True)

    for ph in range(4):
        a[3, ph, pl.ds(PAD, 128), :] = flo * f[4, ph, pl.ds(PAD, 128), :]
        a[12, ph, pl.ds(PAD, 128), :] = fhi * f[11, ph, pl.ds(PAD, 128), :]

    @pl.loop(0, 4)
    def _(j):
        for r in range(0, 128, CH):
            out = None
            for dz in range(2):
                z = 4 + 2 * j + dz
                c = center(a, z, r, CH)
                total, shifts = phase_sums(a, z, r, CH, c)
                below, above, src = center(a, z - 1, r, CH), center(a, z + 1, r, CH), center(f, z, r, CH)
                zs = ((below[0] + below[1]) + (below[2] + below[3])) + (
                    (above[0] + above[1]) + (above[2] + above[3])
                )
                q = ((src[0] + src[1]) + (src[2] + src[3])) + N81 * (zs - 4.0 * total + shifts)
                out = q if out is None else out + q
            s1[5 + j, pl.ds(PAD + r, CH), :] = 0.5 * out

    @pl.when(has_lo)
    def _():
        g0_hi.wait_recv()
        s1[5, pl.ds(PAD, 128), :] += g0[0]

    @pl.when(has_hi)
    def _():
        g0_lo.wait_recv()
        s1[8, pl.ds(PAD, 128), :] += g0[1]

    def w1_plane(z, lo, hi):
        for r in range(0, 128, 64):
            c = crow(s1, z, r, 64)
            t = 12.0 * c + nbxy(s1, z, r, 64, c, 128)
            if lo:
                t = t + crow(s1, z - 1, r, 64)
            if hi:
                t = t + crow(s1, z + 1, r, 64)
            a1[z, pl.ds(PAD + r, 64), :] = t

    for z in range(5, 9):
        w1_plane(z, z > 5, z < 8)
    a1[4, pl.ds(PAD, 128), :] = flo * crow(s1, 5, 0, 128)
    a1[9, pl.ds(PAD, 128), :] = fhi * crow(s1, 8, 0, 128)
    for slot, z in ((0, 5), (3, 8)):
        for r in range(0, 128, 64):
            c = crow(s1, z, r, 64)
            t1[slot, pl.ds(r, 64), :] = (0.5 * N81) * (
                nbxy(s1, z, r, 64, c, 128) - 5.0 * c + crow(a1, z, r, 64)
            )
    for slot in (1, 2):
        for r in range(0, 128, 64):
            out = None
            for z in (3 + 2 * slot, 4 + 2 * slot):
                c = crow(a1, z, r, 64)
                nb = nbxy(a1, z, r, 64, c, 128) + (crow(a1, z - 1, r, 64) + crow(a1, z + 1, r, 64))
                q = crow(s1, z, r, 64) + N81 * (nb - 6.0 * c)
                out = q if out is None else out + q
            t1[slot, pl.ds(r, 64), :] = 0.5 * out

    def ypair(ref, slot, n):
        return ref[slot, pl.ds(0, n, stride=2), :] + ref[slot, pl.ds(1, n, stride=2), :]

    m_first = selection((128, 128), lambda i, j: (i >> 1) == j)
    m_second = selection((128, 128), lambda i, j: (i >> 1) + 64 == j)
    g1o[0] = split_dot(ypair(t1, 0, 64), m_second)
    g1o[1] = split_dot(ypair(t1, 3, 64), m_first)
    g1_lo, g1_hi = exchange(g1o, g1, g1s, g1r)

    @pl.when(has_lo)
    def _():
        g1_lo.start()

    @pl.when(has_hi)
    def _():
        g1_hi.start()

    s2[3, pl.ds(PAD, 64), :] = split_dot(ypair(t1, 1, 64), m_first) + split_dot(ypair(t1, 2, 64), m_second)

    def h1_copy(i):
        here, there, step = ((5, 9, -1), (5, 1, 1), (5, 13, -2), (8, 0, 2))[i]
        n = 4 if abs(step) == 1 else 1
        to = jnp.clip(d + step, 0, gz - 1)
        return remote(
            s1.at[pl.ds(here, n), pl.ds(PAD, 128), :], s1.at[pl.ds(there, n), pl.ds(PAD, 128), :],
            h1s.at[i], h1r.at[i], gz=to,
        )

    h1_sends = [d >= 1, d <= gz - 2, d >= 2, d <= gz - 3]
    h1_recvs = [d <= gz - 2, d >= 1, d <= gz - 3, d >= 2]

    def h1_start():
        for i in range(4):
            @pl.when(h1_sends[i])
            def _():
                h1_copy(i).start()

    h1_start()

    @pl.when(has_lo)
    def _():
        g1_hi.wait_recv()
        s2[3, pl.ds(PAD, 64), :] += g1[0]

    @pl.when(has_hi)
    def _():
        g1_lo.wait_recv()
        s2[3, pl.ds(PAD, 64), :] += g1[1]

    low_half = lane_iota((64, 128)) < 64

    def nb2(ref, p, c):
        z = roll(c + jnp.where(low_half, crow(ref, p + 1, 0, 64), crow(ref, p - 1, 0, 64)), 64)
        return nbxy(ref, p, 0, 64, c, 64) + z

    def h2_copy(i):
        step = (-3, -2, -1, 1, 2, 3)[i]
        to = jnp.clip(d + step, 0, gz - 1)
        return remote(
            s2.at[3, pl.ds(PAD, 64), :], s2.at[3 - step, pl.ds(PAD, 64), :], h2s.at[i], h2r.at[i], gz=to
        )

    def inside(step):
        at = d + step
        return jnp.logical_and(at >= 0, at < gz)

    c = crow(s2, 3, 0, 64)
    turned = roll(c, 64)
    w0 = 12.0 * c + nbxy(s2, 3, 0, 64, c, 64) + turned
    a2[3, pl.ds(PAD, 64), :] = w0
    a2[2, pl.ds(PAD, 64), :] = flo * jnp.where(low_half, 0.0, turned)
    a2[4, pl.ds(PAD, 64), :] = fhi * jnp.where(low_half, turned, 0.0)
    for p in (2, 3, 4):
        w = crow(a2, p, 0, 64)
        r = N81 * (nb2(a2, p, w) - 6.0 * w)
        t2[p - 2] = r + c if p == 3 else r
    tile = None
    for p in range(3):
        block = lax.rem(d + p - 1 + gz, 4) * 32
        m = selection((128, 128), lambda i, j: ((i & 63) >> 1) + block == j)
        part = split_dot(ypair(t2, p, 32), m)
        tile = part if tile is None else tile + part
    t3[d] = 0.5 * tile

    def t3_copy(o):
        to = lax.rem(d + o, gz)
        return remote(t3.at[d], t3.at[d], t3s.at[o], t3r.at[d], gz=to)

    @pl.loop(1, gz)
    def _(o):
        t3_copy(o).start()

    for i, step in enumerate((-3, -2, -1, 1, 2, 3)):
        @pl.when(inside(step))
        def _():
            h2_copy(i).start()

    f_start(1, 2, 3)

    @pl.loop(1, gz)
    def _(o):
        peer = lax.rem(d + o, gz)
        remote(t3.at[peer], t3.at[peer], t3s.at[o], t3r.at[peer], gz=peer).wait_recv()

    lane32 = lane_iota((32, 128))
    for q in range(4):
        total = None
        for e in range(max(4 * q - 1, 0), min(4 * q + 5, gz)):
            x = t3[e]
            if e == 4 * q - 1:
                x = jnp.where(lane32 < 32, x, 0.0)
            elif e == 4 * q + 4:
                x = jnp.where(lane32 >= 96, x, 0.0)
            elif e == 4 * q:
                x = jnp.where(lane32 < 96, x, 0.0)
            elif e == 4 * q + 3:
                x = jnp.where(lane32 >= 32, x, 0.0)
            total = x if total is None else total + x
        s3[q] = total * NINTH
        a3[q, pl.ds(PAD, 32), :] = total * NINTH

    def sweep3(src, dst):
        v = [crow(src, q, 0, 32) for q in range(4)]
        for q in range(4):
            after = v[q + 1] if q < 3 else jnp.zeros_like(v[0])
            before = v[q - 1] if q > 0 else jnp.zeros_like(v[0])
            nz = roll(jnp.where(lane32 < 32, after, v[q]), -32)
            nz = nz + roll(jnp.where(lane32 >= 96, before, v[q]), 32)
            nb = nbxy(src, q, 0, 32, v[q], 32) + nz
            dst[q, pl.ds(PAD, 32), :] = (1.0 / 3.0) * v[q] + (NINTH * nb + s3[q])

    @pl.loop(0, 3)
    def _(i):
        sweep3(a3, b3)
        sweep3(b3, a3)

    sweep3(a3, b3)

    for i, step in enumerate((-3, -2, -1, 1, 2, 3)):
        @pl.when(inside(-step))
        def _():
            h2_copy(i).wait_recv()

    flag2 = {p: inside(p - 3).astype(F32) for p in range(1, 6)}
    for p in range(1, 6):
        at = d + p - 3
        q = jnp.clip(at // 4, 0, 3)
        block = lax.rem(at + gz, 4) * 32
        m = selection((128, 128), lambda i, j: i == ((j & 63) >> 1) + block)
        e = split_dot(b3[q, pl.ds(PAD, 32), :], m)
        pe2[p - 1, pl.ds(0, 32, stride=2), :] = e
        pe2[p - 1, pl.ds(1, 32, stride=2), :] = e
    for p in range(1, 6):
        c = crow(s2, p, 0, 64)
        w = 12.0 * c + nb2(s2, p, c)
        a2[p, pl.ds(PAD, 64), :] = flag2[p] * (N81 * w + pe2[p - 1])

    def sweep2(src, dst, p):
        c = crow(src, p, 0, 64)
        dst[p, pl.ds(PAD, 64), :] = flag2[p] * (
            (1.0 / 3.0) * c + NINTH * (nb2(src, p, c) + crow(s2, p, 0, 64))
        )

    for p in range(1, 6):
        sweep2(a2, b2, p)
    for p in range(2, 5):
        sweep2(b2, a2, p)

    for i in range(4):
        @pl.when(h1_recvs[i])
        def _():
            h1_copy(i).wait_recv()

    for half in range(2):
        m = selection((128, 128), lambda i, j: i == (j >> 1) + 64 * half)
        for p in range(3):
            e = split_dot(a2[2 + p, pl.ds(PAD, 64), :], m)
            pe1[2 * p + half, pl.ds(0, 64, stride=2), :] = e
            pe1[2 * p + half, pl.ds(1, 64, stride=2), :] = e

    def bounds(first, last, own):
        return jnp.where(has_lo, first, 0), jnp.where(has_hi, last + 1, own)

    lo1, hi1 = bounds(-4, 7, 4)

    @pl.loop(lo1 + 5, hi1 + 5)
    def _(z):
        for r in range(0, 128, 64):
            c = crow(s1, z, r, 64)
            w = 12.0 * c + nbxy(s1, z, r, 64, c, 128) + (crow(s1, z - 1, r, 64) + crow(s1, z + 1, r, 64))
            a1[z, pl.ds(PAD + r, 64), :] = N81 * w + pe1[(z - 1) // 2, pl.ds(r, 64), :]

    def sweep1(src, dst, first, last):
        lo, hi = bounds(first, last, 4)

        @pl.loop(lo + 5, hi + 5)
        def _(z):
            for r in range(0, 128, 64):
                c = crow(src, z, r, 64)
                nb = nbxy(src, z, r, 64, c, 128) + (crow(src, z - 1, r, 64) + crow(src, z + 1, r, 64))
                dst[z, pl.ds(PAD + r, 64), :] = (1.0 / 3.0) * c + NINTH * (nb + crow(s1, z, r, 64))

    sweep1(a1, b1, -3, 6)
    sweep1(b1, a1, -2, 5)

    @pl.when(has_lo)
    def _():
        for k in range(4):
            f_copy(1, k).wait_recv()

    @pl.when(has_hi)
    def _():
        for k in range(4):
            f_copy(0, k).wait_recv()

    lo0, hi0 = bounds(-3, 10, 8)

    @pl.loop(lo0 + 4, 5)
    def _(z):
        w_plane(z, True, True)

    @pl.loop(11, hi0 + 4)
    def _(z):
        w_plane(z, True, True)

    @pl.loop(lo0 + 4, hi0 + 4)
    def _(z):
        e = a1[z // 2 + 3, pl.ds(PAD, 128), :]
        for ph in range(4):
            a[z, ph, pl.ds(PAD, 128), :] = N81 * a[z, ph, pl.ds(PAD, 128), :] + e

    def sweep0(src, dst, first, last):
        lo, hi = bounds(first, last, 8)

        @pl.loop(lo + 4, hi + 4)
        def _(z):
            for r in range(0, 128, CH):
                c = center(src, z, r, CH)
                nb = nbxy0(src, z, r, CH, c)
                for ph in range(4):
                    t = nb[ph] + (rows(src, z - 1, ph, r, CH) + rows(src, z + 1, ph, r, CH))
                    t = t + rows(f, z, ph, r, CH)
                    dst[z, ph, pl.ds(PAD + r, CH), :] = (1.0 / 3.0) * c[ph] + NINTH * t

    sweep0(a, b, -2, 9)
    sweep0(b, a, -1, 8)

    def final(z, carry):
        squares, products = carry
        for r in range(0, 128, CH):
            c = center(a, z, r, CH)
            nb = nbxy0(a, z, r, CH, c)
            for ph in range(4):
                t = nb[ph] + (rows(a, z - 1, ph, r, CH) + rows(a, z + 1, ph, r, CH))
                src = rows(f, z, ph, r, CH)
                left = (src - 6.0 * c[ph]) + t
                squares = squares + fold(left * left)
                products = products + fold(src * c[ph])
        return squares, products

    zero = jnp.zeros((8, 128), F32)
    squares, products = lax.fori_loop(4, 12, final, (zero, zero))
    sums[d, pl.ds(0, 8), :] = squares
    sums[d, pl.ds(8, 8), :] = products

    @pl.loop(1, gz)
    def _(o):
        remote(sums.at[d], sums.at[d], ss.at[o], sr.at[d], gz=lax.rem(d + o, gz)).start()

    px[...] = selection((256, 256), lambda i, j: i == (j & 1) * 128 + (j >> 1))

    def out_copy(z, half):
        return pltpu.make_async_copy(
            obuf.at[z, half], pot.at[0, z, :, pl.ds(128 * half, 128)], out_sem.at[z, half]
        )

    @pl.loop(0, 8)
    def _(z):
        for yp in range(2):
            x = jnp.concatenate(
                [a[z + 4, 2 * yp, pl.ds(PAD, 128), :], a[z + 4, 2 * yp + 1, pl.ds(PAD, 128), :]], axis=1
            )
            y = split_dot(x, px[...])
            for half in range(2):
                obuf[z, half, pl.ds(yp, 128, stride=2), :] = y[:, 128 * half:128 * half + 128]
        for half in range(2):
            out_copy(z, half).start()

    @pl.loop(1, gz)
    def _(o):
        peer = lax.rem(d + o, gz)
        remote(sums.at[peer], sums.at[peer], ss.at[o], sr.at[peer], gz=peer).wait_recv()

    total = sums[0]
    for e in range(1, gz):
        total = total + sums[e]
    cells = 1.0 / (gz * 8 * 256 * 256)
    ens[me] = pweight[0] * total[8:]

    @pl.loop(1, pairs)
    def _(o):
        remote(ens.at[me], ens.at[me], es.at[o], er.at[me], pair=lax.rem(me + o, pairs)).start()

    norm = jnp.sqrt(jnp.full((8, 128), jnp.sum(total[:8]) * cells, F32))
    res_out[0] = jnp.max(norm)

    @pl.loop(1, pairs)
    def _(o):
        peer = lax.rem(me + o, pairs)
        remote(ens.at[peer], ens.at[peer], es.at[o], er.at[peer], pair=peer).wait_recv()

    energy = ens[0]
    for e in range(1, pairs):
        energy = energy + ens[e]
    en_out[0] = jnp.sum(energy) * (-0.5 * cells)

    for cond, side in ((has_lo, 0), (has_hi, 1)):
        @pl.when(cond)
        def _():
            (g0_lo, g0_hi)[side].wait_send()
            (g1_lo, g1_hi)[side].wait_send()
            for k in range(4):
                f_copy(side, k).wait_send()

    for i in range(4):
        @pl.when(h1_sends[i])
        def _():
            h1_copy(i).wait_send()

    for i, step in enumerate((-3, -2, -1, 1, 2, 3)):
        @pl.when(inside(step))
        def _():
            h2_copy(i).wait_send()

    @pl.loop(1, gz)
    def _(o):
        t3_copy(o).wait_send()
        remote(sums.at[d], sums.at[d], ss.at[o], sr.at[d], gz=lax.rem(d + o, gz)).wait_send()

    @pl.loop(1, pairs)
    def _(o):
        remote(ens.at[me], ens.at[me], es.at[o], er.at[me], pair=lax.rem(me + o, pairs)).wait_send()

    @pl.loop(0, 8)
    def _(z):
        for half in range(2):
            out_copy(z, half).wait()


def solution(mesh):
    gz, pairs = mesh.shape["gz"], mesh.shape["pair"]
    dma, vmem = pltpu.SemaphoreType.DMA, pltpu.VMEM
    field = vmem((16, 4, 144, 128), F32)
    level1, level2, level3 = vmem((14, 144, 128), F32), vmem((7, 80, 128), F32), vmem((4, 48, 128), F32)

    def per_device(orbitals, pair_index, pair_weight):
        return pl.pallas_call(
            functools.partial(kernel, gz, pairs),
            out_shape=(
                jax.ShapeDtypeStruct((1, 8, 256, 256), F32),
                jax.ShapeDtypeStruct((1,), F32),
                jax.ShapeDtypeStruct((1,), F32),
            ),
            in_specs=[
                pl.BlockSpec(memory_space=pltpu.SMEM),
                pl.BlockSpec(memory_space=pltpu.SMEM),
                pl.BlockSpec(memory_space=pl.ANY),
            ],
            out_specs=(
                pl.BlockSpec(memory_space=pl.ANY),
                pl.BlockSpec(memory_space=pltpu.SMEM),
                pl.BlockSpec(memory_space=pltpu.SMEM),
            ),
            scratch_shapes=[
                *[vmem((8, 256, 256), BF16)] * 8,
                vmem((256, 256), BF16),
                vmem((2, 2, 256, 128), F32),
                field, field, field,
                vmem((2, 128, 128), F32), vmem((2, 128, 128), F32),
                level1, level1, level1,
                vmem((4, 128, 128), F32),
                vmem((2, 64, 128), F32), vmem((2, 64, 128), F32),
                vmem((6, 128, 128), F32),
                level2, level2, level2,
                vmem((3, 64, 128), F32),
                vmem((5, 64, 128), F32),
                vmem((gz, 32, 128), F32),
                vmem((4, 32, 128), F32),
                level3, level3,
                vmem((gz, 16, 128), F32),
                vmem((pairs, 8, 128), F32),
                vmem((8, 2, 256, 128), F32),
                dma((8,)),
                dma((2, 4)), dma((2, 4)),
                dma((2,)), dma((2,)),
                dma((4,)), dma((4,)),
                dma((2,)), dma((2,)),
                dma((6,)), dma((6,)),
                dma((gz,)), dma((gz,)),
                dma((gz,)), dma((gz,)),
                dma((pairs,)), dma((pairs,)),
                dma((8, 2)),
            ],
            compiler_params=pltpu.CompilerParams(
                collective_id=0, has_side_effects=True, vmem_limit_bytes=60 * 1024 * 1024
            ),
            name="vcycle",
        )(pair_index, pair_weight, orbitals)

    return jax.shard_map(
        per_device,
        mesh=mesh,
        in_specs=(P(None, "gz", None, None), P("pair", None), P("pair")),
        out_specs=(P("pair", "gz", None, None), P("pair"), P()),
        check_vma=False,
    )
```

```python
import functools

import jax
import jax.numpy as jnp
from jax import lax
from jax.experimental import pallas as pl
from jax.experimental.pallas import tpu as pltpu
from jax.sharding import PartitionSpec as P

MESH = pl.DeviceIdType.MESH
F32, BF16 = jnp.float32, jnp.bfloat16
PAD = 8
CH = 32
NINTH = 1.0 / 9.0
N81 = 1.0 / 81.0


def lane_iota(shape):
    return lax.broadcasted_iota(jnp.int32, shape, len(shape) - 1)


def roll(x, shift):
    return pltpu.roll(x, shift % x.shape[-1], x.ndim - 1)


def from_left(x, width=128):
    return jnp.where(lane_iota(x.shape) % width == 0, 0.0, roll(x, 1))


def from_right(x, width=128):
    return jnp.where(lane_iota(x.shape) % width == width - 1, 0.0, roll(x, -1))


def split_dot(x, m):
    hi = x.astype(BF16)
    rest = x - hi.astype(F32)
    mid = rest.astype(BF16)
    low = (rest - mid.astype(F32)).astype(BF16)
    dot = functools.partial(jnp.dot, preferred_element_type=F32)
    return dot(hi, m) + dot(mid, m) + dot(low, m)


def selection(shape, test):
    a = lax.broadcasted_iota(jnp.int32, shape, 0)
    b = lax.broadcasted_iota(jnp.int32, shape, 1)
    return jnp.where(test(a, b), 1.0, 0.0).astype(BF16)


def fold(x):
    return x.reshape(x.shape[0] // 8, 8, x.shape[1]).sum(axis=0)


def rows(ref, z, ph, r, n, dr=0):
    return ref[z, ph, pl.ds(PAD + r + dr, n), :]


def nbxy0(ref, z, r, n, c):
    out = []
    for yp in range(2):
        for xp in range(2):
            side = c[2 * yp + 1 - xp]
            x = side + (from_right(side) if xp else from_left(side))
            other = 2 * (1 - yp) + xp
            y = c[other] + rows(ref, z, other, r, n, 1 if yp else -1)
            out.append(x + y)
    return out


def phase_sums(ref, z, r, n, c):
    total = (c[0] + c[1]) + (c[2] + c[3])
    shifts = from_left(c[1] + c[3]) + from_right(c[0] + c[2])
    shifts = shifts + (rows(ref, z, 2, r, n, -1) + rows(ref, z, 3, r, n, -1))
    shifts = shifts + (rows(ref, z, 0, r, n, 1) + rows(ref, z, 1, r, n, 1))
    return total, shifts


def center(ref, z, r, n):
    return [rows(ref, z, ph, r, n) for ph in range(4)]


def crow(ref, z, r, n, dr=0):
    return ref[z, pl.ds(PAD + r + dr, n), :]


def nbxy(ref, z, r, n, c, width):
    y = crow(ref, z, r, n, -1) + crow(ref, z, r, n, 1)
    return y + (from_left(c, width) + from_right(c, width))


def kernel(
    gz, pairs,
    pidx, pweight, orbitals, pot, res_out, en_out,
    orb0, orb1, orb2, orb3, orb4, orb5, orb6, orb7, px, tmp, pidx2, fx, f, a, b, g0, g0o, s1, a1, b1, t1, g1, g1o, pe1,
    s2, a2, b2, t2, pe2, t3, s3, a3, b3, sums, ens, obuf,
    orb_sem, ixs, ixr, fs, fr, g0s, g0r, h1s, h1r, g1s, g1r, h2s, h2r, t3s, t3r, ss, sr, es, er, out_sem,
):
    d = lax.axis_index("gz")
    me = lax.axis_index("pair")
    has_lo, has_hi = d > 0, d < gz - 1
    flo, fhi = has_lo.astype(F32), has_hi.astype(F32)

    def remote(src, dst, s_sem, r_sem, **to):
        return pltpu.make_async_remote_copy(
            src_ref=src, dst_ref=dst, send_sem=s_sem, recv_sem=r_sem, device_id=to, device_id_type=MESH
        )

    orb = (orb0, orb1, orb2, orb3, orb4, orb5, orb6, orb7)

    def orb_copy(z):
        return pltpu.make_async_copy(orbitals.at[:, z], orb[z], orb_sem.at[z])

    for z in (0, 7, 1, 6, 2, 5, 3, 4):
        orb_copy(z).start()
    barrier = pltpu.get_barrier_semaphore()

    @pl.loop(1, gz)
    def _(o):
        pl.semaphore_signal(barrier, inc=1, device_id={"gz": lax.rem(d + o, gz)}, device_id_type=MESH)

    @pl.loop(1, pairs)
    def _(o):
        pl.semaphore_signal(barrier, inc=1, device_id={"pair": lax.rem(me + o, pairs)}, device_id_type=MESH)

    other = lax.rem(me + pairs // 2, pairs)
    even = lax.rem(d, 2) == 0
    across = jnp.where(even, d - 1, d + 1)
    has_across = jnp.logical_and(across >= 0, across < gz)

    @pl.when(has_across)
    def _():
        pl.semaphore_signal(barrier, inc=1, device_id={"gz": across, "pair": other}, device_id_type=MESH)

    px[...] = selection((256, 256), lambda i, j: j == (i & 1) * 128 + (i >> 1))
    pad0 = jnp.zeros((4, PAD, 128), F32)

    @pl.loop(0, 16)
    def _(z):
        for ref in (f, a, b):
            ref[z, :, pl.ds(0, PAD), :] = pad0
            ref[z, :, pl.ds(PAD + 128, PAD), :] = pad0

    def clear_outside(first):
        @pl.loop(first, first + 4)
        def _(z):
            for ref in (f, a, b):
                for ph in range(4):
                    ref[z, ph, pl.ds(PAD, 128), :] = jnp.zeros((128, 128), F32)

        @pl.when(first == 0)
        def _():
            @pl.loop(0, 5)
            def _(z):
                s1[z, pl.ds(PAD, 128), :] = jnp.zeros((128, 128), F32)

        @pl.when(first > 0)
        def _():
            @pl.loop(9, 14)
            def _(z):
                s1[z, pl.ds(PAD, 128), :] = jnp.zeros((128, 128), F32)

    @pl.when(d == 0)
    def _():
        clear_outside(0)
        g0[0] = jnp.zeros((128, 128), F32)
        g1[0] = jnp.zeros((64, 128), F32)

    @pl.when(d == gz - 1)
    def _():
        clear_outside(12)
        g0[1] = jnp.zeros((128, 128), F32)
        g1[1] = jnp.zeros((64, 128), F32)

    @pl.when(d == 1)
    def _():
        s1[0, pl.ds(PAD, 128), :] = jnp.zeros((128, 128), F32)

    @pl.when(d == gz - 2)
    def _():
        s1[13, pl.ds(PAD, 128), :] = jnp.zeros((128, 128), F32)

    @pl.loop(0, 14)
    def _(z):
        s1[z, pl.ds(0, PAD), :] = jnp.zeros((PAD, 128), F32)
        s1[z, pl.ds(PAD + 128, PAD), :] = jnp.zeros((PAD, 128), F32)
        a1[z] = jnp.zeros((144, 128), F32)
        b1[z] = jnp.zeros((144, 128), F32)

    @pl.loop(0, 7)
    def _(p):
        s2[p, pl.ds(0, PAD), :] = jnp.zeros((PAD, 128), F32)
        s2[p, pl.ds(PAD + 64, PAD), :] = jnp.zeros((PAD, 128), F32)
        a2[p] = jnp.zeros((80, 128), F32)
        b2[p] = jnp.zeros((80, 128), F32)
        at = d + p - 3

        @pl.when(jnp.logical_or(at < 0, at >= gz))
        def _():
            s2[p, pl.ds(PAD, 64), :] = jnp.zeros((64, 128), F32)

    for q in range(4):
        a3[q] = jnp.zeros((48, 128), F32)
        b3[q] = jnp.zeros((48, 128), F32)

    def density(z, which, slot, put):
        left = jnp.dot(orb[z][which[0, 0]], px[...], preferred_element_type=F32)
        right = jnp.dot(orb[z][which[0, 1]], px[...], preferred_element_type=F32)
        both = left * right
        tmp[slot, 0] = both[:, :128]
        tmp[slot, 1] = both[:, 128:]
        for yp in range(2):
            for xp in range(2):
                put(2 * yp + xp, tmp[slot, xp, pl.ds(yp, 128, stride=2), :])

    for i, z in enumerate((0, 7, 1, 6, 2, 5, 3, 4)):
        orb_copy(z).wait()

        def put(ph, value):
            f[z + 4, ph, pl.ds(PAD, 128), :] = value

        density(z, pidx, i % 2, put)

    def w_plane(z, lo, hi):
        for r in range(0, 128, CH):
            c = center(f, z, r, CH)
            nb = nbxy0(f, z, r, CH, c)
            for ph in range(4):
                t = 12.0 * c[ph] + nb[ph]
                if lo:
                    t = t + rows(f, z - 1, ph, r, CH)
                if hi:
                    t = t + rows(f, z + 1, ph, r, CH)
                a[z, ph, pl.ds(PAD + r, CH), :] = t

    w_plane(4, False, True)
    w_plane(11, True, False)

    pl.semaphore_wait(barrier, gz - 1 + pairs - 1 + has_across.astype(jnp.int32))

    index_copy = remote(pidx, pidx2, ixs.at[0], ixr.at[0], pair=other)
    index_copy.start()

    for side, z in ((0, 4), (1, 11)):
        for r in range(0, 128, CH):
            total, shifts = phase_sums(f, z, r, CH, center(f, z, r, CH))
            w = center(a, z, r, CH)
            g0o[side, pl.ds(r, CH), :] = (0.5 * N81) * (
                shifts - 3.0 * total + ((w[0] + w[1]) + (w[2] + w[3]))
            )

    def exchange(out, landed, s_sems, r_sems):
        lo = remote(out.at[0], landed.at[1], s_sems.at[0], r_sems.at[1], gz=jnp.maximum(d - 1, 0))
        hi = remote(out.at[1], landed.at[0], s_sems.at[1], r_sems.at[0], gz=jnp.minimum(d + 1, gz - 1))
        return lo, hi

    g0_lo, g0_hi = exchange(g0o, g0, g0s, g0r)

    @pl.when(has_lo)
    def _():
        g0_lo.start()

    @pl.when(has_hi)
    def _():
        g0_hi.start()

    turn = lax.rem(d, 4)
    straight = jnp.logical_or(turn == 1, turn == 2)

    def f_copy(side, far, of_other):
        k = far if side == 0 else 3 - far
        here = k if side == 0 else 4 + k
        there = 12 + k if side == 0 else k
        to = jnp.maximum(d - 1, 0) if side == 0 else jnp.minimum(d + 1, gz - 1)
        landed = f.at[there, :, pl.ds(PAD, 128), :]
        if of_other:
            return remote(fx.at[k], landed, fs.at[side, far], fr.at[1 - side, far], gz=to, pair=other)
        return remote(
            f.at[4 + here, :, pl.ds(PAD, 128), :], landed, fs.at[side, far], fr.at[1 - side, far], gz=to, pair=me
        )

    def on_chip(act):
        for side, cond in ((0, jnp.logical_not(even)), (1, even)):
            @pl.when(cond)
            def _():
                for far in range(4):
                    act(side, far, False)

    def crossing(far, act, of_other):
        for side, cond in ((0, jnp.logical_and(even, has_lo)), (1, jnp.logical_and(jnp.logical_not(even), has_hi))):
            if far == 3:
                cond = jnp.logical_and(cond, jnp.logical_not(straight) if of_other else straight)
            elif not of_other:
                continue

            @pl.when(cond)
            def _():
                act(side, far, of_other)

    def begin(side, far, of_other):
        f_copy(side, far, of_other).start()

    def sent(side, far, of_other):
        f_copy(side, far, of_other).wait_send()

    on_chip(begin)

    @pl.loop(5, 11)
    def _(z):
        w_plane(z, True, True)

    for ph in range(4):
        a[3, ph, pl.ds(PAD, 128), :] = flo * f[4, ph, pl.ds(PAD, 128), :]
        a[12, ph, pl.ds(PAD, 128), :] = fhi * f[11, ph, pl.ds(PAD, 128), :]

    @pl.loop(0, 4)
    def _(j):
        for r in range(0, 128, CH):
            out = None
            for dz in range(2):
                z = 4 + 2 * j + dz
                c = center(a, z, r, CH)
                total, shifts = phase_sums(a, z, r, CH, c)
                below, above, src = center(a, z - 1, r, CH), center(a, z + 1, r, CH), center(f, z, r, CH)
                zs = ((below[0] + below[1]) + (below[2] + below[3])) + (
                    (above[0] + above[1]) + (above[2] + above[3])
                )
                q = ((src[0] + src[1]) + (src[2] + src[3])) + N81 * (zs - 4.0 * total + shifts)
                out = q if out is None else out + q
            s1[5 + j, pl.ds(PAD + r, CH), :] = 0.5 * out

    index_copy.wait_recv()
    for far in range(4):
        for side, cond in ((0, even), (1, jnp.logical_not(even))):
            k = far if side == 0 else 3 - far

            def put_other(ph, value):
                fx[k, ph] = value

            @pl.when(cond)
            def _():
                density(k + 4 * side, pidx2, far % 2, put_other)

        crossing(far, begin, True)

    @pl.when(has_lo)
    def _():
        g0_hi.wait_recv()
        s1[5, pl.ds(PAD, 128), :] += g0[0]

    @pl.when(has_hi)
    def _():
        g0_lo.wait_recv()
        s1[8, pl.ds(PAD, 128), :] += g0[1]

    def w1_plane(z, lo, hi):
        for r in range(0, 128, 64):
            c = crow(s1, z, r, 64)
            t = 12.0 * c + nbxy(s1, z, r, 64, c, 128)
            if lo:
                t = t + crow(s1, z - 1, r, 64)
            if hi:
                t = t + crow(s1, z + 1, r, 64)
            a1[z, pl.ds(PAD + r, 64), :] = t

    for z in range(5, 9):
        w1_plane(z, z > 5, z < 8)
    a1[4, pl.ds(PAD, 128), :] = flo * crow(s1, 5, 0, 128)
    a1[9, pl.ds(PAD, 128), :] = fhi * crow(s1, 8, 0, 128)
    for slot, z in ((0, 5), (3, 8)):
        for r in range(0, 128, 64):
            c = crow(s1, z, r, 64)
            t1[slot, pl.ds(r, 64), :] = (0.5 * N81) * (
                nbxy(s1, z, r, 64, c, 128) - 5.0 * c + crow(a1, z, r, 64)
            )
    for slot in (1, 2):
        for r in range(0, 128, 64):
            out = None
            for z in (3 + 2 * slot, 4 + 2 * slot):
                c = crow(a1, z, r, 64)
                nb = nbxy(a1, z, r, 64, c, 128) + (crow(a1, z - 1, r, 64) + crow(a1, z + 1, r, 64))
                q = crow(s1, z, r, 64) + N81 * (nb - 6.0 * c)
                out = q if out is None else out + q
            t1[slot, pl.ds(r, 64), :] = 0.5 * out

    def ypair(ref, slot, n):
        return ref[slot, pl.ds(0, n, stride=2), :] + ref[slot, pl.ds(1, n, stride=2), :]

    m_first = selection((128, 128), lambda i, j: (i >> 1) == j)
    m_second = selection((128, 128), lambda i, j: (i >> 1) + 64 == j)
    g1o[0] = split_dot(ypair(t1, 0, 64), m_second)
    g1o[1] = split_dot(ypair(t1, 3, 64), m_first)
    g1_lo, g1_hi = exchange(g1o, g1, g1s, g1r)

    @pl.when(has_lo)
    def _():
        g1_lo.start()

    @pl.when(has_hi)
    def _():
        g1_hi.start()

    s2[3, pl.ds(PAD, 64), :] = split_dot(ypair(t1, 1, 64), m_first) + split_dot(ypair(t1, 2, 64), m_second)

    def h1_copy(i):
        here, there, step = ((5, 9, -1), (5, 1, 1), (5, 13, -2), (8, 0, 2))[i]
        n = 4 if abs(step) == 1 else 1
        to = jnp.clip(d + step, 0, gz - 1)
        return remote(
            s1.at[pl.ds(here, n), pl.ds(PAD, 128), :], s1.at[pl.ds(there, n), pl.ds(PAD, 128), :],
            h1s.at[i], h1r.at[i], gz=to,
        )

    h1_sends = [d >= 1, d <= gz - 2, d >= 2, d <= gz - 3]
    h1_recvs = [d <= gz - 2, d >= 1, d <= gz - 3, d >= 2]

    def h1_start():
        for i in range(4):
            @pl.when(h1_sends[i])
            def _():
                h1_copy(i).start()

    @pl.when(has_lo)
    def _():
        g1_hi.wait_recv()
        s2[3, pl.ds(PAD, 64), :] += g1[0]

    @pl.when(has_hi)
    def _():
        g1_lo.wait_recv()
        s2[3, pl.ds(PAD, 64), :] += g1[1]

    low_half = lane_iota((64, 128)) < 64

    def nb2(ref, p, c):
        z = roll(c + jnp.where(low_half, crow(ref, p + 1, 0, 64), crow(ref, p - 1, 0, 64)), 64)
        return nbxy(ref, p, 0, 64, c, 64) + z

    def h2_copy(i):
        step = (-3, -2, -1, 1, 2, 3)[i]
        to = jnp.clip(d + step, 0, gz - 1)
        return remote(
            s2.at[3, pl.ds(PAD, 64), :], s2.at[3 - step, pl.ds(PAD, 64), :], h2s.at[i], h2r.at[i], gz=to
        )

    def inside(step):
        at = d + step
        return jnp.logical_and(at >= 0, at < gz)

    c = crow(s2, 3, 0, 64)
    turned = roll(c, 64)
    w0 = 12.0 * c + nbxy(s2, 3, 0, 64, c, 64) + turned
    a2[3, pl.ds(PAD, 64), :] = w0
    a2[2, pl.ds(PAD, 64), :] = flo * jnp.where(low_half, 0.0, turned)
    a2[4, pl.ds(PAD, 64), :] = fhi * jnp.where(low_half, turned, 0.0)
    for p in (2, 3, 4):
        w = crow(a2, p, 0, 64)
        r = N81 * (nb2(a2, p, w) - 6.0 * w)
        t2[p - 2] = r + c if p == 3 else r
    tile = None
    for p in range(3):
        block = lax.rem(d + p - 1 + gz, 4) * 32
        m = selection((128, 128), lambda i, j: ((i & 63) >> 1) + block == j)
        part = split_dot(ypair(t2, p, 32), m)
        tile = part if tile is None else tile + part
    t3[d] = 0.5 * tile

    def t3_copy(o):
        to = lax.rem(d + o, gz)
        return remote(t3.at[d], t3.at[d], t3s.at[o], t3r.at[d], gz=to)

    @pl.loop(1, gz)
    def _(o):
        t3_copy(o).start()

    for i, step in enumerate((-3, -2, -1, 1, 2, 3)):
        @pl.when(inside(step))
        def _():
            h2_copy(i).start()

    h1_start()
    crossing(3, begin, False)

    @pl.loop(1, gz)
    def _(o):
        peer = lax.rem(d + o, gz)
        remote(t3.at[peer], t3.at[peer], t3s.at[o], t3r.at[peer], gz=peer).wait_recv()

    lane32 = lane_iota((32, 128))
    for q in range(4):
        total = None
        for e in range(max(4 * q - 1, 0), min(4 * q + 5, gz)):
            x = t3[e]
            if e == 4 * q - 1:
                x = jnp.where(lane32 < 32, x, 0.0)
            elif e == 4 * q + 4:
                x = jnp.where(lane32 >= 96, x, 0.0)
            elif e == 4 * q:
                x = jnp.where(lane32 < 96, x, 0.0)
            elif e == 4 * q + 3:
                x = jnp.where(lane32 >= 32, x, 0.0)
            total = x if total is None else total + x
        s3[q] = total * NINTH
        a3[q, pl.ds(PAD, 32), :] = total * NINTH

    def sweep3(src, dst):
        v = [crow(src, q, 0, 32) for q in range(4)]
        for q in range(4):
            after = v[q + 1] if q < 3 else jnp.zeros_like(v[0])
            before = v[q - 1] if q > 0 else jnp.zeros_like(v[0])
            nz = roll(jnp.where(lane32 < 32, after, v[q]), -32)
            nz = nz + roll(jnp.where(lane32 >= 96, before, v[q]), 32)
            nb = nbxy(src, q, 0, 32, v[q], 32) + nz
            dst[q, pl.ds(PAD, 32), :] = (1.0 / 3.0) * v[q] + (NINTH * nb + s3[q])

    @pl.loop(0, 3)
    def _(i):
        sweep3(a3, b3)
        sweep3(b3, a3)

    sweep3(a3, b3)

    for i, step in enumerate((-3, -2, -1, 1, 2, 3)):
        @pl.when(inside(-step))
        def _():
            h2_copy(i).wait_recv()

    flag2 = {p: inside(p - 3).astype(F32) for p in range(1, 6)}
    for p in range(1, 6):
        at = d + p - 3
        q = jnp.clip(at // 4, 0, 3)
        block = lax.rem(at + gz, 4) * 32
        m = selection((128, 128), lambda i, j: i == ((j & 63) >> 1) + block)
        e = split_dot(b3[q, pl.ds(PAD, 32), :], m)
        pe2[p - 1, pl.ds(0, 32, stride=2), :] = e
        pe2[p - 1, pl.ds(1, 32, stride=2), :] = e
    for p in range(1, 6):
        c = crow(s2, p, 0, 64)
        w = 12.0 * c + nb2(s2, p, c)
        a2[p, pl.ds(PAD, 64), :] = flag2[p] * (N81 * w + pe2[p - 1])

    def sweep2(src, dst, p):
        c = crow(src, p, 0, 64)
        dst[p, pl.ds(PAD, 64), :] = flag2[p] * (
            (1.0 / 3.0) * c + NINTH * (nb2(src, p, c) + crow(s2, p, 0, 64))
        )

    for p in range(1, 6):
        sweep2(a2, b2, p)
    for p in range(2, 5):
        sweep2(b2, a2, p)

    for i in range(4):
        @pl.when(h1_recvs[i])
        def _():
            h1_copy(i).wait_recv()

    for half in range(2):
        m = selection((128, 128), lambda i, j: i == (j >> 1) + 64 * half)
        for p in range(3):
            e = split_dot(a2[2 + p, pl.ds(PAD, 64), :], m)
            pe1[2 * p + half, pl.ds(0, 64, stride=2), :] = e
            pe1[2 * p + half, pl.ds(1, 64, stride=2), :] = e

    def bounds(first, last, own):
        return jnp.where(has_lo, first, 0), jnp.where(has_hi, last + 1, own)

    lo1, hi1 = bounds(-4, 7, 4)

    @pl.loop(lo1 + 5, hi1 + 5)
    def _(z):
        for r in range(0, 128, 64):
            c = crow(s1, z, r, 64)
            w = 12.0 * c + nbxy(s1, z, r, 64, c, 128) + (crow(s1, z - 1, r, 64) + crow(s1, z + 1, r, 64))
            a1[z, pl.ds(PAD + r, 64), :] = N81 * w + pe1[(z - 1) // 2, pl.ds(r, 64), :]

    def sweep1(src, dst, first, last):
        lo, hi = bounds(first, last, 4)

        @pl.loop(lo + 5, hi + 5)
        def _(z):
            for r in range(0, 128, 64):
                c = crow(src, z, r, 64)
                nb = nbxy(src, z, r, 64, c, 128) + (crow(src, z - 1, r, 64) + crow(src, z + 1, r, 64))
                dst[z, pl.ds(PAD + r, 64), :] = (1.0 / 3.0) * c + NINTH * (nb + crow(s1, z, r, 64))

    sweep1(a1, b1, -3, 6)
    sweep1(b1, a1, -2, 5)

    @pl.when(has_lo)
    def _():
        for far in range(4):
            f_copy(1, far, False).wait_recv()

    @pl.when(has_hi)
    def _():
        for far in range(4):
            f_copy(0, far, False).wait_recv()

    lo0, hi0 = bounds(-3, 10, 8)

    @pl.loop(lo0 + 4, 5)
    def _(z):
        w_plane(z, True, True)

    @pl.loop(11, hi0 + 4)
    def _(z):
        w_plane(z, True, True)

    @pl.loop(lo0 + 4, hi0 + 4)
    def _(z):
        e = a1[z // 2 + 3, pl.ds(PAD, 128), :]
        for ph in range(4):
            a[z, ph, pl.ds(PAD, 128), :] = N81 * a[z, ph, pl.ds(PAD, 128), :] + e

    def sweep0(src, dst, first, last):
        lo, hi = bounds(first, last, 8)

        @pl.loop(lo + 4, hi + 4)
        def _(z):
            for r in range(0, 128, CH):
                c = center(src, z, r, CH)
                nb = nbxy0(src, z, r, CH, c)
                for ph in range(4):
                    t = nb[ph] + (rows(src, z - 1, ph, r, CH) + rows(src, z + 1, ph, r, CH))
                    t = t + rows(f, z, ph, r, CH)
                    dst[z, ph, pl.ds(PAD + r, CH), :] = (1.0 / 3.0) * c[ph] + NINTH * t

    sweep0(a, b, -2, 9)
    sweep0(b, a, -1, 8)

    def final(z, carry):
        squares, products = carry
        for r in range(0, 128, CH):
            c = center(a, z, r, CH)
            nb = nbxy0(a, z, r, CH, c)
            for ph in range(4):
                t = nb[ph] + (rows(a, z - 1, ph, r, CH) + rows(a, z + 1, ph, r, CH))
                src = rows(f, z, ph, r, CH)
                left = (src - 6.0 * c[ph]) + t
                squares = squares + fold(left * left)
                products = products + fold(src * c[ph])
        return squares, products

    zero = jnp.zeros((8, 128), F32)
    squares, products = lax.fori_loop(4, 12, final, (zero, zero))
    sums[d] = jnp.concatenate([squares.sum(axis=0, keepdims=True), products.sum(axis=0, keepdims=True)], axis=0)

    @pl.loop(1, gz)
    def _(o):
        remote(sums.at[d], sums.at[d], ss.at[o], sr.at[d], gz=lax.rem(d + o, gz)).start()

    px[...] = selection((256, 256), lambda i, j: i == (j & 1) * 128 + (j >> 1))

    def out_copy(z, half):
        return pltpu.make_async_copy(
            obuf.at[z, half], pot.at[0, z, :, pl.ds(128 * half, 128)], out_sem.at[z, half]
        )

    @pl.loop(0, 8)
    def _(z):
        for yp in range(2):
            x = jnp.concatenate(
                [a[z + 4, 2 * yp, pl.ds(PAD, 128), :], a[z + 4, 2 * yp + 1, pl.ds(PAD, 128), :]], axis=1
            )
            y = split_dot(x, px[...])
            for half in range(2):
                obuf[z, half, pl.ds(yp, 128, stride=2), :] = y[:, 128 * half:128 * half + 128]
        for half in range(2):
            out_copy(z, half).start()

    @pl.loop(1, gz)
    def _(o):
        peer = lax.rem(d + o, gz)
        remote(sums.at[peer], sums.at[peer], ss.at[o], sr.at[peer], gz=peer).wait_recv()

    total = sums[0]
    for e in range(1, gz):
        total = total + sums[e]
    cells = 1.0 / (gz * 8 * 256 * 256)
    ens[me] = pweight[0] * total[1:]

    @pl.loop(1, pairs)
    def _(o):
        remote(ens.at[me], ens.at[me], es.at[o], er.at[me], pair=lax.rem(me + o, pairs)).start()

    norm = jnp.sqrt(jnp.full((8, 128), jnp.sum(total[:1]) * cells, F32))
    res_out[0] = jnp.max(norm)

    @pl.loop(1, pairs)
    def _(o):
        peer = lax.rem(me + o, pairs)
        remote(ens.at[peer], ens.at[peer], es.at[o], er.at[peer], pair=peer).wait_recv()

    energy = ens[0]
    for e in range(1, pairs):
        energy = energy + ens[e]
    en_out[0] = jnp.sum(energy) * (-0.5 * cells)

    for cond, side in ((has_lo, 0), (has_hi, 1)):
        @pl.when(cond)
        def _():
            (g0_lo, g0_hi)[side].wait_send()
            (g1_lo, g1_hi)[side].wait_send()

    index_copy.wait_send()
    on_chip(sent)
    for far in range(4):
        crossing(far, sent, True)
    crossing(3, sent, False)

    for i in range(4):
        @pl.when(h1_sends[i])
        def _():
            h1_copy(i).wait_send()

    for i, step in enumerate((-3, -2, -1, 1, 2, 3)):
        @pl.when(inside(step))
        def _():
            h2_copy(i).wait_send()

    @pl.loop(1, gz)
    def _(o):
        t3_copy(o).wait_send()
        remote(sums.at[d], sums.at[d], ss.at[o], sr.at[d], gz=lax.rem(d + o, gz)).wait_send()

    @pl.loop(1, pairs)
    def _(o):
        remote(ens.at[me], ens.at[me], es.at[o], er.at[me], pair=lax.rem(me + o, pairs)).wait_send()

    @pl.loop(0, 8)
    def _(z):
        for half in range(2):
            out_copy(z, half).wait()


def solution(mesh):
    gz, pairs = mesh.shape["gz"], mesh.shape["pair"]
    dma, vmem = pltpu.SemaphoreType.DMA, pltpu.VMEM
    field = vmem((16, 4, 144, 128), F32)
    level1, level2, level3 = vmem((14, 144, 128), F32), vmem((7, 80, 128), F32), vmem((4, 48, 128), F32)

    def per_device(orbitals, pair_index, pair_weight):
        return pl.pallas_call(
            functools.partial(kernel, gz, pairs),
            out_shape=(
                jax.ShapeDtypeStruct((1, 8, 256, 256), F32),
                jax.ShapeDtypeStruct((1,), F32),
                jax.ShapeDtypeStruct((1,), F32),
            ),
            in_specs=[
                pl.BlockSpec(memory_space=pltpu.SMEM),
                pl.BlockSpec(memory_space=pltpu.SMEM),
                pl.BlockSpec(memory_space=pl.ANY),
            ],
            out_specs=(
                pl.BlockSpec(memory_space=pl.ANY),
                pl.BlockSpec(memory_space=pltpu.SMEM),
                pl.BlockSpec(memory_space=pltpu.SMEM),
            ),
            scratch_shapes=[
                *[vmem((8, 256, 256), BF16)] * 8,
                vmem((256, 256), BF16),
                vmem((2, 2, 256, 128), F32),
                pltpu.SMEM((1, 2), jnp.int32),
                vmem((4, 4, 128, 128), F32),
                field, field, field,
                vmem((2, 128, 128), F32), vmem((2, 128, 128), F32),
                level1, level1, level1,
                vmem((4, 128, 128), F32),
                vmem((2, 64, 128), F32), vmem((2, 64, 128), F32),
                vmem((6, 128, 128), F32),
                level2, level2, level2,
                vmem((3, 64, 128), F32),
                vmem((5, 64, 128), F32),
                vmem((gz, 32, 128), F32),
                vmem((4, 32, 128), F32),
                level3, level3,
                vmem((gz, 2, 128), F32),
                vmem((pairs, 1, 128), F32),
                vmem((8, 2, 256, 128), F32),
                dma((8,)),
                dma((1,)), dma((1,)),
                dma((2, 4)), dma((2, 4)),
                dma((2,)), dma((2,)),
                dma((4,)), dma((4,)),
                dma((2,)), dma((2,)),
                dma((6,)), dma((6,)),
                dma((gz,)), dma((gz,)),
                dma((gz,)), dma((gz,)),
                dma((pairs,)), dma((pairs,)),
                dma((8, 2)),
            ],
            compiler_params=pltpu.CompilerParams(
                collective_id=0, has_side_effects=True, vmem_limit_bytes=60 * 1024 * 1024
            ),
            name="vcycle",
        )(pair_index, pair_weight, orbitals)

    return jax.shard_map(
        per_device,
        mesh=mesh,
        in_specs=(P(None, "gz", None, None), P("pair", None), P("pair")),
        out_specs=(P("pair", "gz", None, None), P("pair"), P()),
        check_vma=False,
    )
```

```python
import functools

import jax
import jax.numpy as jnp
from jax import lax
from jax.experimental import pallas as pl
from jax.experimental.pallas import tpu as pltpu
from jax.sharding import PartitionSpec as P

MESH = pl.DeviceIdType.MESH
F32, BF16 = jnp.float32, jnp.bfloat16
PAD = 8
CH = 32
NINTH = 1.0 / 9.0
N81 = 1.0 / 81.0


def lane_iota(shape):
    return lax.broadcasted_iota(jnp.int32, shape, len(shape) - 1)


def roll(x, shift):
    return pltpu.roll(x, shift % x.shape[-1], x.ndim - 1)


def from_left(x, width=128):
    return jnp.where(lane_iota(x.shape) % width == 0, 0.0, roll(x, 1))


def from_right(x, width=128):
    return jnp.where(lane_iota(x.shape) % width == width - 1, 0.0, roll(x, -1))


def split_dot(x, m):
    hi = x.astype(BF16)
    rest = x - hi.astype(F32)
    mid = rest.astype(BF16)
    low = (rest - mid.astype(F32)).astype(BF16)
    dot = functools.partial(jnp.dot, preferred_element_type=F32)
    return dot(hi, m) + dot(mid, m) + dot(low, m)


def selection(shape, test):
    a = lax.broadcasted_iota(jnp.int32, shape, 0)
    b = lax.broadcasted_iota(jnp.int32, shape, 1)
    return jnp.where(test(a, b), 1.0, 0.0).astype(BF16)


def fold(x):
    return x.reshape(x.shape[0] // 8, 8, x.shape[1]).sum(axis=0)


def rows(ref, z, ph, r, n, dr=0):
    return ref[z, ph, pl.ds(PAD + r + dr, n), :]


def nbxy0(ref, z, r, n, c):
    out = []
    for yp in range(2):
        for xp in range(2):
            side = c[2 * yp + 1 - xp]
            x = side + (from_right(side) if xp else from_left(side))
            other = 2 * (1 - yp) + xp
            y = c[other] + rows(ref, z, other, r, n, 1 if yp else -1)
            out.append(x + y)
    return out


def phase_sums(ref, z, r, n, c):
    total = (c[0] + c[1]) + (c[2] + c[3])
    shifts = from_left(c[1] + c[3]) + from_right(c[0] + c[2])
    shifts = shifts + (rows(ref, z, 2, r, n, -1) + rows(ref, z, 3, r, n, -1))
    shifts = shifts + (rows(ref, z, 0, r, n, 1) + rows(ref, z, 1, r, n, 1))
    return total, shifts


def center(ref, z, r, n):
    return [rows(ref, z, ph, r, n) for ph in range(4)]


def crow(ref, z, r, n, dr=0):
    return ref[z, pl.ds(PAD + r + dr, n), :]


def nbxy(ref, z, r, n, c, width):
    y = crow(ref, z, r, n, -1) + crow(ref, z, r, n, 1)
    return y + (from_left(c, width) + from_right(c, width))


def kernel(
    gz, pairs,
    index_in, weight_in, orbitals, pot, res_out, en_out,
    orb0, orb1, orb2, orb3, orb4, orb5, orb6, orb7, px, tmp, pidx, pweight, pidx2, fx, f, a, b, g0, g0o, s1, a1, b1, t1, g1, g1o, pe1,
    s2, a2, b2, t2, pe2, t3, s3, a3, b3, sums, ens,
    scalar_sem, orb_sem, ixs, ixr, fs, fr, g0s, g0r, h1s, h1r, g1s, g1r, h2s, h2r, t3s, t3r, ss, sr, es, er,
):
    d = lax.axis_index("gz")
    me = lax.axis_index("pair")
    has_lo, has_hi = d > 0, d < gz - 1
    flo, fhi = has_lo.astype(F32), has_hi.astype(F32)

    def remote(src, dst, s_sem, r_sem, **to):
        return pltpu.make_async_remote_copy(
            src_ref=src, dst_ref=dst, send_sem=s_sem, recv_sem=r_sem, device_id=to, device_id_type=MESH
        )

    orb = (orb0, orb1, orb2, orb3, orb4, orb5, orb6, orb7)

    def orb_copy(z):
        return pltpu.make_async_copy(orbitals.at[:, z], orb[z], orb_sem.at[z])

    index_load = pltpu.make_async_copy(index_in, pidx, scalar_sem.at[0])
    weight_load = pltpu.make_async_copy(weight_in, pweight, scalar_sem.at[1])
    index_load.start()
    weight_load.start()
    for z in (0, 7, 1, 6, 2, 5, 3, 4):
        orb_copy(z).start()
    barrier = pltpu.get_barrier_semaphore()

    @pl.loop(1, gz)
    def _(o):
        pl.semaphore_signal(barrier, inc=1, device_id={"gz": lax.rem(d + o, gz)}, device_id_type=MESH)

    @pl.loop(1, pairs)
    def _(o):
        pl.semaphore_signal(barrier, inc=1, device_id={"pair": lax.rem(me + o, pairs)}, device_id_type=MESH)

    other = lax.rem(me + pairs // 2, pairs)
    even = lax.rem(d, 2) == 0
    across = jnp.where(even, d - 1, d + 1)
    has_across = jnp.logical_and(across >= 0, across < gz)

    @pl.when(has_across)
    def _():
        pl.semaphore_signal(barrier, inc=1, device_id={"gz": across, "pair": other}, device_id_type=MESH)

    px[...] = selection((256, 256), lambda i, j: j == (i & 1) * 128 + (i >> 1))
    pad0 = jnp.zeros((4, PAD, 128), F32)

    @pl.loop(0, 16)
    def _(z):
        for ref in (f, a, b):
            ref[z, :, pl.ds(0, PAD), :] = pad0
            ref[z, :, pl.ds(PAD + 128, PAD), :] = pad0

    def clear_outside(first):
        @pl.loop(first, first + 4)
        def _(z):
            for ref in (f, a, b):
                for ph in range(4):
                    ref[z, ph, pl.ds(PAD, 128), :] = jnp.zeros((128, 128), F32)

        @pl.when(first == 0)
        def _():
            @pl.loop(0, 5)
            def _(z):
                s1[z, pl.ds(PAD, 128), :] = jnp.zeros((128, 128), F32)

        @pl.when(first > 0)
        def _():
            @pl.loop(9, 14)
            def _(z):
                s1[z, pl.ds(PAD, 128), :] = jnp.zeros((128, 128), F32)

    @pl.when(d == 0)
    def _():
        clear_outside(0)
        g0[0] = jnp.zeros((128, 128), F32)
        g1[0] = jnp.zeros((64, 128), F32)

    @pl.when(d == gz - 1)
    def _():
        clear_outside(12)
        g0[1] = jnp.zeros((128, 128), F32)
        g1[1] = jnp.zeros((64, 128), F32)

    @pl.when(d == 1)
    def _():
        s1[0, pl.ds(PAD, 128), :] = jnp.zeros((128, 128), F32)

    @pl.when(d == gz - 2)
    def _():
        s1[13, pl.ds(PAD, 128), :] = jnp.zeros((128, 128), F32)

    @pl.loop(0, 14)
    def _(z):
        s1[z, pl.ds(0, PAD), :] = jnp.zeros((PAD, 128), F32)
        s1[z, pl.ds(PAD + 128, PAD), :] = jnp.zeros((PAD, 128), F32)
        a1[z] = jnp.zeros((144, 128), F32)
        b1[z] = jnp.zeros((144, 128), F32)

    @pl.loop(0, 7)
    def _(p):
        s2[p, pl.ds(0, PAD), :] = jnp.zeros((PAD, 128), F32)
        s2[p, pl.ds(PAD + 64, PAD), :] = jnp.zeros((PAD, 128), F32)
        a2[p] = jnp.zeros((80, 128), F32)
        b2[p] = jnp.zeros((80, 128), F32)
        at = d + p - 3

        @pl.when(jnp.logical_or(at < 0, at >= gz))
        def _():
            s2[p, pl.ds(PAD, 64), :] = jnp.zeros((64, 128), F32)

    for q in range(4):
        a3[q] = jnp.zeros((48, 128), F32)
        b3[q] = jnp.zeros((48, 128), F32)

    def density(z, which, slot, put):
        left = jnp.dot(orb[z][which[0, 0]], px[...], preferred_element_type=F32)
        right = jnp.dot(orb[z][which[0, 1]], px[...], preferred_element_type=F32)
        both = left * right
        tmp[slot, 0] = both[:, :128]
        tmp[slot, 1] = both[:, 128:]
        for yp in range(2):
            for xp in range(2):
                put(2 * yp + xp, tmp[slot, xp, pl.ds(yp, 128, stride=2), :])

    index_load.wait()
    weight_load.wait()
    for i, z in enumerate((0, 7, 1, 6, 2, 5, 3, 4)):
        orb_copy(z).wait()

        def put(ph, value):
            f[z + 4, ph, pl.ds(PAD, 128), :] = value

        density(z, pidx, i % 2, put)

    def w_plane(z, lo, hi):
        for r in range(0, 128, CH):
            c = center(f, z, r, CH)
            nb = nbxy0(f, z, r, CH, c)
            for ph in range(4):
                t = 12.0 * c[ph] + nb[ph]
                if lo:
                    t = t + rows(f, z - 1, ph, r, CH)
                if hi:
                    t = t + rows(f, z + 1, ph, r, CH)
                a[z, ph, pl.ds(PAD + r, CH), :] = t

    w_plane(4, False, True)
    w_plane(11, True, False)

    pl.semaphore_wait(barrier, gz - 1 + pairs - 1 + has_across.astype(jnp.int32))

    index_copy = remote(pidx, pidx2, ixs.at[0], ixr.at[0], pair=other)
    index_copy.start()

    for side, z in ((0, 4), (1, 11)):
        for r in range(0, 128, CH):
            total, shifts = phase_sums(f, z, r, CH, center(f, z, r, CH))
            w = center(a, z, r, CH)
            g0o[side, pl.ds(r, CH), :] = (0.5 * N81) * (
                shifts - 3.0 * total + ((w[0] + w[1]) + (w[2] + w[3]))
            )

    def exchange(out, landed, s_sems, r_sems):
        lo = remote(out.at[0], landed.at[1], s_sems.at[0], r_sems.at[1], gz=jnp.maximum(d - 1, 0))
        hi = remote(out.at[1], landed.at[0], s_sems.at[1], r_sems.at[0], gz=jnp.minimum(d + 1, gz - 1))
        return lo, hi

    g0_lo, g0_hi = exchange(g0o, g0, g0s, g0r)

    @pl.when(has_lo)
    def _():
        g0_lo.start()

    @pl.when(has_hi)
    def _():
        g0_hi.start()

    turn = lax.rem(d, 4)
    straight = jnp.logical_or(turn == 1, turn == 2)

    def f_copy(side, far, of_other):
        k = far if side == 0 else 3 - far
        here = k if side == 0 else 4 + k
        there = 12 + k if side == 0 else k
        to = jnp.maximum(d - 1, 0) if side == 0 else jnp.minimum(d + 1, gz - 1)
        landed = f.at[there, :, pl.ds(PAD, 128), :]
        if of_other:
            return remote(fx.at[k], landed, fs.at[side, far], fr.at[1 - side, far], gz=to, pair=other)
        return remote(
            f.at[4 + here, :, pl.ds(PAD, 128), :], landed, fs.at[side, far], fr.at[1 - side, far], gz=to, pair=me
        )

    def on_chip(act):
        for side, cond in ((0, jnp.logical_not(even)), (1, even)):
            @pl.when(cond)
            def _():
                for far in range(4):
                    act(side, far, False)

    def crossing(far, act, of_other):
        for side, cond in ((0, jnp.logical_and(even, has_lo)), (1, jnp.logical_and(jnp.logical_not(even), has_hi))):
            if far in (0, 3):
                cond = jnp.logical_and(cond, jnp.logical_not(straight) if of_other else straight)
            elif not of_other:
                continue

            @pl.when(cond)
            def _():
                act(side, far, of_other)

    def begin(side, far, of_other):
        f_copy(side, far, of_other).start()

    def sent(side, far, of_other):
        f_copy(side, far, of_other).wait_send()

    crossing(0, begin, False)
    on_chip(begin)

    @pl.loop(5, 11)
    def _(z):
        w_plane(z, True, True)

    for ph in range(4):
        a[3, ph, pl.ds(PAD, 128), :] = flo * f[4, ph, pl.ds(PAD, 128), :]
        a[12, ph, pl.ds(PAD, 128), :] = fhi * f[11, ph, pl.ds(PAD, 128), :]

    @pl.loop(0, 4)
    def _(j):
        for r in range(0, 128, CH):
            out = None
            for dz in range(2):
                z = 4 + 2 * j + dz
                c = center(a, z, r, CH)
                total, shifts = phase_sums(a, z, r, CH, c)
                below, above, src = center(a, z - 1, r, CH), center(a, z + 1, r, CH), center(f, z, r, CH)
                zs = ((below[0] + below[1]) + (below[2] + below[3])) + (
                    (above[0] + above[1]) + (above[2] + above[3])
                )
                q = ((src[0] + src[1]) + (src[2] + src[3])) + N81 * (zs - 4.0 * total + shifts)
                out = q if out is None else out + q
            s1[5 + j, pl.ds(PAD + r, CH), :] = 0.5 * out
            b1[5 + j, pl.ds(PAD + r, CH), :] = 0.5 * out

    def ypair(ref, slot, n):
        return ref[slot, pl.ds(0, n, stride=2), :] + ref[slot, pl.ds(1, n, stride=2), :]

    def inside(step):
        at = d + step
        return jnp.logical_and(at >= 0, at < gz)

    flag2 = {p: inside(p - 3).astype(F32) for p in range(1, 6)}
    m_first = selection((128, 128), lambda i, j: (i >> 1) == j)
    m_second = selection((128, 128), lambda i, j: (i >> 1) + 64 == j)
    low_half = lane_iota((64, 128)) < 64

    def nb2(ref, p, c):
        z = roll(c + jnp.where(low_half, crow(ref, p + 1, 0, 64), crow(ref, p - 1, 0, 64)), 64)
        return nbxy(ref, p, 0, 64, c, 64) + z

    b1[4, pl.ds(PAD, 128), :] = flo * g0o[0]
    b1[9, pl.ds(PAD, 128), :] = fhi * g0o[1]

    @pl.loop(3, 11)
    def _(z):
        flag = jnp.where(z < 5, flo, jnp.where(z > 8, fhi, 1.0))
        for r in range(0, 128, 64):
            c = crow(b1, z, r, 64)
            nb = nbxy(b1, z, r, 64, c, 128) + (crow(b1, z - 1, r, 64) + crow(b1, z + 1, r, 64))
            a1[z, pl.ds(PAD + r, 64), :] = flag * (12.0 * c + nb)

    @pl.loop(0, 6)
    def _(j):
        for r in range(0, 128, 64):
            out = None
            for dz in range(2):
                z = 1 + 2 * j + dz
                c = crow(a1, z, r, 64)
                nb = nbxy(a1, z, r, 64, c, 128) + (crow(a1, z - 1, r, 64) + crow(a1, z + 1, r, 64))
                q = crow(b1, z, r, 64) + N81 * (nb - 6.0 * c)
                out = q if out is None else out + q
            t1[j, pl.ds(r, 64), :] = 0.5 * out

    for p in range(3):
        b2[2 + p, pl.ds(PAD, 64), :] = flag2[2 + p] * (
            split_dot(ypair(t1, 2 * p, 64), m_first) + split_dot(ypair(t1, 2 * p + 1, 64), m_second)
        )
    for p in range(1, 6):
        c = crow(b2, p, 0, 64)
        a2[p, pl.ds(PAD, 64), :] = flag2[p] * (12.0 * c + nb2(b2, p, c))
    for p in range(1, 6):
        w = crow(a2, p, 0, 64)
        t2[p - 1] = crow(b2, p, 0, 64) + N81 * (nb2(a2, p, w) - 6.0 * w)
    tile = None
    for p in range(1, 5):
        block = lax.rem(d + p - 2 + gz, 4) * 32
        m = selection((128, 128), lambda i, j: ((i & 63) >> 1) + block == j)
        part = split_dot(ypair(t2, p, 32), m)
        tile = part if tile is None else tile + part
    t3[d, pl.ds(0, 32), :] = 0.5 * tile
    m = selection((128, 128), lambda i, j: ((i & 63) >> 1) == (j & 31))
    part = split_dot(ypair(t2, 0, 32), m)
    block8 = lane_iota((8, 128)) // 32
    row = part[0:8]
    for k in range(1, 4):
        row = jnp.where(block8 == k, part[8 * k:8 * k + 8], row)
    t3[d, pl.ds(32, 8), :] = 0.5 * row

    def t3_copy(o):
        to = lax.rem(d + o, gz)
        return remote(t3.at[d], t3.at[d], t3s.at[o], t3r.at[d], gz=to)

    @pl.loop(1, gz)
    def _(o):
        t3_copy(o).start()

    index_copy.wait_recv()
    for far in range(4):
        for side, cond in ((0, even), (1, jnp.logical_not(even))):
            k = far if side == 0 else 3 - far
            if far in (0, 3):
                cond = jnp.logical_and(cond, jnp.logical_not(straight))

            def put_other(ph, value):
                fx[k, ph] = value

            @pl.when(cond)
            def _():
                density(k + 4 * side, pidx2, far % 2, put_other)

        crossing(far, begin, True)

    @pl.when(has_lo)
    def _():
        g0_hi.wait_recv()
        s1[5, pl.ds(PAD, 128), :] += g0[0]

    @pl.when(has_hi)
    def _():
        g0_lo.wait_recv()
        s1[8, pl.ds(PAD, 128), :] += g0[1]

    def w1_plane(z, lo, hi):
        for r in range(0, 128, 64):
            c = crow(s1, z, r, 64)
            t = 12.0 * c + nbxy(s1, z, r, 64, c, 128)
            if lo:
                t = t + crow(s1, z - 1, r, 64)
            if hi:
                t = t + crow(s1, z + 1, r, 64)
            a1[z, pl.ds(PAD + r, 64), :] = t

    for z in range(5, 9):
        w1_plane(z, z > 5, z < 8)
    a1[4, pl.ds(PAD, 128), :] = flo * crow(s1, 5, 0, 128)
    a1[9, pl.ds(PAD, 128), :] = fhi * crow(s1, 8, 0, 128)
    for slot, z in ((0, 5), (3, 8)):
        for r in range(0, 128, 64):
            c = crow(s1, z, r, 64)
            t1[slot, pl.ds(r, 64), :] = (0.5 * N81) * (
                nbxy(s1, z, r, 64, c, 128) - 5.0 * c + crow(a1, z, r, 64)
            )
    for slot in (1, 2):
        for r in range(0, 128, 64):
            out = None
            for z in (3 + 2 * slot, 4 + 2 * slot):
                c = crow(a1, z, r, 64)
                nb = nbxy(a1, z, r, 64, c, 128) + (crow(a1, z - 1, r, 64) + crow(a1, z + 1, r, 64))
                q = crow(s1, z, r, 64) + N81 * (nb - 6.0 * c)
                out = q if out is None else out + q
            t1[slot, pl.ds(r, 64), :] = 0.5 * out

    g1o[0] = split_dot(ypair(t1, 0, 64), m_second)
    g1o[1] = split_dot(ypair(t1, 3, 64), m_first)
    g1_lo, g1_hi = exchange(g1o, g1, g1s, g1r)

    @pl.when(has_lo)
    def _():
        g1_lo.start()

    @pl.when(has_hi)
    def _():
        g1_hi.start()

    s2[3, pl.ds(PAD, 64), :] = split_dot(ypair(t1, 1, 64), m_first) + split_dot(ypair(t1, 2, 64), m_second)

    def h1_copy(i):
        here, there, step = ((5, 9, -1), (5, 1, 1), (5, 13, -2), (8, 0, 2))[i]
        n = 4 if abs(step) == 1 else 1
        to = jnp.clip(d + step, 0, gz - 1)
        return remote(
            s1.at[pl.ds(here, n), pl.ds(PAD, 128), :], s1.at[pl.ds(there, n), pl.ds(PAD, 128), :],
            h1s.at[i], h1r.at[i], gz=to,
        )

    h1_sends = [d >= 1, d <= gz - 2, d >= 2, d <= gz - 3]
    h1_recvs = [d <= gz - 2, d >= 1, d <= gz - 3, d >= 2]

    def h1_start():
        for i in range(4):
            @pl.when(h1_sends[i])
            def _():
                h1_copy(i).start()

    h1_start()

    @pl.when(has_lo)
    def _():
        g1_hi.wait_recv()
        s2[3, pl.ds(PAD, 64), :] += g1[0]

    @pl.when(has_hi)
    def _():
        g1_lo.wait_recv()
        s2[3, pl.ds(PAD, 64), :] += g1[1]

    def h2_copy(i):
        step = (-3, -2, -1, 1, 2, 3)[i]
        to = jnp.clip(d + step, 0, gz - 1)
        return remote(
            s2.at[3, pl.ds(PAD, 64), :], s2.at[3 - step, pl.ds(PAD, 64), :], h2s.at[i], h2r.at[i], gz=to
        )

    for i, step in enumerate((-3, -2, -1, 1, 2, 3)):
        @pl.when(inside(step))
        def _():
            h2_copy(i).start()

    crossing(3, begin, False)

    @pl.loop(1, gz)
    def _(o):
        peer = lax.rem(d + o, gz)
        remote(t3.at[peer], t3.at[peer], t3s.at[o], t3r.at[peer], gz=peer).wait_recv()

    lane32 = lane_iota((32, 128))
    for q in range(4):
        total = None
        for e in range(max(4 * q - 2, 0), min(4 * q + 6, gz)):
            low, high = max(e - 1 - 4 * q, 0), min(e + 2 - 4 * q, 3)
            parts = []
            if low <= high:
                x = t3[e, pl.ds(0, 32), :]
                if (low, high) != (0, 3):
                    x = jnp.where(jnp.logical_and(lane32 >= 32 * low, lane32 < 32 * high + 32), x, 0.0)
                parts.append(x)
            block = e - 2 - 4 * q
            if 0 <= block < 4:
                x = t3[e, pl.ds(32, 8), :]
                pieces = [jnp.where(block8 == block, roll(x, 32 * (block - k)), 0.0) for k in range(4)]
                parts.append(jnp.concatenate(pieces, axis=0))
            for x in parts:
                total = x if total is None else total + x
        s3[q] = total * NINTH
        a3[q, pl.ds(PAD, 32), :] = total * NINTH

    def sweep3(src, dst):
        v = [crow(src, q, 0, 32) for q in range(4)]
        for q in range(4):
            after = v[q + 1] if q < 3 else jnp.zeros_like(v[0])
            before = v[q - 1] if q > 0 else jnp.zeros_like(v[0])
            nz = roll(jnp.where(lane32 < 32, after, v[q]), -32)
            nz = nz + roll(jnp.where(lane32 >= 96, before, v[q]), 32)
            nb = nbxy(src, q, 0, 32, v[q], 32) + nz
            dst[q, pl.ds(PAD, 32), :] = (1.0 / 3.0) * v[q] + (NINTH * nb + s3[q])

    @pl.loop(0, 3)
    def _(i):
        sweep3(a3, b3)
        sweep3(b3, a3)

    sweep3(a3, b3)

    for i, step in enumerate((-3, -2, -1, 1, 2, 3)):
        @pl.when(inside(-step))
        def _():
            h2_copy(i).wait_recv()

    for p in range(1, 6):
        at = d + p - 3
        q = jnp.clip(at // 4, 0, 3)
        block = lax.rem(at + gz, 4) * 32
        m = selection((128, 128), lambda i, j: i == ((j & 63) >> 1) + block)
        e = split_dot(b3[q, pl.ds(PAD, 32), :], m)
        pe2[p - 1, pl.ds(0, 32, stride=2), :] = e
        pe2[p - 1, pl.ds(1, 32, stride=2), :] = e
    for p in range(1, 6):
        c = crow(s2, p, 0, 64)
        w = 12.0 * c + nb2(s2, p, c)
        a2[p, pl.ds(PAD, 64), :] = flag2[p] * (N81 * w + pe2[p - 1])

    def sweep2(src, dst, p):
        c = crow(src, p, 0, 64)
        dst[p, pl.ds(PAD, 64), :] = flag2[p] * (
            (1.0 / 3.0) * c + NINTH * (nb2(src, p, c) + crow(s2, p, 0, 64))
        )

    for p in range(1, 6):
        sweep2(a2, b2, p)
    for p in range(2, 5):
        sweep2(b2, a2, p)

    for i in range(4):
        @pl.when(h1_recvs[i])
        def _():
            h1_copy(i).wait_recv()

    for half in range(2):
        m = selection((128, 128), lambda i, j: i == (j >> 1) + 64 * half)
        for p in range(3):
            e = split_dot(a2[2 + p, pl.ds(PAD, 64), :], m)
            pe1[2 * p + half, pl.ds(0, 64, stride=2), :] = e
            pe1[2 * p + half, pl.ds(1, 64, stride=2), :] = e

    def bounds(first, last, own):
        return jnp.where(has_lo, first, 0), jnp.where(has_hi, last + 1, own)

    lo1, hi1 = bounds(-4, 7, 4)

    @pl.loop(lo1 + 5, hi1 + 5)
    def _(z):
        for r in range(0, 128, 64):
            c = crow(s1, z, r, 64)
            w = 12.0 * c + nbxy(s1, z, r, 64, c, 128) + (crow(s1, z - 1, r, 64) + crow(s1, z + 1, r, 64))
            a1[z, pl.ds(PAD + r, 64), :] = N81 * w + pe1[(z - 1) // 2, pl.ds(r, 64), :]

    def sweep1(src, dst, first, last):
        lo, hi = bounds(first, last, 4)

        @pl.loop(lo + 5, hi + 5)
        def _(z):
            for r in range(0, 128, 64):
                c = crow(src, z, r, 64)
                nb = nbxy(src, z, r, 64, c, 128) + (crow(src, z - 1, r, 64) + crow(src, z + 1, r, 64))
                dst[z, pl.ds(PAD + r, 64), :] = (1.0 / 3.0) * c + NINTH * (nb + crow(s1, z, r, 64))

    sweep1(a1, b1, -3, 6)
    sweep1(b1, a1, -2, 5)

    @pl.when(has_lo)
    def _():
        for far in range(4):
            f_copy(1, far, False).wait_recv()

    @pl.when(has_hi)
    def _():
        for far in range(4):
            f_copy(0, far, False).wait_recv()

    lo0, hi0 = bounds(-3, 10, 8)

    @pl.loop(lo0 + 4, 5)
    def _(z):
        w_plane(z, True, True)

    @pl.loop(11, hi0 + 4)
    def _(z):
        w_plane(z, True, True)

    @pl.loop(lo0 + 4, hi0 + 4)
    def _(z):
        e = a1[z // 2 + 3, pl.ds(PAD, 128), :]
        for ph in range(4):
            a[z, ph, pl.ds(PAD, 128), :] = N81 * a[z, ph, pl.ds(PAD, 128), :] + e

    def sweep0(src, dst, first, last):
        lo, hi = bounds(first, last, 8)

        @pl.loop(lo + 4, hi + 4)
        def _(z):
            for r in range(0, 128, CH):
                c = center(src, z, r, CH)
                nb = nbxy0(src, z, r, CH, c)
                for ph in range(4):
                    t = nb[ph] + (rows(src, z - 1, ph, r, CH) + rows(src, z + 1, ph, r, CH))
                    t = t + rows(f, z, ph, r, CH)
                    dst[z, ph, pl.ds(PAD + r, CH), :] = (1.0 / 3.0) * c[ph] + NINTH * t

    sweep0(a, b, -2, 9)
    sweep0(b, a, -1, 8)

    def final(z, carry):
        squares, products = carry
        for r in range(0, 128, CH):
            c = center(a, z, r, CH)
            nb = nbxy0(a, z, r, CH, c)
            for ph in range(4):
                t = nb[ph] + (rows(a, z - 1, ph, r, CH) + rows(a, z + 1, ph, r, CH))
                src = rows(f, z, ph, r, CH)
                left = (src - 6.0 * c[ph]) + t
                squares = squares + fold(left * left)
                products = products + fold(src * c[ph])
        return squares, products

    zero = jnp.zeros((8, 128), F32)
    squares, products = lax.fori_loop(4, 12, final, (zero, zero))
    sums[d] = jnp.concatenate([squares.sum(axis=0, keepdims=True), products.sum(axis=0, keepdims=True)], axis=0)

    @pl.loop(1, gz)
    def _(o):
        remote(sums.at[d], sums.at[d], ss.at[o], sr.at[d], gz=lax.rem(d + o, gz)).start()

    px[...] = selection((256, 256), lambda i, j: i == (j & 1) * 128 + (j >> 1))

    @pl.loop(0, 8)
    def _(z):
        for yp in range(2):
            x = jnp.concatenate(
                [a[z + 4, 2 * yp, pl.ds(PAD, 128), :], a[z + 4, 2 * yp + 1, pl.ds(PAD, 128), :]], axis=1
            )
            y = split_dot(x, px[...])
            for half in range(2):
                tmp[z % 2, half, pl.ds(yp, 128, stride=2), :] = y[:, 128 * half:128 * half + 128]
        for half in range(2):
            pot[0, z, :, pl.ds(128 * half, 128)] = tmp[z % 2, half]

    @pl.loop(1, gz)
    def _(o):
        peer = lax.rem(d + o, gz)
        remote(sums.at[peer], sums.at[peer], ss.at[o], sr.at[peer], gz=peer).wait_recv()

    total = sums[0]
    for e in range(1, gz):
        total = total + sums[e]
    cells = 1.0 / (gz * 8 * 256 * 256)
    ens[me] = pweight[0] * total[1:]

    @pl.loop(1, pairs)
    def _(o):
        remote(ens.at[me], ens.at[me], es.at[o], er.at[me], pair=lax.rem(me + o, pairs)).start()

    res_out[...] = jnp.sqrt(jnp.sum(total[:1], axis=1, keepdims=True) * cells)

    @pl.loop(1, pairs)
    def _(o):
        peer = lax.rem(me + o, pairs)
        remote(ens.at[peer], ens.at[peer], es.at[o], er.at[peer], pair=peer).wait_recv()

    energy = ens[0]
    for e in range(1, pairs):
        energy = energy + ens[e]
    en_out[...] = jnp.sum(energy, axis=1, keepdims=True) * (-0.5 * cells)

    for cond, side in ((has_lo, 0), (has_hi, 1)):
        @pl.when(cond)
        def _():
            (g0_lo, g0_hi)[side].wait_send()
            (g1_lo, g1_hi)[side].wait_send()

    index_copy.wait_send()
    on_chip(sent)
    for far in range(4):
        crossing(far, sent, True)
    crossing(0, sent, False)
    crossing(3, sent, False)

    for i in range(4):
        @pl.when(h1_sends[i])
        def _():
            h1_copy(i).wait_send()

    for i, step in enumerate((-3, -2, -1, 1, 2, 3)):
        @pl.when(inside(step))
        def _():
            h2_copy(i).wait_send()

    @pl.loop(1, gz)
    def _(o):
        t3_copy(o).wait_send()
        remote(sums.at[d], sums.at[d], ss.at[o], sr.at[d], gz=lax.rem(d + o, gz)).wait_send()

    @pl.loop(1, pairs)
    def _(o):
        remote(ens.at[me], ens.at[me], es.at[o], er.at[me], pair=lax.rem(me + o, pairs)).wait_send()


def solution(mesh):
    gz, pairs = mesh.shape["gz"], mesh.shape["pair"]
    dma, vmem = pltpu.SemaphoreType.DMA, pltpu.VMEM
    field = vmem((16, 4, 144, 128), F32)
    level1, level2, level3 = vmem((14, 144, 128), F32), vmem((7, 80, 128), F32), vmem((4, 48, 128), F32)

    def per_device(orbitals, pair_index, pair_weight):
        potential, norm, energy = pl.pallas_call(
            functools.partial(kernel, gz, pairs),
            out_shape=(
                jax.ShapeDtypeStruct((1, 8, 256, 256), F32),
                jax.ShapeDtypeStruct((1, 1), F32),
                jax.ShapeDtypeStruct((1, 1), F32),
            ),
            in_specs=[
                pl.BlockSpec(memory_space=pltpu.HBM),
                pl.BlockSpec(memory_space=pltpu.HBM),
                pl.BlockSpec(memory_space=pl.ANY),
            ],
            out_specs=(
                pl.BlockSpec(memory_space=pltpu.VMEM),
                pl.BlockSpec(memory_space=pltpu.VMEM),
                pl.BlockSpec(memory_space=pltpu.VMEM),
            ),
            scratch_shapes=[
                *[vmem((8, 256, 256), BF16)] * 8,
                vmem((256, 256), BF16),
                vmem((2, 2, 256, 128), F32),
                pltpu.SMEM((1, 2), jnp.int32),
                pltpu.SMEM((1,), F32),
                pltpu.SMEM((1, 2), jnp.int32),
                vmem((4, 4, 128, 128), F32),
                field, field, field,
                vmem((2, 128, 128), F32), vmem((2, 128, 128), F32),
                level1, level1, level1,
                vmem((6, 128, 128), F32),
                vmem((2, 64, 128), F32), vmem((2, 64, 128), F32),
                vmem((6, 128, 128), F32),
                level2, level2, level2,
                vmem((5, 64, 128), F32),
                vmem((5, 64, 128), F32),
                vmem((gz, 40, 128), F32),
                vmem((4, 32, 128), F32),
                level3, level3,
                vmem((gz, 2, 128), F32),
                vmem((pairs, 1, 128), F32),
                dma((2,)),
                dma((8,)),
                dma((1,)), dma((1,)),
                dma((2, 4)), dma((2, 4)),
                dma((2,)), dma((2,)),
                dma((4,)), dma((4,)),
                dma((2,)), dma((2,)),
                dma((6,)), dma((6,)),
                dma((gz,)), dma((gz,)),
                dma((gz,)), dma((gz,)),
                dma((pairs,)), dma((pairs,)),
            ],
            compiler_params=pltpu.CompilerParams(
                collective_id=0, has_side_effects=True, vmem_limit_bytes=48 * 1024 * 1024
            ),
            name="vcycle",
        )(pair_index, pair_weight, orbitals)
        return potential, norm.reshape(1), energy.reshape(1)

    return jax.shard_map(
        per_device,
        mesh=mesh,
        in_specs=(P(None, "gz", None, None), P("pair", None), P("pair")),
        out_specs=(P("pair", "gz", None, None), P("pair"), P()),
        check_vma=False,
    )
```

```python
import functools

import jax
import jax.numpy as jnp
from jax import lax
from jax.experimental import pallas as pl
from jax.experimental.pallas import tpu as pltpu
from jax.sharding import PartitionSpec as P

MESH = pl.DeviceIdType.MESH
F32, BF16 = jnp.float32, jnp.bfloat16
PAD = 8
EARLY = 0
CH = 32
NINTH = 1.0 / 9.0
N81 = 1.0 / 81.0


def lane_iota(shape):
    return lax.broadcasted_iota(jnp.int32, shape, len(shape) - 1)


def roll(x, shift):
    return pltpu.roll(x, shift % x.shape[-1], x.ndim - 1)


def from_left(x, width=128):
    return jnp.where(lane_iota(x.shape) % width == 0, 0.0, roll(x, 1))


def from_right(x, width=128):
    return jnp.where(lane_iota(x.shape) % width == width - 1, 0.0, roll(x, -1))


def split_dot(x, m):
    hi = x.astype(BF16)
    rest = x - hi.astype(F32)
    mid = rest.astype(BF16)
    low = (rest - mid.astype(F32)).astype(BF16)
    dot = functools.partial(jnp.dot, preferred_element_type=F32)
    return dot(hi, m) + dot(mid, m) + dot(low, m)


def selection(shape, test):
    a = lax.broadcasted_iota(jnp.int32, shape, 0)
    b = lax.broadcasted_iota(jnp.int32, shape, 1)
    return jnp.where(test(a, b), 1.0, 0.0).astype(BF16)


def fold(x):
    return x.reshape(x.shape[0] // 8, 8, x.shape[1]).sum(axis=0)


def rows(ref, z, ph, r, n, dr=0):
    return ref[z, ph, pl.ds(PAD + r + dr, n), :]


def nbxy0(ref, z, r, n, c):
    out = []
    for yp in range(2):
        for xp in range(2):
            side = c[2 * yp + 1 - xp]
            x = side + (from_right(side) if xp else from_left(side))
            other = 2 * (1 - yp) + xp
            y = c[other] + rows(ref, z, other, r, n, 1 if yp else -1)
            out.append(x + y)
    return out


def phase_sums(ref, z, r, n, c):
    total = (c[0] + c[1]) + (c[2] + c[3])
    shifts = from_left(c[1] + c[3]) + from_right(c[0] + c[2])
    shifts = shifts + (rows(ref, z, 2, r, n, -1) + rows(ref, z, 3, r, n, -1))
    shifts = shifts + (rows(ref, z, 0, r, n, 1) + rows(ref, z, 1, r, n, 1))
    return total, shifts


def center(ref, z, r, n):
    return [rows(ref, z, ph, r, n) for ph in range(4)]


def crow(ref, z, r, n, dr=0):
    return ref[z, pl.ds(PAD + r + dr, n), :]


def nbxy(ref, z, r, n, c, width):
    y = crow(ref, z, r, n, -1) + crow(ref, z, r, n, 1)
    return y + (from_left(c, width) + from_right(c, width))


def kernel(
    gz, pairs,
    index_in, weight_in, orbitals, pot, res_out, en_out,
    orb0, orb1, orb2, orb3, orb4, orb5, orb6, orb7, px, mats, tmp, pidx, pweight, pidx2, fx, f, a, b, g0, g0o, s1, a1, b1, t1, g1, g1o, pe1, e1, e1h,
    s2, a2, b2, t2, pe2, t3, s3, a3, b3, sums, ens,
    scalar_sem, orb_sem, ixs, ixr, fs, fr, g0s, g0r, h1s, h1r, g1s, g1r, e1s, e1r, h2s, h2r, t3s, t3r, ss, sr, es, er,
):
    d = lax.axis_index("gz")
    me = lax.axis_index("pair")
    has_lo, has_hi = d > 0, d < gz - 1
    flo, fhi = has_lo.astype(F32), has_hi.astype(F32)

    def remote(src, dst, s_sem, r_sem, **to):
        return pltpu.make_async_remote_copy(
            src_ref=src, dst_ref=dst, send_sem=s_sem, recv_sem=r_sem, device_id=to, device_id_type=MESH
        )

    orb = (orb0, orb1, orb2, orb3, orb4, orb5, orb6, orb7)

    def orb_copy(z):
        return pltpu.make_async_copy(orbitals.at[:, z], orb[z], orb_sem.at[z])

    index_load = pltpu.make_async_copy(index_in, pidx, scalar_sem.at[0])
    weight_load = pltpu.make_async_copy(weight_in, pweight, scalar_sem.at[1])
    index_load.start()
    weight_load.start()
    for z in (0, 7, 1, 6, 2, 5, 3, 4):
        orb_copy(z).start()
    barrier = pltpu.get_barrier_semaphore()

    @pl.loop(1, gz)
    def _(o):
        pl.semaphore_signal(barrier, inc=1, device_id={"gz": lax.rem(d + o, gz)}, device_id_type=MESH)

    @pl.loop(1, pairs)
    def _(o):
        pl.semaphore_signal(barrier, inc=1, device_id={"pair": lax.rem(me + o, pairs)}, device_id_type=MESH)

    other = lax.rem(me + pairs // 2, pairs)
    even = lax.rem(d, 2) == 0
    across = jnp.where(even, d - 1, d + 1)
    has_across = jnp.logical_and(across >= 0, across < gz)

    @pl.when(has_across)
    def _():
        pl.semaphore_signal(barrier, inc=1, device_id={"gz": across, "pair": other}, device_id_type=MESH)

    px[...] = selection((256, 256), lambda i, j: j == (i & 1) * 128 + (i >> 1))
    pad0 = jnp.zeros((4, PAD, 128), F32)
    square = (128, 128)
    mats[0] = selection(square, lambda i, j: (i >> 1) == j)
    mats[1] = selection(square, lambda i, j: (i >> 1) + 64 == j)
    for half in range(2):
        mats[2 + half] = selection(square, lambda i, j: i == (j >> 1) + 64 * half)
    for p in range(5):
        block = lax.rem(d + p - 2 + gz, 4) * 32
        mats[4 + p] = selection(square, lambda i, j: ((i & 63) >> 1) + block == j)
        mats[9 + p] = selection(square, lambda i, j: i == ((j & 63) >> 1) + block)
    mats[14] = selection(square, lambda i, j: ((i & 63) >> 1) == (j & 31))

    @pl.loop(0, 16)
    def _(z):
        for ref in (f, a, b):
            ref[z, :, pl.ds(0, PAD), :] = pad0
            ref[z, :, pl.ds(PAD + 128, PAD), :] = pad0

    def clear_outside(first):
        @pl.loop(first, first + 4)
        def _(z):
            for ref in (f, a, b):
                for ph in range(4):
                    ref[z, ph, pl.ds(PAD, 128), :] = jnp.zeros((128, 128), F32)

        @pl.when(first == 0)
        def _():
            @pl.loop(0, 5)
            def _(z):
                s1[z, pl.ds(PAD, 128), :] = jnp.zeros((128, 128), F32)

        @pl.when(first > 0)
        def _():
            @pl.loop(9, 14)
            def _(z):
                s1[z, pl.ds(PAD, 128), :] = jnp.zeros((128, 128), F32)

    @pl.when(d == 0)
    def _():
        clear_outside(0)
        g0[0] = jnp.zeros((128, 128), F32)
        g1[0] = jnp.zeros((64, 128), F32)

    @pl.when(d == gz - 1)
    def _():
        clear_outside(12)
        g0[1] = jnp.zeros((128, 128), F32)
        g1[1] = jnp.zeros((64, 128), F32)

    @pl.loop(0, 14)
    def _(z):
        s1[z, pl.ds(0, PAD), :] = jnp.zeros((PAD, 128), F32)
        s1[z, pl.ds(PAD + 128, PAD), :] = jnp.zeros((PAD, 128), F32)
        a1[z] = jnp.zeros((144, 128), F32)
        b1[z] = jnp.zeros((144, 128), F32)

    @pl.loop(0, 7)
    def _(p):
        s2[p, pl.ds(0, PAD), :] = jnp.zeros((PAD, 128), F32)
        s2[p, pl.ds(PAD + 64, PAD), :] = jnp.zeros((PAD, 128), F32)
        a2[p] = jnp.zeros((80, 128), F32)
        b2[p] = jnp.zeros((80, 128), F32)
        at = d + p - 3

        @pl.when(jnp.logical_or(jnp.logical_or(at < 0, at >= gz), jnp.logical_or(p == 0, p == 6)))
        def _():
            s2[p, pl.ds(PAD, 64), :] = jnp.zeros((64, 128), F32)

    for q in range(4):
        a3[q] = jnp.zeros((48, 128), F32)
        b3[q] = jnp.zeros((48, 128), F32)

    def density(z, which, slot, put):
        left = jnp.dot(orb[z][which[0, 0]], px[...], preferred_element_type=F32)
        right = jnp.dot(orb[z][which[0, 1]], px[...], preferred_element_type=F32)
        both = left * right
        tmp[slot, 0] = both[:, :128]
        tmp[slot, 1] = both[:, 128:]
        for yp in range(2):
            for xp in range(2):
                put(2 * yp + xp, tmp[slot, xp, pl.ds(yp, 128, stride=2), :])

    index_load.wait()
    weight_load.wait()
    for i, z in enumerate((0, 7, 1, 6, 2, 5, 3, 4)):
        orb_copy(z).wait()

        def put(ph, value):
            f[z + 4, ph, pl.ds(PAD, 128), :] = value

        density(z, pidx, i % 2, put)

    def w_plane(z, lo, hi):
        for r in range(0, 128, CH):
            c = center(f, z, r, CH)
            nb = nbxy0(f, z, r, CH, c)
            for ph in range(4):
                t = 12.0 * c[ph] + nb[ph]
                if lo:
                    t = t + rows(f, z - 1, ph, r, CH)
                if hi:
                    t = t + rows(f, z + 1, ph, r, CH)
                a[z, ph, pl.ds(PAD + r, CH), :] = t

    w_plane(4, False, True)
    w_plane(11, True, False)

    pl.semaphore_wait(barrier, gz - 1 + pairs - 1 + has_across.astype(jnp.int32))

    index_copy = remote(pidx, pidx2, ixs.at[0], ixr.at[0], pair=other)
    index_copy.start()

    for side, z in ((0, 4), (1, 11)):
        for r in range(0, 128, CH):
            total, shifts = phase_sums(f, z, r, CH, center(f, z, r, CH))
            w = center(a, z, r, CH)
            g0o[side, pl.ds(r, CH), :] = (0.5 * N81) * (
                shifts - 3.0 * total + ((w[0] + w[1]) + (w[2] + w[3]))
            )

    def exchange(out, landed, s_sems, r_sems):
        lo = remote(out.at[0], landed.at[1], s_sems.at[0], r_sems.at[1], gz=jnp.maximum(d - 1, 0))
        hi = remote(out.at[1], landed.at[0], s_sems.at[1], r_sems.at[0], gz=jnp.minimum(d + 1, gz - 1))
        return lo, hi

    g0_lo, g0_hi = exchange(g0o, g0, g0s, g0r)

    @pl.when(has_lo)
    def _():
        g0_lo.start()

    @pl.when(has_hi)
    def _():
        g0_hi.start()

    turn = lax.rem(d, 4)
    straight = jnp.logical_or(turn == 1, turn == 2)
    diagonal = jnp.logical_not(straight)

    def f_copy(side, far, of_other):
        k = far if side == 0 else 3 - far
        here = k if side == 0 else 4 + k
        there = 12 + k if side == 0 else k
        to = jnp.maximum(d - 1, 0) if side == 0 else jnp.minimum(d + 1, gz - 1)
        landed = f.at[there, :, pl.ds(PAD, 128), :]
        if of_other:
            return remote(fx.at[k], landed, fs.at[side, far], fr.at[1 - side, far], gz=to, pair=other)
        return remote(
            f.at[4 + here, :, pl.ds(PAD, 128), :], landed, fs.at[side, far], fr.at[1 - side, far], gz=to, pair=me
        )

    def on_chip(act):
        for side, cond in ((0, jnp.logical_not(even)), (1, even)):
            @pl.when(cond)
            def _():
                for far in range(4):
                    act(side, far, False)

    def crossing(far, act, of_other, only=True):
        for side, cond in ((0, jnp.logical_and(even, has_lo)), (1, jnp.logical_and(jnp.logical_not(even), has_hi))):
            cond = jnp.logical_and(cond, only)
            if far == 0:
                cond = jnp.logical_and(cond, straight if of_other else diagonal)
            elif not of_other:
                continue

            @pl.when(cond)
            def _():
                act(side, far, of_other)

    def begin(side, far, of_other):
        f_copy(side, far, of_other).start()

    def sent(side, far, of_other):
        f_copy(side, far, of_other).wait_send()

    crossing(0, begin, False)
    on_chip(begin)

    @pl.loop(5, 11)
    def _(z):
        w_plane(z, True, True)

    for ph in range(4):
        a[3, ph, pl.ds(PAD, 128), :] = flo * f[4, ph, pl.ds(PAD, 128), :]
        a[12, ph, pl.ds(PAD, 128), :] = fhi * f[11, ph, pl.ds(PAD, 128), :]

    @pl.loop(0, 4)
    def _(j):
        for r in range(0, 128, CH):
            out = None
            for dz in range(2):
                z = 4 + 2 * j + dz
                c = center(a, z, r, CH)
                total, shifts = phase_sums(a, z, r, CH, c)
                below, above, src = center(a, z - 1, r, CH), center(a, z + 1, r, CH), center(f, z, r, CH)
                zs = ((below[0] + below[1]) + (below[2] + below[3])) + (
                    (above[0] + above[1]) + (above[2] + above[3])
                )
                q = ((src[0] + src[1]) + (src[2] + src[3])) + N81 * (zs - 4.0 * total + shifts)
                out = q if out is None else out + q
            s1[5 + j, pl.ds(PAD + r, CH), :] = 0.5 * out
            b1[5 + j, pl.ds(PAD + r, CH), :] = 0.5 * out

    def ypair(ref, slot, n):
        return ref[slot, pl.ds(0, n, stride=2), :] + ref[slot, pl.ds(1, n, stride=2), :]

    def inside(step):
        at = d + step
        return jnp.logical_and(at >= 0, at < gz)

    flag2 = {p: inside(p - 3).astype(F32) for p in range(1, 6)}
    m_first, m_second = mats[0], mats[1]
    low_half = lane_iota((64, 128)) < 64

    def nb2(ref, p, c):
        z = roll(c + jnp.where(low_half, crow(ref, p + 1, 0, 64), crow(ref, p - 1, 0, 64)), 64)
        return nbxy(ref, p, 0, 64, c, 64) + z

    b1[4, pl.ds(PAD, 128), :] = flo * g0o[0]
    b1[9, pl.ds(PAD, 128), :] = fhi * g0o[1]

    @pl.loop(3, 11, unroll=4)
    def _(z):
        flag = jnp.where(z < 5, flo, jnp.where(z > 8, fhi, 1.0))
        for r in range(0, 128, 64):
            c = crow(b1, z, r, 64)
            nb = nbxy(b1, z, r, 64, c, 128) + (crow(b1, z - 1, r, 64) + crow(b1, z + 1, r, 64))
            a1[z, pl.ds(PAD + r, 64), :] = flag * (12.0 * c + nb)

    @pl.loop(0, 6, unroll=2)
    def _(j):
        for r in range(0, 128, 64):
            out = None
            for dz in range(2):
                z = 1 + 2 * j + dz
                c = crow(a1, z, r, 64)
                nb = nbxy(a1, z, r, 64, c, 128) + (crow(a1, z - 1, r, 64) + crow(a1, z + 1, r, 64))
                q = crow(b1, z, r, 64) + N81 * (nb - 6.0 * c)
                out = q if out is None else out + q
            t1[j, pl.ds(r, 64), :] = 0.5 * out

    for p in range(3):
        b2[2 + p, pl.ds(PAD, 64), :] = flag2[2 + p] * (
            split_dot(ypair(t1, 2 * p, 64), m_first) + split_dot(ypair(t1, 2 * p + 1, 64), m_second)
        )
    for p in range(1, 6):
        c = crow(b2, p, 0, 64)
        a2[p, pl.ds(PAD, 64), :] = flag2[p] * (12.0 * c + nb2(b2, p, c))
    for p in range(1, 6):
        w = crow(a2, p, 0, 64)
        t2[p - 1] = crow(b2, p, 0, 64) + N81 * (nb2(a2, p, w) - 6.0 * w)
    tile = None
    for p in range(1, 5):
        part = split_dot(ypair(t2, p, 32), mats[4 + p])
        tile = part if tile is None else tile + part
    t3[d, pl.ds(0, 32), :] = 0.5 * tile
    part = split_dot(ypair(t2, 0, 32), mats[14])
    block8 = lane_iota((8, 128)) // 32
    row = part[0:8]
    for k in range(1, 4):
        row = jnp.where(block8 == k, part[8 * k:8 * k + 8], row)
    t3[d, pl.ds(32, 8), :] = 0.5 * row

    def t3_copy(o):
        to = lax.rem(d + o, gz)
        return remote(t3.at[d], t3.at[d], t3s.at[o], t3r.at[d], gz=to)

    @pl.loop(1, gz)
    def _(o):
        t3_copy(o).start()

    index_copy.wait_recv()
    for far in range(4):
        for side, cond in ((0, even), (1, jnp.logical_not(even))):
            k = far if side == 0 else 3 - far
            if far == 0:
                cond = jnp.logical_and(cond, straight)

            def put_other(ph, value):
                fx[k, ph] = value

            @pl.when(cond)
            def _():
                density(k + 4 * side, pidx2, far % 2, put_other)

        crossing(far, begin, True, straight if far > EARLY else True)

    @pl.when(has_lo)
    def _():
        g0_hi.wait_recv()
        s1[5, pl.ds(PAD, 128), :] += g0[0]

    @pl.when(has_hi)
    def _():
        g0_lo.wait_recv()
        s1[8, pl.ds(PAD, 128), :] += g0[1]

    def w1_plane(z, lo, hi):
        for r in range(0, 128, 64):
            c = crow(s1, z, r, 64)
            t = 12.0 * c + nbxy(s1, z, r, 64, c, 128)
            if lo:
                t = t + crow(s1, z - 1, r, 64)
            if hi:
                t = t + crow(s1, z + 1, r, 64)
            a1[z, pl.ds(PAD + r, 64), :] = t

    for z in range(5, 9):
        w1_plane(z, z > 5, z < 8)
    a1[4, pl.ds(PAD, 128), :] = flo * crow(s1, 5, 0, 128)
    a1[9, pl.ds(PAD, 128), :] = fhi * crow(s1, 8, 0, 128)
    for slot, z in ((0, 5), (3, 8)):
        for r in range(0, 128, 64):
            c = crow(s1, z, r, 64)
            t1[slot, pl.ds(r, 64), :] = (0.5 * N81) * (
                nbxy(s1, z, r, 64, c, 128) - 5.0 * c + crow(a1, z, r, 64)
            )
    for slot in (1, 2):
        for r in range(0, 128, 64):
            out = None
            for z in (3 + 2 * slot, 4 + 2 * slot):
                c = crow(a1, z, r, 64)
                nb = nbxy(a1, z, r, 64, c, 128) + (crow(a1, z - 1, r, 64) + crow(a1, z + 1, r, 64))
                q = crow(s1, z, r, 64) + N81 * (nb - 6.0 * c)
                out = q if out is None else out + q
            t1[slot, pl.ds(r, 64), :] = 0.5 * out

    g1o[0] = split_dot(ypair(t1, 0, 64), m_second)
    g1o[1] = split_dot(ypair(t1, 3, 64), m_first)
    g1_lo, g1_hi = exchange(g1o, g1, g1s, g1r)

    @pl.when(has_lo)
    def _():
        g1_lo.start()

    @pl.when(has_hi)
    def _():
        g1_hi.start()

    s2[3, pl.ds(PAD, 64), :] = split_dot(ypair(t1, 1, 64), m_first) + split_dot(ypair(t1, 2, 64), m_second)

    def h1_copy(i):
        here, there, step = ((5, 9, -1), (6, 2, 1))[i]
        to = jnp.clip(d + step, 0, gz - 1)
        return remote(
            s1.at[pl.ds(here, 3), pl.ds(PAD, 128), :], s1.at[pl.ds(there, 3), pl.ds(PAD, 128), :],
            h1s.at[i], h1r.at[i], gz=to,
        )

    h1_sends, h1_recvs = [has_lo, has_hi], [has_hi, has_lo]

    def h1_start():
        for i in range(2):
            @pl.when(h1_sends[i])
            def _():
                h1_copy(i).start()

    h1_start()

    @pl.when(has_lo)
    def _():
        g1_hi.wait_recv()
        s2[3, pl.ds(PAD, 64), :] += g1[0]

    @pl.when(has_hi)
    def _():
        g1_lo.wait_recv()
        s2[3, pl.ds(PAD, 64), :] += g1[1]

    def h2_copy(i):
        step = (-2, -1, 1, 2)[i]
        to = jnp.clip(d + step, 0, gz - 1)
        return remote(
            s2.at[3, pl.ds(PAD, 64), :], s2.at[3 - step, pl.ds(PAD, 64), :], h2s.at[i], h2r.at[i], gz=to
        )

    for i, step in enumerate((-2, -1, 1, 2)):
        @pl.when(inside(step))
        def _():
            h2_copy(i).start()


    @pl.loop(1, gz)
    def _(o):
        peer = lax.rem(d + o, gz)
        remote(t3.at[peer], t3.at[peer], t3s.at[o], t3r.at[peer], gz=peer).wait_recv()

    for far in range(EARLY + 1, 4):
        crossing(far, begin, True, diagonal)

    lane32 = lane_iota((32, 128))
    for q in range(4):
        total = None
        for e in range(max(4 * q - 2, 0), min(4 * q + 6, gz)):
            low, high = max(e - 1 - 4 * q, 0), min(e + 2 - 4 * q, 3)
            parts = []
            if low <= high:
                x = t3[e, pl.ds(0, 32), :]
                if (low, high) != (0, 3):
                    x = jnp.where(jnp.logical_and(lane32 >= 32 * low, lane32 < 32 * high + 32), x, 0.0)
                parts.append(x)
            block = e - 2 - 4 * q
            if 0 <= block < 4:
                x = t3[e, pl.ds(32, 8), :]
                pieces = [jnp.where(block8 == block, roll(x, 32 * (block - k)), 0.0) for k in range(4)]
                parts.append(jnp.concatenate(pieces, axis=0))
            for x in parts:
                total = x if total is None else total + x
        s3[q] = total * NINTH
        a3[q, pl.ds(PAD, 32), :] = total * NINTH

    def sweep3(src, dst):
        v = [crow(src, q, 0, 32) for q in range(4)]
        for q in range(4):
            after = v[q + 1] if q < 3 else jnp.zeros_like(v[0])
            before = v[q - 1] if q > 0 else jnp.zeros_like(v[0])
            nz = roll(jnp.where(lane32 < 32, after, v[q]), -32)
            nz = nz + roll(jnp.where(lane32 >= 96, before, v[q]), 32)
            nb = nbxy(src, q, 0, 32, v[q], 32) + nz
            dst[q, pl.ds(PAD, 32), :] = (1.0 / 3.0) * v[q] + (NINTH * nb + s3[q])

    @pl.loop(0, 3)
    def _(i):
        sweep3(a3, b3)
        sweep3(b3, a3)

    sweep3(a3, b3)

    for i, step in enumerate((-2, -1, 1, 2)):
        @pl.when(inside(-step))
        def _():
            h2_copy(i).wait_recv()

    for p in range(1, 6):
        at = d + p - 3
        q = jnp.clip(at // 4, 0, 3)
        e = split_dot(b3[q, pl.ds(PAD, 32), :], mats[8 + p])
        pe2[p - 1, pl.ds(0, 32, stride=2), :] = e
        pe2[p - 1, pl.ds(1, 32, stride=2), :] = e
    for p in range(1, 6):
        c = crow(s2, p, 0, 64)
        w = 12.0 * c + nb2(s2, p, c)
        a2[p, pl.ds(PAD, 64), :] = flag2[p] * (N81 * w + pe2[p - 1])

    def sweep2(src, dst, p):
        c = crow(src, p, 0, 64)
        dst[p, pl.ds(PAD, 64), :] = flag2[p] * (
            (1.0 / 3.0) * c + NINTH * (nb2(src, p, c) + crow(s2, p, 0, 64))
        )

    for p in range(2, 5):
        sweep2(a2, b2, p)
    for p in range(2, 5):
        sweep2(b2, a2, p)

    for i in range(2):
        @pl.when(h1_recvs[i])
        def _():
            h1_copy(i).wait_recv()

    for j in range(1, 5):
        e = split_dot(a2[2 + j // 2, pl.ds(PAD, 64), :], mats[2 + j % 2])
        pe1[j, pl.ds(0, 64, stride=2), :] = e
        pe1[j, pl.ds(1, 64, stride=2), :] = e

    def in_grid(z):
        return jnp.where(z < 5, flo, jnp.where(z > 8, fhi, 1.0))

    def nb1(ref, z, r, c):
        return nbxy(ref, z, r, 64, c, 128) + (crow(ref, z - 1, r, 64) + crow(ref, z + 1, r, 64))

    @pl.loop(3, 11, unroll=4)
    def _(z):
        flag = in_grid(z)
        for r in range(0, 128, 64):
            c = crow(s1, z, r, 64)
            w = 12.0 * c + nb1(s1, z, r, c)
            a1[z, pl.ds(PAD + r, 64), :] = flag * (N81 * w + pe1[(z - 1) // 2, pl.ds(r, 64), :])

    @pl.loop(4, 10, unroll=3)
    def _(z):
        flag = in_grid(z)
        for r in range(0, 128, 64):
            c = crow(a1, z, r, 64)
            t = nb1(a1, z, r, c) + crow(s1, z, r, 64)
            b1[z, pl.ds(PAD + r, 64), :] = flag * ((1.0 / 3.0) * c + NINTH * t)

    @pl.loop(5, 9, unroll=4)
    def _(z):
        for r in range(0, 128, 64):
            c = crow(b1, z, r, 64)
            t = nb1(b1, z, r, c) + crow(s1, z, r, 64)
            e1[z - 5, pl.ds(r, 64), :] = (1.0 / 3.0) * c + NINTH * t

    e1_lo = remote(
        e1.at[pl.ds(0, 2)], e1h.at[1], e1s.at[0], e1r.at[1], gz=jnp.maximum(d - 1, 0)
    )
    e1_hi = remote(
        e1.at[pl.ds(2, 2)], e1h.at[0], e1s.at[1], e1r.at[0], gz=jnp.minimum(d + 1, gz - 1)
    )

    @pl.when(has_lo)
    def _():
        e1_lo.start()

    @pl.when(has_hi)
    def _():
        e1_hi.start()

    def f_wait(*which):
        @pl.when(has_lo)
        def _():
            for far in which:
                f_copy(1, far, False).wait_recv()

        @pl.when(has_hi)
        def _():
            for far in which:
                f_copy(0, far, False).wait_recv()

    def correct(z, ref, k):
        e = ref[k]
        for ph in range(4):
            a[z, ph, pl.ds(PAD, 128), :] = N81 * a[z, ph, pl.ds(PAD, 128), :] + e

    def sweep0(src, dst, first, last):
        @pl.loop(first + 4, last + 5)
        def _(z):
            for r in range(0, 128, CH):
                c = center(src, z, r, CH)
                nb = nbxy0(src, z, r, CH, c)
                for ph in range(4):
                    t = nb[ph] + (rows(src, z - 1, ph, r, CH) + rows(src, z + 1, ph, r, CH))
                    t = t + rows(f, z, ph, r, CH)
                    dst[z, ph, pl.ds(PAD + r, CH), :] = (1.0 / 3.0) * c[ph] + NINTH * t

    def below(first):
        return jnp.where(has_lo, first, 0)

    def above(last):
        return jnp.where(has_hi, last, 7)

    f_wait(0)
    w_plane(4, True, True)
    w_plane(11, True, True)

    @pl.loop(0, 8)
    def _(z):
        correct(z + 4, e1, z // 2)

    sweep0(a, b, 1, 6)
    sweep0(b, a, 2, 5)

    f_wait(1, 2, 3)

    @pl.loop(below(-3) + 4, 4)
    def _(z):
        w_plane(z, True, True)

    @pl.loop(12, above(10) + 5)
    def _(z):
        w_plane(z, True, True)

    @pl.when(has_lo)
    def _():
        e1_hi.wait_recv()
        for z in range(-3, 0):
            correct(z + 4, e1h.at[0], (z + 4) // 2)

    @pl.when(has_hi)
    def _():
        e1_lo.wait_recv()
        for z in range(8, 11):
            correct(z + 4, e1h.at[1], (z - 8) // 2)

    sweep0(a, b, below(-2), 0)
    sweep0(a, b, 7, above(9))
    sweep0(b, a, below(-1), 1)
    sweep0(b, a, 6, above(8))

    def final(z, carry):
        squares, products = carry
        for r in range(0, 128, CH):
            c = center(a, z, r, CH)
            nb = nbxy0(a, z, r, CH, c)
            for ph in range(4):
                t = nb[ph] + (rows(a, z - 1, ph, r, CH) + rows(a, z + 1, ph, r, CH))
                src = rows(f, z, ph, r, CH)
                left = (src - 6.0 * c[ph]) + t
                squares = squares + fold(left * left)
                products = products + fold(src * c[ph])
        return squares, products

    zero = jnp.zeros((8, 128), F32)
    squares, products = lax.fori_loop(4, 12, final, (zero, zero))
    sums[d] = jnp.concatenate([squares.sum(axis=0, keepdims=True), products.sum(axis=0, keepdims=True)], axis=0)

    @pl.loop(1, gz)
    def _(o):
        remote(sums.at[d], sums.at[d], ss.at[o], sr.at[d], gz=lax.rem(d + o, gz)).start()

    px[...] = selection((256, 256), lambda i, j: i == (j & 1) * 128 + (j >> 1))

    @pl.loop(0, 8)
    def _(z):
        for yp in range(2):
            x = jnp.concatenate(
                [a[z + 4, 2 * yp, pl.ds(PAD, 128), :], a[z + 4, 2 * yp + 1, pl.ds(PAD, 128), :]], axis=1
            )
            y = split_dot(x, px[...])
            for half in range(2):
                tmp[z % 2, half, pl.ds(yp, 128, stride=2), :] = y[:, 128 * half:128 * half + 128]
        for half in range(2):
            pot[0, z, :, pl.ds(128 * half, 128)] = tmp[z % 2, half]

    @pl.loop(1, gz)
    def _(o):
        peer = lax.rem(d + o, gz)
        remote(sums.at[peer], sums.at[peer], ss.at[o], sr.at[peer], gz=peer).wait_recv()

    total = sums[0]
    for e in range(1, gz):
        total = total + sums[e]
    cells = 1.0 / (gz * 8 * 256 * 256)
    ens[me] = pweight[0, 0] * total[1:]

    @pl.loop(1, pairs)
    def _(o):
        remote(ens.at[me], ens.at[me], es.at[o], er.at[me], pair=lax.rem(me + o, pairs)).start()

    res_out[...] = jnp.sqrt(jnp.sum(total[:1], axis=1, keepdims=True) * cells)

    @pl.loop(1, pairs)
    def _(o):
        peer = lax.rem(me + o, pairs)
        remote(ens.at[peer], ens.at[peer], es.at[o], er.at[peer], pair=peer).wait_recv()

    energy = ens[0]
    for e in range(1, pairs):
        energy = energy + ens[e]
    en_out[...] = jnp.sum(energy, axis=1, keepdims=True) * (-0.5 * cells)

    for cond, side in ((has_lo, 0), (has_hi, 1)):
        @pl.when(cond)
        def _():
            (g0_lo, g0_hi)[side].wait_send()
            (g1_lo, g1_hi)[side].wait_send()
            (e1_lo, e1_hi)[side].wait_send()

    index_copy.wait_send()
    on_chip(sent)
    for far in range(4):
        crossing(far, sent, True)
    crossing(0, sent, False)

    for i in range(2):
        @pl.when(h1_sends[i])
        def _():
            h1_copy(i).wait_send()

    for i, step in enumerate((-2, -1, 1, 2)):
        @pl.when(inside(step))
        def _():
            h2_copy(i).wait_send()

    @pl.loop(1, gz)
    def _(o):
        t3_copy(o).wait_send()
        remote(sums.at[d], sums.at[d], ss.at[o], sr.at[d], gz=lax.rem(d + o, gz)).wait_send()

    @pl.loop(1, pairs)
    def _(o):
        remote(ens.at[me], ens.at[me], es.at[o], er.at[me], pair=lax.rem(me + o, pairs)).wait_send()


def solution(mesh):
    gz, pairs = mesh.shape["gz"], mesh.shape["pair"]
    dma, vmem = pltpu.SemaphoreType.DMA, pltpu.VMEM
    field = vmem((16, 4, 144, 128), F32)
    level1, level2, level3 = vmem((14, 144, 128), F32), vmem((7, 80, 128), F32), vmem((4, 48, 128), F32)

    def per_device(orbitals, pair_index, pair_weight):
        potential, norm, energy = pl.pallas_call(
            functools.partial(kernel, gz, pairs),
            out_shape=(
                jax.ShapeDtypeStruct((1, 8, 256, 256), F32),
                jax.ShapeDtypeStruct((1, 1), F32),
                jax.ShapeDtypeStruct((1, 1), F32),
            ),
            in_specs=[
                pl.BlockSpec(memory_space=pltpu.HBM),
                pl.BlockSpec(memory_space=pltpu.HBM),
                pl.BlockSpec(memory_space=pl.ANY),
            ],
            out_specs=(
                pl.BlockSpec(memory_space=pltpu.VMEM),
                pl.BlockSpec(memory_space=pltpu.VMEM),
                pl.BlockSpec(memory_space=pltpu.VMEM),
            ),
            scratch_shapes=[
                *[vmem((8, 256, 256), BF16)] * 8,
                vmem((256, 256), BF16),
                vmem((15, 128, 128), BF16),
                vmem((2, 2, 256, 128), F32),
                pltpu.SMEM((1, 2), jnp.int32),
                pltpu.SMEM((1, 1), F32),
                pltpu.SMEM((1, 2), jnp.int32),
                vmem((4, 4, 128, 128), F32),
                field, field, field,
                vmem((2, 128, 128), F32), vmem((2, 128, 128), F32),
                level1, level1, level1,
                vmem((6, 128, 128), F32),
                vmem((2, 64, 128), F32), vmem((2, 64, 128), F32),
                vmem((6, 128, 128), F32),
                vmem((4, 128, 128), F32), vmem((2, 2, 128, 128), F32),
                level2, level2, level2,
                vmem((5, 64, 128), F32),
                vmem((5, 64, 128), F32),
                vmem((gz, 40, 128), F32),
                vmem((4, 32, 128), F32),
                level3, level3,
                vmem((gz, 2, 128), F32),
                vmem((pairs, 1, 128), F32),
                dma((2,)),
                dma((8,)),
                dma((1,)), dma((1,)),
                dma((2, 4)), dma((2, 4)),
                dma((2,)), dma((2,)),
                dma((2,)), dma((2,)),
                dma((2,)), dma((2,)),
                dma((2,)), dma((2,)),
                dma((4,)), dma((4,)),
                dma((gz,)), dma((gz,)),
                dma((gz,)), dma((gz,)),
                dma((pairs,)), dma((pairs,)),
            ],
            compiler_params=pltpu.CompilerParams(
                collective_id=0, has_side_effects=True, vmem_limit_bytes=48 * 1024 * 1024
            ),
            name="vcycle",
        )(pltpu.with_memory_space_constraint(pair_index, pltpu.HBM), pair_weight.reshape(1, 1), orbitals)
        return potential, norm.reshape(1), energy.reshape(1)

    return jax.shard_map(
        per_device,
        mesh=mesh,
        in_specs=(P(None, "gz", None, None), P("pair", None), P("pair")),
        out_specs=(P("pair", "gz", None, None), P("pair"), P()),
        check_vma=False,
    )
```

```python
import functools

import jax
import jax.numpy as jnp
from jax import lax
from jax.experimental import pallas as pl
from jax.experimental.pallas import tpu as pltpu
from jax.sharding import PartitionSpec as P

MESH = pl.DeviceIdType.MESH
F32, BF16 = jnp.float32, jnp.bfloat16
PAD = 8
EARLY = 1
CH = 32
NINTH = 1.0 / 9.0
N81 = 1.0 / 81.0


def lane_iota(shape):
    return lax.broadcasted_iota(jnp.int32, shape, len(shape) - 1)


def roll(x, shift):
    return pltpu.roll(x, shift % x.shape[-1], x.ndim - 1)


def from_left(x, width=128):
    return jnp.where(lane_iota(x.shape) % width == 0, 0.0, roll(x, 1))


def from_right(x, width=128):
    return jnp.where(lane_iota(x.shape) % width == width - 1, 0.0, roll(x, -1))


def split_dot(x, m):
    hi = x.astype(BF16)
    rest = x - hi.astype(F32)
    mid = rest.astype(BF16)
    low = (rest - mid.astype(F32)).astype(BF16)
    dot = functools.partial(jnp.dot, preferred_element_type=F32)
    return dot(hi, m) + dot(mid, m) + dot(low, m)


def selection(shape, test):
    a = lax.broadcasted_iota(jnp.int32, shape, 0)
    b = lax.broadcasted_iota(jnp.int32, shape, 1)
    return jnp.where(test(a, b), 1.0, 0.0).astype(BF16)


def fold(x):
    return x.reshape(x.shape[0] // 8, 8, x.shape[1]).sum(axis=0)


def rows(ref, z, ph, r, n, dr=0):
    return ref[z, ph, pl.ds(PAD + r + dr, n), :]


def nbxy0(ref, z, r, n, c):
    out = []
    for yp in range(2):
        for xp in range(2):
            side = c[2 * yp + 1 - xp]
            x = side + (from_right(side) if xp else from_left(side))
            other = 2 * (1 - yp) + xp
            y = c[other] + rows(ref, z, other, r, n, 1 if yp else -1)
            out.append(x + y)
    return out


def phase_sums(ref, z, r, n, c):
    total = (c[0] + c[1]) + (c[2] + c[3])
    shifts = from_left(c[1] + c[3]) + from_right(c[0] + c[2])
    shifts = shifts + (rows(ref, z, 2, r, n, -1) + rows(ref, z, 3, r, n, -1))
    shifts = shifts + (rows(ref, z, 0, r, n, 1) + rows(ref, z, 1, r, n, 1))
    return total, shifts


def center(ref, z, r, n):
    return [rows(ref, z, ph, r, n) for ph in range(4)]


def crow(ref, z, r, n, dr=0):
    return ref[z, pl.ds(PAD + r + dr, n), :]


def nbxy(ref, z, r, n, c, width):
    y = crow(ref, z, r, n, -1) + crow(ref, z, r, n, 1)
    return y + (from_left(c, width) + from_right(c, width))


def kernel(
    gz, pairs,
    index_in, weight_in, orbitals, pot, res_out, en_out,
    orb0, orb1, orb2, orb3, orb4, orb5, orb6, orb7, px, mats, tmp, pidx, pweight, pidx2, fx, f, a, b, g0, g0o, s1, a1, b1, t1, g1, g1o, pe1, e1, e1h,
    s2, a2, b2, t2, pe2, t3, s3, a3, b3, prods, sums, ens,
    scalar_sem, orb_sem, ixs, ixr, fs, fr, g0s, g0r, h1s, h1r, g1s, g1r, e1s, e1r, h2s, h2r, t3s, t3r, ps, pr, ss, sr, es, er,
):
    d = lax.axis_index("gz")
    me = lax.axis_index("pair")
    has_lo, has_hi = d > 0, d < gz - 1
    flo, fhi = has_lo.astype(F32), has_hi.astype(F32)

    def remote(src, dst, s_sem, r_sem, **to):
        return pltpu.make_async_remote_copy(
            src_ref=src, dst_ref=dst, send_sem=s_sem, recv_sem=r_sem, device_id=to, device_id_type=MESH
        )

    orb = (orb0, orb1, orb2, orb3, orb4, orb5, orb6, orb7)

    def orb_copy(z):
        return pltpu.make_async_copy(orbitals.at[:, z], orb[z], orb_sem.at[z])

    index_load = pltpu.make_async_copy(index_in, pidx, scalar_sem.at[0])
    weight_load = pltpu.make_async_copy(weight_in, pweight, scalar_sem.at[1])
    index_load.start()
    weight_load.start()
    for z in (0, 7, 1, 6, 2, 5, 3, 4):
        orb_copy(z).start()
    barrier = pltpu.get_barrier_semaphore()

    @pl.loop(1, gz)
    def _(o):
        pl.semaphore_signal(barrier, inc=1, device_id={"gz": lax.rem(d + o, gz)}, device_id_type=MESH)

    @pl.loop(1, pairs)
    def _(o):
        pl.semaphore_signal(barrier, inc=1, device_id={"pair": lax.rem(me + o, pairs)}, device_id_type=MESH)

    other = lax.rem(me + pairs // 2, pairs)
    even = lax.rem(d, 2) == 0
    across = jnp.where(even, d - 1, d + 1)
    has_across = jnp.logical_and(across >= 0, across < gz)

    @pl.when(has_across)
    def _():
        pl.semaphore_signal(barrier, inc=1, device_id={"gz": across, "pair": other}, device_id_type=MESH)

    px[...] = selection((256, 256), lambda i, j: j == (i & 1) * 128 + (i >> 1))
    pad0 = jnp.zeros((4, PAD, 128), F32)
    square = (128, 128)
    mats[0] = selection(square, lambda i, j: (i >> 1) == j)
    mats[1] = selection(square, lambda i, j: (i >> 1) + 64 == j)
    for half in range(2):
        mats[2 + half] = selection(square, lambda i, j: i == (j >> 1) + 64 * half)
    for p in range(5):
        block = lax.rem(d + p - 2 + gz, 4) * 32
        mats[4 + p] = selection(square, lambda i, j: ((i & 63) >> 1) + block == j)
        mats[9 + p] = selection(square, lambda i, j: i == ((j & 63) >> 1) + block)
    mats[14] = selection(square, lambda i, j: ((i & 63) >> 1) == (j & 31))

    @pl.loop(0, 16)
    def _(z):
        for ref in (f, a, b):
            ref[z, :, pl.ds(0, PAD), :] = pad0
            ref[z, :, pl.ds(PAD + 128, PAD), :] = pad0

    def clear_outside(first):
        @pl.loop(first, first + 4)
        def _(z):
            for ref in (f, a, b):
                for ph in range(4):
                    ref[z, ph, pl.ds(PAD, 128), :] = jnp.zeros((128, 128), F32)

        @pl.when(first == 0)
        def _():
            @pl.loop(0, 5)
            def _(z):
                s1[z, pl.ds(PAD, 128), :] = jnp.zeros((128, 128), F32)

        @pl.when(first > 0)
        def _():
            @pl.loop(9, 14)
            def _(z):
                s1[z, pl.ds(PAD, 128), :] = jnp.zeros((128, 128), F32)

    @pl.when(d == 0)
    def _():
        clear_outside(0)
        g0[0] = jnp.zeros((128, 128), F32)
        g1[0] = jnp.zeros((64, 128), F32)

    @pl.when(d == gz - 1)
    def _():
        clear_outside(12)
        g0[1] = jnp.zeros((128, 128), F32)
        g1[1] = jnp.zeros((64, 128), F32)

    @pl.loop(0, 14)
    def _(z):
        s1[z, pl.ds(0, PAD), :] = jnp.zeros((PAD, 128), F32)
        s1[z, pl.ds(PAD + 128, PAD), :] = jnp.zeros((PAD, 128), F32)
        a1[z] = jnp.zeros((144, 128), F32)
        b1[z] = jnp.zeros((144, 128), F32)

    @pl.loop(0, 7)
    def _(p):
        s2[p, pl.ds(0, PAD), :] = jnp.zeros((PAD, 128), F32)
        s2[p, pl.ds(PAD + 64, PAD), :] = jnp.zeros((PAD, 128), F32)
        a2[p] = jnp.zeros((80, 128), F32)
        b2[p] = jnp.zeros((80, 128), F32)
        at = d + p - 3

        @pl.when(jnp.logical_or(jnp.logical_or(at < 0, at >= gz), jnp.logical_or(p == 0, p == 6)))
        def _():
            s2[p, pl.ds(PAD, 64), :] = jnp.zeros((64, 128), F32)

    for q in range(4):
        a3[q] = jnp.zeros((48, 128), F32)
        b3[q] = jnp.zeros((48, 128), F32)

    def density(z, which, slot, put):
        left = jnp.dot(orb[z][which[0, 0]], px[...], preferred_element_type=F32)
        right = jnp.dot(orb[z][which[0, 1]], px[...], preferred_element_type=F32)
        both = left * right
        tmp[slot, 0] = both[:, :128]
        tmp[slot, 1] = both[:, 128:]
        for yp in range(2):
            for xp in range(2):
                put(2 * yp + xp, tmp[slot, xp, pl.ds(yp, 128, stride=2), :])

    index_load.wait()
    weight_load.wait()
    for i, z in enumerate((0, 7, 1, 6, 2, 5, 3, 4)):
        orb_copy(z).wait()

        def put(ph, value):
            f[z + 4, ph, pl.ds(PAD, 128), :] = value

        density(z, pidx, i % 2, put)

    def w_plane(z, lo, hi):
        for r in range(0, 128, CH):
            c = center(f, z, r, CH)
            nb = nbxy0(f, z, r, CH, c)
            for ph in range(4):
                t = 12.0 * c[ph] + nb[ph]
                if lo:
                    t = t + rows(f, z - 1, ph, r, CH)
                if hi:
                    t = t + rows(f, z + 1, ph, r, CH)
                a[z, ph, pl.ds(PAD + r, CH), :] = t

    w_plane(4, False, True)
    w_plane(11, True, False)

    pl.semaphore_wait(barrier, gz - 1 + pairs - 1 + has_across.astype(jnp.int32))

    index_copy = remote(pidx, pidx2, ixs.at[0], ixr.at[0], pair=other)
    index_copy.start()

    for side, z in ((0, 4), (1, 11)):
        for r in range(0, 128, CH):
            total, shifts = phase_sums(f, z, r, CH, center(f, z, r, CH))
            w = center(a, z, r, CH)
            g0o[side, pl.ds(r, CH), :] = (0.5 * N81) * (
                shifts - 3.0 * total + ((w[0] + w[1]) + (w[2] + w[3]))
            )

    def exchange(out, landed, s_sems, r_sems):
        lo = remote(out.at[0], landed.at[1], s_sems.at[0], r_sems.at[1], gz=jnp.maximum(d - 1, 0))
        hi = remote(out.at[1], landed.at[0], s_sems.at[1], r_sems.at[0], gz=jnp.minimum(d + 1, gz - 1))
        return lo, hi

    g0_lo, g0_hi = exchange(g0o, g0, g0s, g0r)

    @pl.when(has_lo)
    def _():
        g0_lo.start()

    @pl.when(has_hi)
    def _():
        g0_hi.start()

    turn = lax.rem(d, 4)
    straight = jnp.logical_or(turn == 1, turn == 2)
    diagonal = jnp.logical_not(straight)

    def f_copy(side, far, of_other):
        k = far if side == 0 else 3 - far
        here = k if side == 0 else 4 + k
        there = 12 + k if side == 0 else k
        to = jnp.maximum(d - 1, 0) if side == 0 else jnp.minimum(d + 1, gz - 1)
        landed = f.at[there, :, pl.ds(PAD, 128), :]
        if of_other:
            return remote(fx.at[k], landed, fs.at[side, far], fr.at[1 - side, far], gz=to, pair=other)
        return remote(
            f.at[4 + here, :, pl.ds(PAD, 128), :], landed, fs.at[side, far], fr.at[1 - side, far], gz=to, pair=me
        )

    def on_chip(act):
        for side, cond in ((0, jnp.logical_not(even)), (1, even)):
            @pl.when(cond)
            def _():
                for far in range(4):
                    act(side, far, False)

    def crossing(far, act, of_other, only=True):
        for side, cond in ((0, jnp.logical_and(even, has_lo)), (1, jnp.logical_and(jnp.logical_not(even), has_hi))):
            cond = jnp.logical_and(cond, only)
            if far == 0:
                cond = jnp.logical_and(cond, straight if of_other else diagonal)
            elif not of_other:
                continue

            @pl.when(cond)
            def _():
                act(side, far, of_other)

    def begin(side, far, of_other):
        f_copy(side, far, of_other).start()

    def sent(side, far, of_other):
        f_copy(side, far, of_other).wait_send()

    crossing(0, begin, False)
    on_chip(begin)

    @pl.loop(5, 11)
    def _(z):
        w_plane(z, True, True)

    for ph in range(4):
        a[3, ph, pl.ds(PAD, 128), :] = flo * f[4, ph, pl.ds(PAD, 128), :]
        a[12, ph, pl.ds(PAD, 128), :] = fhi * f[11, ph, pl.ds(PAD, 128), :]

    @pl.loop(0, 4)
    def _(j):
        for r in range(0, 128, CH):
            out = None
            for dz in range(2):
                z = 4 + 2 * j + dz
                c = center(a, z, r, CH)
                total, shifts = phase_sums(a, z, r, CH, c)
                below, above, src = center(a, z - 1, r, CH), center(a, z + 1, r, CH), center(f, z, r, CH)
                zs = ((below[0] + below[1]) + (below[2] + below[3])) + (
                    (above[0] + above[1]) + (above[2] + above[3])
                )
                q = ((src[0] + src[1]) + (src[2] + src[3])) + N81 * (zs - 4.0 * total + shifts)
                out = q if out is None else out + q
            s1[5 + j, pl.ds(PAD + r, CH), :] = 0.5 * out
            b1[5 + j, pl.ds(PAD + r, CH), :] = 0.5 * out

    def ypair(ref, slot, n):
        return ref[slot, pl.ds(0, n, stride=2), :] + ref[slot, pl.ds(1, n, stride=2), :]

    def inside(step):
        at = d + step
        return jnp.logical_and(at >= 0, at < gz)

    flag2 = {p: inside(p - 3).astype(F32) for p in range(1, 6)}
    m_first, m_second = mats[0], mats[1]
    low_half = lane_iota((64, 128)) < 64

    def nb2(ref, p, c):
        z = roll(c + jnp.where(low_half, crow(ref, p + 1, 0, 64), crow(ref, p - 1, 0, 64)), 64)
        return nbxy(ref, p, 0, 64, c, 64) + z

    b1[4, pl.ds(PAD, 128), :] = flo * g0o[0]
    b1[9, pl.ds(PAD, 128), :] = fhi * g0o[1]

    @pl.loop(3, 11, unroll=4)
    def _(z):
        flag = jnp.where(z < 5, flo, jnp.where(z > 8, fhi, 1.0))
        for r in range(0, 128, 64):
            c = crow(b1, z, r, 64)
            nb = nbxy(b1, z, r, 64, c, 128) + (crow(b1, z - 1, r, 64) + crow(b1, z + 1, r, 64))
            a1[z, pl.ds(PAD + r, 64), :] = flag * (12.0 * c + nb)

    @pl.loop(0, 6, unroll=2)
    def _(j):
        for r in range(0, 128, 64):
            out = None
            for dz in range(2):
                z = 1 + 2 * j + dz
                c = crow(a1, z, r, 64)
                nb = nbxy(a1, z, r, 64, c, 128) + (crow(a1, z - 1, r, 64) + crow(a1, z + 1, r, 64))
                q = crow(b1, z, r, 64) + N81 * (nb - 6.0 * c)
                out = q if out is None else out + q
            t1[j, pl.ds(r, 64), :] = 0.5 * out

    for p in range(3):
        b2[2 + p, pl.ds(PAD, 64), :] = flag2[2 + p] * (
            split_dot(ypair(t1, 2 * p, 64), m_first) + split_dot(ypair(t1, 2 * p + 1, 64), m_second)
        )
    for p in range(1, 6):
        c = crow(b2, p, 0, 64)
        a2[p, pl.ds(PAD, 64), :] = flag2[p] * (12.0 * c + nb2(b2, p, c))
    for p in range(1, 6):
        w = crow(a2, p, 0, 64)
        t2[p - 1] = crow(b2, p, 0, 64) + N81 * (nb2(a2, p, w) - 6.0 * w)
    tile = None
    for p in range(1, 5):
        part = split_dot(ypair(t2, p, 32), mats[4 + p])
        tile = part if tile is None else tile + part
    t3[d, pl.ds(0, 32), :] = 0.5 * tile
    part = split_dot(ypair(t2, 0, 32), mats[14])
    block8 = lane_iota((8, 128)) // 32
    row = part[0:8]
    for k in range(1, 4):
        row = jnp.where(block8 == k, part[8 * k:8 * k + 8], row)
    t3[d, pl.ds(32, 8), :] = 0.5 * row

    def t3_copy(o):
        to = lax.rem(d + o, gz)
        return remote(t3.at[d], t3.at[d], t3s.at[o], t3r.at[d], gz=to)

    @pl.loop(1, gz)
    def _(o):
        t3_copy(o).start()

    index_copy.wait_recv()
    for far in range(4):
        for side, cond in ((0, even), (1, jnp.logical_not(even))):
            k = far if side == 0 else 3 - far
            if far == 0:
                cond = jnp.logical_and(cond, straight)

            def put_other(ph, value):
                fx[k, ph] = value

            @pl.when(cond)
            def _():
                density(k + 4 * side, pidx2, far % 2, put_other)

        crossing(far, begin, True, straight if far > EARLY else True)

    @pl.when(has_lo)
    def _():
        g0_hi.wait_recv()
        s1[5, pl.ds(PAD, 128), :] += g0[0]

    @pl.when(has_hi)
    def _():
        g0_lo.wait_recv()
        s1[8, pl.ds(PAD, 128), :] += g0[1]

    def w1_plane(z, lo, hi):
        for r in range(0, 128, 64):
            c = crow(s1, z, r, 64)
            t = 12.0 * c + nbxy(s1, z, r, 64, c, 128)
            if lo:
                t = t + crow(s1, z - 1, r, 64)
            if hi:
                t = t + crow(s1, z + 1, r, 64)
            a1[z, pl.ds(PAD + r, 64), :] = t

    for z in range(5, 9):
        w1_plane(z, z > 5, z < 8)
    a1[4, pl.ds(PAD, 128), :] = flo * crow(s1, 5, 0, 128)
    a1[9, pl.ds(PAD, 128), :] = fhi * crow(s1, 8, 0, 128)
    for slot, z in ((0, 5), (3, 8)):
        for r in range(0, 128, 64):
            c = crow(s1, z, r, 64)
            t1[slot, pl.ds(r, 64), :] = (0.5 * N81) * (
                nbxy(s1, z, r, 64, c, 128) - 5.0 * c + crow(a1, z, r, 64)
            )
    for slot in (1, 2):
        for r in range(0, 128, 64):
            out = None
            for z in (3 + 2 * slot, 4 + 2 * slot):
                c = crow(a1, z, r, 64)
                nb = nbxy(a1, z, r, 64, c, 128) + (crow(a1, z - 1, r, 64) + crow(a1, z + 1, r, 64))
                q = crow(s1, z, r, 64) + N81 * (nb - 6.0 * c)
                out = q if out is None else out + q
            t1[slot, pl.ds(r, 64), :] = 0.5 * out

    g1o[0] = split_dot(ypair(t1, 0, 64), m_second)
    g1o[1] = split_dot(ypair(t1, 3, 64), m_first)
    g1_lo, g1_hi = exchange(g1o, g1, g1s, g1r)

    @pl.when(has_lo)
    def _():
        g1_lo.start()

    @pl.when(has_hi)
    def _():
        g1_hi.start()

    s2[3, pl.ds(PAD, 64), :] = split_dot(ypair(t1, 1, 64), m_first) + split_dot(ypair(t1, 2, 64), m_second)

    def h1_copy(i):
        here, there, step = ((5, 9, -1), (6, 2, 1))[i]
        to = jnp.clip(d + step, 0, gz - 1)
        return remote(
            s1.at[pl.ds(here, 3), pl.ds(PAD, 128), :], s1.at[pl.ds(there, 3), pl.ds(PAD, 128), :],
            h1s.at[i], h1r.at[i], gz=to,
        )

    h1_sends, h1_recvs = [has_lo, has_hi], [has_hi, has_lo]

    def h1_start():
        for i in range(2):
            @pl.when(h1_sends[i])
            def _():
                h1_copy(i).start()

    h1_start()

    @pl.when(has_lo)
    def _():
        g1_hi.wait_recv()
        s2[3, pl.ds(PAD, 64), :] += g1[0]

    @pl.when(has_hi)
    def _():
        g1_lo.wait_recv()
        s2[3, pl.ds(PAD, 64), :] += g1[1]

    def h2_copy(i):
        step = (-2, -1, 1, 2)[i]
        to = jnp.clip(d + step, 0, gz - 1)
        return remote(
            s2.at[3, pl.ds(PAD, 64), :], s2.at[3 - step, pl.ds(PAD, 64), :], h2s.at[i], h2r.at[i], gz=to
        )

    for i, step in enumerate((-2, -1, 1, 2)):
        @pl.when(inside(step))
        def _():
            h2_copy(i).start()


    @pl.loop(1, gz)
    def _(o):
        peer = lax.rem(d + o, gz)
        remote(t3.at[peer], t3.at[peer], t3s.at[o], t3r.at[peer], gz=peer).wait_recv()

    for far in range(EARLY + 1, 4):
        crossing(far, begin, True, diagonal)

    lane32 = lane_iota((32, 128))
    for q in range(4):
        total = None
        for e in range(max(4 * q - 2, 0), min(4 * q + 6, gz)):
            low, high = max(e - 1 - 4 * q, 0), min(e + 2 - 4 * q, 3)
            parts = []
            if low <= high:
                x = t3[e, pl.ds(0, 32), :]
                if (low, high) != (0, 3):
                    x = jnp.where(jnp.logical_and(lane32 >= 32 * low, lane32 < 32 * high + 32), x, 0.0)
                parts.append(x)
            block = e - 2 - 4 * q
            if 0 <= block < 4:
                x = t3[e, pl.ds(32, 8), :]
                pieces = [jnp.where(block8 == block, roll(x, 32 * (block - k)), 0.0) for k in range(4)]
                parts.append(jnp.concatenate(pieces, axis=0))
            for x in parts:
                total = x if total is None else total + x
        s3[q] = total * NINTH
        a3[q, pl.ds(PAD, 32), :] = total * NINTH

    def sweep3(src, dst):
        v = [crow(src, q, 0, 32) for q in range(4)]
        for q in range(4):
            after = v[q + 1] if q < 3 else jnp.zeros_like(v[0])
            before = v[q - 1] if q > 0 else jnp.zeros_like(v[0])
            nz = roll(jnp.where(lane32 < 32, after, v[q]), -32)
            nz = nz + roll(jnp.where(lane32 >= 96, before, v[q]), 32)
            nb = nbxy(src, q, 0, 32, v[q], 32) + nz
            dst[q, pl.ds(PAD, 32), :] = (1.0 / 3.0) * v[q] + (NINTH * nb + s3[q])

    @pl.loop(0, 3)
    def _(i):
        sweep3(a3, b3)
        sweep3(b3, a3)

    sweep3(a3, b3)

    for i, step in enumerate((-2, -1, 1, 2)):
        @pl.when(inside(-step))
        def _():
            h2_copy(i).wait_recv()

    for p in range(1, 6):
        at = d + p - 3
        q = jnp.clip(at // 4, 0, 3)
        e = split_dot(b3[q, pl.ds(PAD, 32), :], mats[8 + p])
        pe2[p - 1, pl.ds(0, 32, stride=2), :] = e
        pe2[p - 1, pl.ds(1, 32, stride=2), :] = e
    for p in range(1, 6):
        c = crow(s2, p, 0, 64)
        w = 12.0 * c + nb2(s2, p, c)
        a2[p, pl.ds(PAD, 64), :] = flag2[p] * (N81 * w + pe2[p - 1])

    def sweep2(src, dst, p):
        c = crow(src, p, 0, 64)
        dst[p, pl.ds(PAD, 64), :] = flag2[p] * (
            (1.0 / 3.0) * c + NINTH * (nb2(src, p, c) + crow(s2, p, 0, 64))
        )

    for p in range(2, 5):
        sweep2(a2, b2, p)
    for p in range(2, 5):
        sweep2(b2, a2, p)

    for i in range(2):
        @pl.when(h1_recvs[i])
        def _():
            h1_copy(i).wait_recv()

    for j in range(1, 5):
        e = split_dot(a2[2 + j // 2, pl.ds(PAD, 64), :], mats[2 + j % 2])
        pe1[j, pl.ds(0, 64, stride=2), :] = e
        pe1[j, pl.ds(1, 64, stride=2), :] = e

    def in_grid(z):
        return jnp.where(z < 5, flo, jnp.where(z > 8, fhi, 1.0))

    def nb1(ref, z, r, c):
        return nbxy(ref, z, r, 64, c, 128) + (crow(ref, z - 1, r, 64) + crow(ref, z + 1, r, 64))

    @pl.loop(3, 11, unroll=4)
    def _(z):
        flag = in_grid(z)
        for r in range(0, 128, 64):
            c = crow(s1, z, r, 64)
            w = 12.0 * c + nb1(s1, z, r, c)
            a1[z, pl.ds(PAD + r, 64), :] = flag * (N81 * w + pe1[(z - 1) // 2, pl.ds(r, 64), :])

    @pl.loop(4, 10, unroll=3)
    def _(z):
        flag = in_grid(z)
        for r in range(0, 128, 64):
            c = crow(a1, z, r, 64)
            t = nb1(a1, z, r, c) + crow(s1, z, r, 64)
            b1[z, pl.ds(PAD + r, 64), :] = flag * ((1.0 / 3.0) * c + NINTH * t)

    @pl.loop(5, 9, unroll=4)
    def _(z):
        for r in range(0, 128, 64):
            c = crow(b1, z, r, 64)
            t = nb1(b1, z, r, c) + crow(s1, z, r, 64)
            e1[z - 5, pl.ds(r, 64), :] = (1.0 / 3.0) * c + NINTH * t

    e1_lo = remote(
        e1.at[pl.ds(0, 2)], e1h.at[1], e1s.at[0], e1r.at[1], gz=jnp.maximum(d - 1, 0)
    )
    e1_hi = remote(
        e1.at[pl.ds(2, 2)], e1h.at[0], e1s.at[1], e1r.at[0], gz=jnp.minimum(d + 1, gz - 1)
    )

    @pl.when(has_lo)
    def _():
        e1_lo.start()

    @pl.when(has_hi)
    def _():
        e1_hi.start()

    def f_wait(*which):
        @pl.when(has_lo)
        def _():
            for far in which:
                f_copy(1, far, False).wait_recv()

        @pl.when(has_hi)
        def _():
            for far in which:
                f_copy(0, far, False).wait_recv()

    def correct(z, ref, k):
        e = ref[k]
        for ph in range(4):
            a[z, ph, pl.ds(PAD, 128), :] = N81 * a[z, ph, pl.ds(PAD, 128), :] + e

    def sweep0(src, dst, first, last):
        @pl.loop(first + 4, last + 5)
        def _(z):
            for r in range(0, 128, CH):
                c = center(src, z, r, CH)
                nb = nbxy0(src, z, r, CH, c)
                for ph in range(4):
                    t = nb[ph] + (rows(src, z - 1, ph, r, CH) + rows(src, z + 1, ph, r, CH))
                    t = t + rows(f, z, ph, r, CH)
                    dst[z, ph, pl.ds(PAD + r, CH), :] = (1.0 / 3.0) * c[ph] + NINTH * t

    def below(first):
        return jnp.where(has_lo, first, 0)

    def above(last):
        return jnp.where(has_hi, last, 7)

    f_wait(0, 1)
    w_plane(4, True, True)
    w_plane(11, True, True)

    @pl.when(has_hi)
    def _():
        w_plane(12, True, True)

    def products(z, carry):
        plain, edges = carry
        for r in range(0, 128, CH):
            c, src, up = center(a, z, r, CH), center(f, z, r, CH), center(a, z + 1, r, CH)
            for ph in range(4):
                plain = plain + fold(c[ph] * (src[ph] - (3.0 * N81) * c[ph]))
            e = c[0] * c[1] + c[2] * c[3] + (c[0] * c[2] + c[1] * c[3])
            e = e + (c[1] * from_right(c[0]) + c[3] * from_right(c[2]))
            e = e + (c[2] * rows(a, z, 0, r, CH, 1) + c[3] * rows(a, z, 1, r, CH, 1))
            for ph in range(4):
                e = e + c[ph] * up[ph]
            edges = edges + fold(e)
        return plain, edges

    zero = jnp.zeros((8, 128), F32)
    plain, edges = lax.fori_loop(4, 12, products, (zero, zero))
    coarse = zero
    for j in range(4):
        coarse = coarse + fold(s1[5 + j, pl.ds(PAD, 128), :] * e1[j])
    part = (2.0 * N81) * (plain + N81 * edges) + 2.0 * coarse
    prods[d] = part.sum(axis=0, keepdims=True)

    @pl.loop(1, gz)
    def _(o):
        remote(prods.at[d], prods.at[d], ps.at[o], pr.at[d], gz=lax.rem(d + o, gz)).start()


    @pl.loop(0, 8)
    def _(z):
        correct(z + 4, e1, z // 2)

    sweep0(a, b, 1, 6)
    sweep0(b, a, 2, 5)

    f_wait(2, 3)

    @pl.loop(below(-3) + 4, 4)
    def _(z):
        w_plane(z, True, True)

    @pl.loop(12, above(10) + 5)
    def _(z):
        w_plane(z, True, True)

    @pl.when(has_lo)
    def _():
        e1_hi.wait_recv()
        for z in range(-3, 0):
            correct(z + 4, e1h.at[0], (z + 4) // 2)

    @pl.when(has_hi)
    def _():
        e1_lo.wait_recv()
        for z in range(8, 11):
            correct(z + 4, e1h.at[1], (z - 8) // 2)

    sweep0(a, b, below(-2), 0)
    sweep0(a, b, 7, above(9))
    sweep0(b, a, below(-1), 1)
    sweep0(b, a, 6, above(8))

    def final(z, squares):
        for r in range(0, 128, CH):
            c = center(a, z, r, CH)
            nb = nbxy0(a, z, r, CH, c)
            for ph in range(4):
                t = nb[ph] + (rows(a, z - 1, ph, r, CH) + rows(a, z + 1, ph, r, CH))
                left = (rows(f, z, ph, r, CH) - 6.0 * c[ph]) + t
                squares = squares + fold(left * left)
        return squares

    sums[d] = lax.fori_loop(4, 12, final, zero).sum(axis=0, keepdims=True)

    @pl.loop(1, gz)
    def _(o):
        remote(sums.at[d], sums.at[d], ss.at[o], sr.at[d], gz=lax.rem(d + o, gz)).start()

    @pl.loop(1, gz)
    def _(o):
        peer = lax.rem(d + o, gz)
        remote(prods.at[peer], prods.at[peer], ps.at[o], pr.at[peer], gz=peer).wait_recv()

    total = prods[0]
    for e in range(1, gz):
        total = total + prods[e]
    ens[me] = pweight[0, 0] * total

    @pl.loop(1, pairs)
    def _(o):
        remote(ens.at[me], ens.at[me], es.at[o], er.at[me], pair=lax.rem(me + o, pairs)).start()

    px[...] = selection((256, 256), lambda i, j: i == (j & 1) * 128 + (j >> 1))

    @pl.loop(0, 8)
    def _(z):
        for yp in range(2):
            x = jnp.concatenate(
                [a[z + 4, 2 * yp, pl.ds(PAD, 128), :], a[z + 4, 2 * yp + 1, pl.ds(PAD, 128), :]], axis=1
            )
            y = split_dot(x, px[...])
            for half in range(2):
                tmp[z % 2, half, pl.ds(yp, 128, stride=2), :] = y[:, 128 * half:128 * half + 128]
        for half in range(2):
            pot[0, z, :, pl.ds(128 * half, 128)] = tmp[z % 2, half]

    @pl.loop(1, gz)
    def _(o):
        peer = lax.rem(d + o, gz)
        remote(sums.at[peer], sums.at[peer], ss.at[o], sr.at[peer], gz=peer).wait_recv()

    total = sums[0]
    for e in range(1, gz):
        total = total + sums[e]
    cells = 1.0 / (gz * 8 * 256 * 256)
    res_out[...] = jnp.sqrt(jnp.sum(total, axis=1, keepdims=True) * cells)

    @pl.loop(1, pairs)
    def _(o):
        peer = lax.rem(me + o, pairs)
        remote(ens.at[peer], ens.at[peer], es.at[o], er.at[peer], pair=peer).wait_recv()

    energy = ens[0]
    for e in range(1, pairs):
        energy = energy + ens[e]
    en_out[...] = jnp.sum(energy, axis=1, keepdims=True) * (-0.5 * cells)

    for cond, side in ((has_lo, 0), (has_hi, 1)):
        @pl.when(cond)
        def _():
            (g0_lo, g0_hi)[side].wait_send()
            (g1_lo, g1_hi)[side].wait_send()
            (e1_lo, e1_hi)[side].wait_send()

    index_copy.wait_send()
    on_chip(sent)
    for far in range(4):
        crossing(far, sent, True)
    crossing(0, sent, False)

    for i in range(2):
        @pl.when(h1_sends[i])
        def _():
            h1_copy(i).wait_send()

    for i, step in enumerate((-2, -1, 1, 2)):
        @pl.when(inside(step))
        def _():
            h2_copy(i).wait_send()

    @pl.loop(1, gz)
    def _(o):
        t3_copy(o).wait_send()
        remote(sums.at[d], sums.at[d], ss.at[o], sr.at[d], gz=lax.rem(d + o, gz)).wait_send()
        remote(prods.at[d], prods.at[d], ps.at[o], pr.at[d], gz=lax.rem(d + o, gz)).wait_send()

    @pl.loop(1, pairs)
    def _(o):
        remote(ens.at[me], ens.at[me], es.at[o], er.at[me], pair=lax.rem(me + o, pairs)).wait_send()


def solution(mesh):
    gz, pairs = mesh.shape["gz"], mesh.shape["pair"]
    dma, vmem = pltpu.SemaphoreType.DMA, pltpu.VMEM
    field = vmem((16, 4, 144, 128), F32)
    level1, level2, level3 = vmem((14, 144, 128), F32), vmem((7, 80, 128), F32), vmem((4, 48, 128), F32)

    def per_device(orbitals, pair_index, pair_weight):
        potential, norm, energy = pl.pallas_call(
            functools.partial(kernel, gz, pairs),
            out_shape=(
                jax.ShapeDtypeStruct((1, 8, 256, 256), F32),
                jax.ShapeDtypeStruct((1, 1), F32),
                jax.ShapeDtypeStruct((1, 1), F32),
            ),
            in_specs=[
                pl.BlockSpec(memory_space=pltpu.HBM),
                pl.BlockSpec(memory_space=pltpu.HBM),
                pl.BlockSpec(memory_space=pl.ANY),
            ],
            out_specs=(
                pl.BlockSpec(memory_space=pltpu.VMEM),
                pl.BlockSpec(memory_space=pltpu.VMEM),
                pl.BlockSpec(memory_space=pltpu.VMEM),
            ),
            scratch_shapes=[
                *[vmem((8, 256, 256), BF16)] * 8,
                vmem((256, 256), BF16),
                vmem((15, 128, 128), BF16),
                vmem((2, 2, 256, 128), F32),
                pltpu.SMEM((1, 2), jnp.int32),
                pltpu.SMEM((1, 1), F32),
                pltpu.SMEM((1, 2), jnp.int32),
                vmem((4, 4, 128, 128), F32),
                field, field, field,
                vmem((2, 128, 128), F32), vmem((2, 128, 128), F32),
                level1, level1, level1,
                vmem((6, 128, 128), F32),
                vmem((2, 64, 128), F32), vmem((2, 64, 128), F32),
                vmem((6, 128, 128), F32),
                vmem((4, 128, 128), F32), vmem((2, 2, 128, 128), F32),
                level2, level2, level2,
                vmem((5, 64, 128), F32),
                vmem((5, 64, 128), F32),
                vmem((gz, 40, 128), F32),
                vmem((4, 32, 128), F32),
                level3, level3,
                vmem((gz, 1, 128), F32), vmem((gz, 1, 128), F32),
                vmem((pairs, 1, 128), F32),
                dma((2,)),
                dma((8,)),
                dma((1,)), dma((1,)),
                dma((2, 4)), dma((2, 4)),
                dma((2,)), dma((2,)),
                dma((2,)), dma((2,)),
                dma((2,)), dma((2,)),
                dma((2,)), dma((2,)),
                dma((4,)), dma((4,)),
                dma((gz,)), dma((gz,)),
                dma((gz,)), dma((gz,)),
                dma((gz,)), dma((gz,)),
                dma((pairs,)), dma((pairs,)),
            ],
            compiler_params=pltpu.CompilerParams(
                collective_id=0, has_side_effects=True, vmem_limit_bytes=48 * 1024 * 1024
            ),
            name="vcycle",
        )(pltpu.with_memory_space_constraint(pair_index, pltpu.HBM), pair_weight.reshape(1, 1), orbitals)
        return potential, norm.reshape(1), energy.reshape(1)

    return jax.shard_map(
        per_device,
        mesh=mesh,
        in_specs=(P(None, "gz", None, None), P("pair", None), P("pair")),
        out_specs=(P("pair", "gz", None, None), P("pair"), P()),
        check_vma=False,
    )
```

```python
import functools

import jax
import jax.numpy as jnp
from jax import lax
from jax.experimental import pallas as pl
from jax.experimental.pallas import tpu as pltpu
from jax.sharding import PartitionSpec as P

MESH = pl.DeviceIdType.MESH
F32, BF16 = jnp.float32, jnp.bfloat16
PAD = 8
EARLY = True
CH = 32
NINTH = 1.0 / 9.0
N81 = 1.0 / 81.0


def lane_iota(shape):
    return lax.broadcasted_iota(jnp.int32, shape, len(shape) - 1)


def roll(x, shift):
    return pltpu.roll(x, shift % x.shape[-1], x.ndim - 1)


def from_left(x, width=128):
    return jnp.where(lane_iota(x.shape) % width == 0, 0.0, roll(x, 1))


def from_right(x, width=128):
    return jnp.where(lane_iota(x.shape) % width == width - 1, 0.0, roll(x, -1))


def split_dot(x, m):
    hi = x.astype(BF16)
    rest = x - hi.astype(F32)
    mid = rest.astype(BF16)
    low = (rest - mid.astype(F32)).astype(BF16)
    dot = functools.partial(jnp.dot, preferred_element_type=F32)
    return dot(hi, m) + dot(mid, m) + dot(low, m)


def selection(shape, test):
    a = lax.broadcasted_iota(jnp.int32, shape, 0)
    b = lax.broadcasted_iota(jnp.int32, shape, 1)
    return jnp.where(test(a, b), 1.0, 0.0).astype(BF16)


def fold(x):
    return x.reshape(x.shape[0] // 8, 8, x.shape[1]).sum(axis=0)


def rows(ref, z, ph, r, n, dr=0):
    return ref[z, ph, pl.ds(PAD + r + dr, n), :]


def nbxy0(ref, z, r, n, c):
    out = []
    for yp in range(2):
        for xp in range(2):
            side = c[2 * yp + 1 - xp]
            x = side + (from_right(side) if xp else from_left(side))
            other = 2 * (1 - yp) + xp
            y = c[other] + rows(ref, z, other, r, n, 1 if yp else -1)
            out.append(x + y)
    return out


def phase_sums(ref, z, r, n, c):
    total = (c[0] + c[1]) + (c[2] + c[3])
    shifts = from_left(c[1] + c[3]) + from_right(c[0] + c[2])
    shifts = shifts + (rows(ref, z, 2, r, n, -1) + rows(ref, z, 3, r, n, -1))
    shifts = shifts + (rows(ref, z, 0, r, n, 1) + rows(ref, z, 1, r, n, 1))
    return total, shifts


def center(ref, z, r, n):
    return [rows(ref, z, ph, r, n) for ph in range(4)]


def crow(ref, z, r, n, dr=0):
    return ref[z, pl.ds(PAD + r + dr, n), :]


def nbxy(ref, z, r, n, c, width):
    y = crow(ref, z, r, n, -1) + crow(ref, z, r, n, 1)
    return y + (from_left(c, width) + from_right(c, width))


def kernel(
    gz, pairs,
    index_in, weight_in, orbitals, pot, res_out, en_out,
    orb0, orb1, orb2, orb3, orb4, orb5, orb6, orb7, px, mats, tmp, pidx, pweight, pidx2, fx, relay, f, a, b, g0, g0o, s1, a1, b1, t1, g1, g1o, pe1, e1, e1h,
    s2, a2, b2, t2, pe2, t3, s3, a3, b3, prods, sums, ens,
    scalar_sem, orb_sem, ixs, ixr, ys, yr, yf, fs, fr, g0s, g0r, h1s, h1r, g1s, g1r, e1s, e1r, h2s, h2r, t3s, t3r, ps, pr, ss, sr, es, er,
):
    d = lax.axis_index("gz")
    me = lax.axis_index("pair")
    has_lo, has_hi = d > 0, d < gz - 1
    flo, fhi = has_lo.astype(F32), has_hi.astype(F32)

    def remote(src, dst, s_sem, r_sem, **to):
        return pltpu.make_async_remote_copy(
            src_ref=src, dst_ref=dst, send_sem=s_sem, recv_sem=r_sem, device_id=to, device_id_type=MESH
        )

    orb = (orb0, orb1, orb2, orb3, orb4, orb5, orb6, orb7)

    def orb_copy(z):
        return pltpu.make_async_copy(orbitals.at[:, z], orb[z], orb_sem.at[z])

    index_load = pltpu.make_async_copy(index_in, pidx, scalar_sem.at[0])
    weight_load = pltpu.make_async_copy(weight_in, pweight, scalar_sem.at[1])
    index_load.start()
    weight_load.start()
    for z in range(8):
        orb_copy(z).start()
    barrier = pltpu.get_barrier_semaphore()

    @pl.loop(1, gz)
    def _(o):
        pl.semaphore_signal(barrier, inc=1, device_id={"gz": lax.rem(d + o, gz)}, device_id_type=MESH)

    @pl.loop(1, pairs)
    def _(o):
        pl.semaphore_signal(barrier, inc=1, device_id={"pair": lax.rem(me + o, pairs)}, device_id_type=MESH)

    other = lax.rem(me + pairs // 2, pairs)
    even = lax.rem(d, 2) == 0
    across = jnp.where(even, d - 1, d + 1)
    has_across = jnp.logical_and(across >= 0, across < gz)

    @pl.when(has_across)
    def _():
        pl.semaphore_signal(barrier, inc=1, device_id={"gz": across, "pair": other}, device_id_type=MESH)

    turn = lax.rem(d, 4)
    straight = jnp.logical_or(turn == 1, turn == 2)
    diagonal = jnp.logical_not(straight)
    partner = jnp.where(turn == 0, d + 3, d - 3)

    @pl.when(diagonal)
    def _():
        pl.semaphore_signal(barrier, inc=1, device_id={"gz": partner, "pair": other}, device_id_type=MESH)

    px[...] = selection((256, 256), lambda i, j: j == (i & 1) * 128 + (i >> 1))
    pad0 = jnp.zeros((4, PAD, 128), F32)
    square = (128, 128)
    mats[0] = selection(square, lambda i, j: (i >> 1) == j)
    mats[1] = selection(square, lambda i, j: (i >> 1) + 64 == j)
    for half in range(2):
        mats[2 + half] = selection(square, lambda i, j: i == (j >> 1) + 64 * half)
    for p in range(5):
        block = lax.rem(d + p - 2 + gz, 4) * 32
        mats[4 + p] = selection(square, lambda i, j: ((i & 63) >> 1) + block == j)
        mats[9 + p] = selection(square, lambda i, j: i == ((j & 63) >> 1) + block)
    mats[14] = selection(square, lambda i, j: ((i & 63) >> 1) == (j & 31))

    @pl.loop(0, 16)
    def _(z):
        for ref in (f, a, b):
            ref[z, :, pl.ds(0, PAD), :] = pad0
            ref[z, :, pl.ds(PAD + 128, PAD), :] = pad0

    def clear_outside(first):
        @pl.loop(first, first + 4)
        def _(z):
            for ref in (f, a, b):
                for ph in range(4):
                    ref[z, ph, pl.ds(PAD, 128), :] = jnp.zeros((128, 128), F32)

        @pl.when(first == 0)
        def _():
            @pl.loop(0, 5)
            def _(z):
                s1[z, pl.ds(PAD, 128), :] = jnp.zeros((128, 128), F32)

        @pl.when(first > 0)
        def _():
            @pl.loop(9, 14)
            def _(z):
                s1[z, pl.ds(PAD, 128), :] = jnp.zeros((128, 128), F32)

    @pl.when(d == 0)
    def _():
        clear_outside(0)
        g0[0] = jnp.zeros((128, 128), F32)
        g1[0] = jnp.zeros((64, 128), F32)

    @pl.when(d == gz - 1)
    def _():
        clear_outside(12)
        g0[1] = jnp.zeros((128, 128), F32)
        g1[1] = jnp.zeros((64, 128), F32)

    @pl.loop(0, 14)
    def _(z):
        s1[z, pl.ds(0, PAD), :] = jnp.zeros((PAD, 128), F32)
        s1[z, pl.ds(PAD + 128, PAD), :] = jnp.zeros((PAD, 128), F32)
        a1[z] = jnp.zeros((144, 128), F32)
        b1[z] = jnp.zeros((144, 128), F32)

    @pl.loop(0, 7)
    def _(p):
        s2[p, pl.ds(0, PAD), :] = jnp.zeros((PAD, 128), F32)
        s2[p, pl.ds(PAD + 64, PAD), :] = jnp.zeros((PAD, 128), F32)
        a2[p] = jnp.zeros((80, 128), F32)
        b2[p] = jnp.zeros((80, 128), F32)
        at = d + p - 3

        @pl.when(jnp.logical_or(jnp.logical_or(at < 0, at >= gz), jnp.logical_or(p == 0, p == 6)))
        def _():
            s2[p, pl.ds(PAD, 64), :] = jnp.zeros((64, 128), F32)

    for q in range(4):
        a3[q] = jnp.zeros((48, 128), F32)
        b3[q] = jnp.zeros((48, 128), F32)

    def density(z, which, slot, put):
        left = jnp.dot(orb[z][which[0, 0]], px[...], preferred_element_type=F32)
        right = jnp.dot(orb[z][which[0, 1]], px[...], preferred_element_type=F32)
        both = left * right
        tmp[slot, 0] = both[:, :128]
        tmp[slot, 1] = both[:, 128:]
        for yp in range(2):
            for xp in range(2):
                put(2 * yp + xp, tmp[slot, xp, pl.ds(yp, 128, stride=2), :])

    index_load.wait()
    weight_load.wait()
    def w_plane(z, lo, hi):
        for r in range(0, 128, CH):
            c = center(f, z, r, CH)
            nb = nbxy0(f, z, r, CH, c)
            for ph in range(4):
                t = 12.0 * c[ph] + nb[ph]
                if lo:
                    t = t + rows(f, z - 1, ph, r, CH)
                if hi:
                    t = t + rows(f, z + 1, ph, r, CH)
                a[z, ph, pl.ds(PAD + r, CH), :] = t

    for i, z in enumerate(range(8)):
        orb_copy(z).wait()

        def put(ph, value):
            f[z + 4, ph, pl.ds(PAD, 128), :] = value

        density(z, pidx, i % 2, put)
        if z:
            w_plane(z + 3, z > 1, True)

    w_plane(11, True, False)

    pl.semaphore_wait(barrier, gz - 1 + pairs - 1 + has_across.astype(jnp.int32) + diagonal.astype(jnp.int32))

    index_copy = remote(pidx, pidx2, ixs.at[0], ixr.at[0], pair=other)
    index_copy.start()

    for side, z in ((0, 4), (1, 11)):
        for r in range(0, 128, CH):
            total, shifts = phase_sums(f, z, r, CH, center(f, z, r, CH))
            w = center(a, z, r, CH)
            g0o[side, pl.ds(r, CH), :] = (0.5 * N81) * (
                shifts - 3.0 * total + ((w[0] + w[1]) + (w[2] + w[3]))
            )

    def exchange(out, landed, s_sems, r_sems):
        lo = remote(out.at[0], landed.at[1], s_sems.at[0], r_sems.at[1], gz=jnp.maximum(d - 1, 0))
        hi = remote(out.at[1], landed.at[0], s_sems.at[1], r_sems.at[0], gz=jnp.minimum(d + 1, gz - 1))
        return lo, hi

    g0_lo, g0_hi = exchange(g0o, g0, g0s, g0r)

    @pl.when(has_lo)
    def _():
        g0_lo.start()

    @pl.when(has_hi)
    def _():
        g0_hi.start()

    def f_copy(side, far, of_other):
        k = far if side == 0 else 3 - far
        here = k if side == 0 else 4 + k
        there = 12 + k if side == 0 else k
        to = jnp.maximum(d - 1, 0) if side == 0 else jnp.minimum(d + 1, gz - 1)
        landed = f.at[there, :, pl.ds(PAD, 128), :]
        if of_other:
            return remote(fx.at[k], landed, fs.at[side, far], fr.at[1 - side, far], gz=to, pair=other)
        return remote(
            f.at[4 + here, :, pl.ds(PAD, 128), :], landed, fs.at[side, far], fr.at[1 - side, far], gz=to, pair=me
        )

    def on_chip(act):
        for side, cond in ((0, jnp.logical_not(even)), (1, even)):
            @pl.when(cond)
            def _():
                for far in range(4):
                    act(side, far, False)

    def crossing(far, act, of_other, only=True):
        kind = {
            (0, False): diagonal, (3, False): straight,
            (0, True): straight, (1, True): True, (2, True): straight,
        }.get((far, of_other))
        if kind is None:
            return
        for side, cond in ((0, jnp.logical_and(even, has_lo)), (1, jnp.logical_and(jnp.logical_not(even), has_hi))):
            @pl.when(jnp.logical_and(cond, jnp.logical_and(kind, only)))
            def _():
                act(side, far, of_other)

    relays = ((0, jnp.logical_and(turn == 0, has_lo), jnp.logical_and(turn == 0, d < gz - 4), -4),
              (1, jnp.logical_and(turn == 3, has_hi), jnp.logical_and(turn == 3, d >= 4), 4))

    def to_relay(side, far, step):
        k = far if side == 0 else 3 - far
        return remote(
            fx.at[k], relay.at[far - 2], ys.at[far - 2], yr.at[far - 2], gz=jnp.clip(d + step, 0, gz - 1), pair=me
        )

    def hand_on(side, far):
        there = 12 + far if side == 0 else 3 - far
        return remote(
            relay.at[far - 2], f.at[there, :, pl.ds(PAD, 128), :], yf.at[far - 2], fr.at[1 - side, far],
            gz=jnp.clip(partner, 0, gz - 1), pair=other,
        )

    def begin(side, far, of_other):
        f_copy(side, far, of_other).start()

    def sent(side, far, of_other):
        f_copy(side, far, of_other).wait_send()

    crossing(0, begin, False)
    on_chip(begin)

    for ph in range(4):
        a[3, ph, pl.ds(PAD, 128), :] = flo * f[4, ph, pl.ds(PAD, 128), :]
        a[12, ph, pl.ds(PAD, 128), :] = fhi * f[11, ph, pl.ds(PAD, 128), :]

    @pl.loop(0, 4)
    def _(j):
        for r in range(0, 128, CH):
            out = None
            for dz in range(2):
                z = 4 + 2 * j + dz
                c = center(a, z, r, CH)
                total, shifts = phase_sums(a, z, r, CH, c)
                below, above, src = center(a, z - 1, r, CH), center(a, z + 1, r, CH), center(f, z, r, CH)
                zs = ((below[0] + below[1]) + (below[2] + below[3])) + (
                    (above[0] + above[1]) + (above[2] + above[3])
                )
                q = ((src[0] + src[1]) + (src[2] + src[3])) + N81 * (zs - 4.0 * total + shifts)
                out = q if out is None else out + q
            s1[5 + j, pl.ds(PAD + r, CH), :] = 0.5 * out
            b1[5 + j, pl.ds(PAD + r, CH), :] = 0.5 * out

    def ypair(ref, slot, n):
        return ref[slot, pl.ds(0, n, stride=2), :] + ref[slot, pl.ds(1, n, stride=2), :]

    def inside(step):
        at = d + step
        return jnp.logical_and(at >= 0, at < gz)

    flag2 = {p: inside(p - 3).astype(F32) for p in range(1, 6)}
    m_first, m_second = mats[0], mats[1]
    low_half = lane_iota((64, 128)) < 64

    def nb2(ref, p, c):
        z = roll(c + jnp.where(low_half, crow(ref, p + 1, 0, 64), crow(ref, p - 1, 0, 64)), 64)
        return nbxy(ref, p, 0, 64, c, 64) + z

    b1[4, pl.ds(PAD, 128), :] = flo * g0o[0]
    b1[9, pl.ds(PAD, 128), :] = fhi * g0o[1]

    @pl.loop(3, 11, unroll=4)
    def _(z):
        flag = jnp.where(z < 5, flo, jnp.where(z > 8, fhi, 1.0))
        for r in range(0, 128, 64):
            c = crow(b1, z, r, 64)
            nb = nbxy(b1, z, r, 64, c, 128) + (crow(b1, z - 1, r, 64) + crow(b1, z + 1, r, 64))
            a1[z, pl.ds(PAD + r, 64), :] = flag * (12.0 * c + nb)

    @pl.loop(0, 6, unroll=2)
    def _(j):
        for r in range(0, 128, 64):
            out = None
            for dz in range(2):
                z = 1 + 2 * j + dz
                c = crow(a1, z, r, 64)
                nb = nbxy(a1, z, r, 64, c, 128) + (crow(a1, z - 1, r, 64) + crow(a1, z + 1, r, 64))
                q = crow(b1, z, r, 64) + N81 * (nb - 6.0 * c)
                out = q if out is None else out + q
            t1[j, pl.ds(r, 64), :] = 0.5 * out

    for p in range(3):
        b2[2 + p, pl.ds(PAD, 64), :] = flag2[2 + p] * (
            split_dot(ypair(t1, 2 * p, 64), m_first) + split_dot(ypair(t1, 2 * p + 1, 64), m_second)
        )
    for p in range(1, 6):
        c = crow(b2, p, 0, 64)
        a2[p, pl.ds(PAD, 64), :] = flag2[p] * (12.0 * c + nb2(b2, p, c))
    for p in range(1, 6):
        w = crow(a2, p, 0, 64)
        t2[p - 1] = crow(b2, p, 0, 64) + N81 * (nb2(a2, p, w) - 6.0 * w)
    tile = None
    for p in range(1, 5):
        part = split_dot(ypair(t2, p, 32), mats[4 + p])
        tile = part if tile is None else tile + part
    t3[d, pl.ds(0, 32), :] = 0.5 * tile
    part = split_dot(ypair(t2, 0, 32), mats[14])
    block8 = lane_iota((8, 128)) // 32
    row = part[0:8]
    for k in range(1, 4):
        row = jnp.where(block8 == k, part[8 * k:8 * k + 8], row)
    t3[d, pl.ds(32, 8), :] = 0.5 * row

    def t3_copy(o):
        to = lax.rem(d + o, gz)
        return remote(t3.at[d], t3.at[d], t3s.at[o], t3r.at[d], gz=to)

    @pl.loop(1, gz)
    def _(o):
        t3_copy(o).start()

    index_copy.wait_recv()
    for far in range(4):
        for side, cond in ((0, even), (1, jnp.logical_not(even))):
            k = far if side == 0 else 3 - far
            if far in (0, 3):
                cond = jnp.logical_and(cond, straight if far == 0 else diagonal)

            def put_other(ph, value):
                fx[k, ph] = value

            @pl.when(cond)
            def _():
                density(k + 4 * side, pidx2, far % 2, put_other)

        crossing(far, begin, True, True if EARLY else straight)
        if far >= 2:
            for side, cond, _, step in relays:
                @pl.when(cond)
                def _():
                    to_relay(side, far, step).start()

    @pl.when(has_lo)
    def _():
        g0_hi.wait_recv()
        s1[5, pl.ds(PAD, 128), :] += g0[0]

    @pl.when(has_hi)
    def _():
        g0_lo.wait_recv()
        s1[8, pl.ds(PAD, 128), :] += g0[1]

    def w1_plane(z, lo, hi):
        for r in range(0, 128, 64):
            c = crow(s1, z, r, 64)
            t = 12.0 * c + nbxy(s1, z, r, 64, c, 128)
            if lo:
                t = t + crow(s1, z - 1, r, 64)
            if hi:
                t = t + crow(s1, z + 1, r, 64)
            a1[z, pl.ds(PAD + r, 64), :] = t

    for z in range(5, 9):
        w1_plane(z, z > 5, z < 8)
    a1[4, pl.ds(PAD, 128), :] = flo * crow(s1, 5, 0, 128)
    a1[9, pl.ds(PAD, 128), :] = fhi * crow(s1, 8, 0, 128)
    for slot, z in ((0, 5), (3, 8)):
        for r in range(0, 128, 64):
            c = crow(s1, z, r, 64)
            t1[slot, pl.ds(r, 64), :] = (0.5 * N81) * (
                nbxy(s1, z, r, 64, c, 128) - 5.0 * c + crow(a1, z, r, 64)
            )
    for slot in (1, 2):
        for r in range(0, 128, 64):
            out = None
            for z in (3 + 2 * slot, 4 + 2 * slot):
                c = crow(a1, z, r, 64)
                nb = nbxy(a1, z, r, 64, c, 128) + (crow(a1, z - 1, r, 64) + crow(a1, z + 1, r, 64))
                q = crow(s1, z, r, 64) + N81 * (nb - 6.0 * c)
                out = q if out is None else out + q
            t1[slot, pl.ds(r, 64), :] = 0.5 * out

    g1o[0] = split_dot(ypair(t1, 0, 64), m_second)
    g1o[1] = split_dot(ypair(t1, 3, 64), m_first)
    g1_lo, g1_hi = exchange(g1o, g1, g1s, g1r)

    @pl.when(has_lo)
    def _():
        g1_lo.start()

    @pl.when(has_hi)
    def _():
        g1_hi.start()

    s2[3, pl.ds(PAD, 64), :] = split_dot(ypair(t1, 1, 64), m_first) + split_dot(ypair(t1, 2, 64), m_second)

    def h1_copy(i):
        here, there, step = ((5, 9, -1), (6, 2, 1))[i]
        to = jnp.clip(d + step, 0, gz - 1)
        return remote(
            s1.at[pl.ds(here, 3), pl.ds(PAD, 128), :], s1.at[pl.ds(there, 3), pl.ds(PAD, 128), :],
            h1s.at[i], h1r.at[i], gz=to,
        )

    h1_sends, h1_recvs = [has_lo, has_hi], [has_hi, has_lo]

    def h1_start():
        for i in range(2):
            @pl.when(h1_sends[i])
            def _():
                h1_copy(i).start()

    h1_start()

    @pl.when(has_lo)
    def _():
        g1_hi.wait_recv()
        s2[3, pl.ds(PAD, 64), :] += g1[0]

    @pl.when(has_hi)
    def _():
        g1_lo.wait_recv()
        s2[3, pl.ds(PAD, 64), :] += g1[1]

    def h2_copy(i):
        step = (-2, -1, 1, 2)[i]
        to = jnp.clip(d + step, 0, gz - 1)
        return remote(
            s2.at[3, pl.ds(PAD, 64), :], s2.at[3 - step, pl.ds(PAD, 64), :], h2s.at[i], h2r.at[i], gz=to
        )

    for i, step in enumerate((-2, -1, 1, 2)):
        @pl.when(inside(step))
        def _():
            h2_copy(i).start()

    crossing(3, begin, False)


    @pl.loop(1, gz)
    def _(o):
        peer = lax.rem(d + o, gz)
        remote(t3.at[peer], t3.at[peer], t3s.at[o], t3r.at[peer], gz=peer).wait_recv()

    if not EARLY:
        crossing(1, begin, True, diagonal)
    for far in (2, 3):
        for side, _, cond, step in relays:
            @pl.when(cond)
            def _():
                to_relay(side, far, step).wait_recv()
                hand_on(side, far).start()

    lane32 = lane_iota((32, 128))
    for q in range(4):
        total = None
        for e in range(max(4 * q - 2, 0), min(4 * q + 6, gz)):
            low, high = max(e - 1 - 4 * q, 0), min(e + 2 - 4 * q, 3)
            parts = []
            if low <= high:
                x = t3[e, pl.ds(0, 32), :]
                if (low, high) != (0, 3):
                    x = jnp.where(jnp.logical_and(lane32 >= 32 * low, lane32 < 32 * high + 32), x, 0.0)
                parts.append(x)
            block = e - 2 - 4 * q
            if 0 <= block < 4:
                x = t3[e, pl.ds(32, 8), :]
                pieces = [jnp.where(block8 == block, roll(x, 32 * (block - k)), 0.0) for k in range(4)]
                parts.append(jnp.concatenate(pieces, axis=0))
            for x in parts:
                total = x if total is None else total + x
        s3[q] = total * NINTH
        a3[q, pl.ds(PAD, 32), :] = total * NINTH

    def sweep3(src, dst):
        v = [crow(src, q, 0, 32) for q in range(4)]
        for q in range(4):
            after = v[q + 1] if q < 3 else jnp.zeros_like(v[0])
            before = v[q - 1] if q > 0 else jnp.zeros_like(v[0])
            nz = roll(jnp.where(lane32 < 32, after, v[q]), -32)
            nz = nz + roll(jnp.where(lane32 >= 96, before, v[q]), 32)
            nb = nbxy(src, q, 0, 32, v[q], 32) + nz
            dst[q, pl.ds(PAD, 32), :] = (1.0 / 3.0) * v[q] + (NINTH * nb + s3[q])

    @pl.loop(0, 3)
    def _(i):
        sweep3(a3, b3)
        sweep3(b3, a3)

    sweep3(a3, b3)

    for i, step in enumerate((-2, -1, 1, 2)):
        @pl.when(inside(-step))
        def _():
            h2_copy(i).wait_recv()

    for p in range(1, 6):
        at = d + p - 3
        q = jnp.clip(at // 4, 0, 3)
        e = split_dot(b3[q, pl.ds(PAD, 32), :], mats[8 + p])
        pe2[p - 1, pl.ds(0, 32, stride=2), :] = e
        pe2[p - 1, pl.ds(1, 32, stride=2), :] = e
    for p in range(1, 6):
        c = crow(s2, p, 0, 64)
        w = 12.0 * c + nb2(s2, p, c)
        a2[p, pl.ds(PAD, 64), :] = flag2[p] * (N81 * w + pe2[p - 1])

    def sweep2(src, dst, p):
        c = crow(src, p, 0, 64)
        dst[p, pl.ds(PAD, 64), :] = flag2[p] * (
            (1.0 / 3.0) * c + NINTH * (nb2(src, p, c) + crow(s2, p, 0, 64))
        )

    for p in range(2, 5):
        sweep2(a2, b2, p)
    for p in range(2, 5):
        sweep2(b2, a2, p)

    for i in range(2):
        @pl.when(h1_recvs[i])
        def _():
            h1_copy(i).wait_recv()

    for j in range(1, 5):
        e = split_dot(a2[2 + j // 2, pl.ds(PAD, 64), :], mats[2 + j % 2])
        pe1[j, pl.ds(0, 64, stride=2), :] = e
        pe1[j, pl.ds(1, 64, stride=2), :] = e

    def in_grid(z):
        return jnp.where(z < 5, flo, jnp.where(z > 8, fhi, 1.0))

    def nb1(ref, z, r, c):
        return nbxy(ref, z, r, 64, c, 128) + (crow(ref, z - 1, r, 64) + crow(ref, z + 1, r, 64))

    @pl.loop(3, 11, unroll=4)
    def _(z):
        flag = in_grid(z)
        for r in range(0, 128, 64):
            c = crow(s1, z, r, 64)
            w = 12.0 * c + nb1(s1, z, r, c)
            a1[z, pl.ds(PAD + r, 64), :] = flag * (N81 * w + pe1[(z - 1) // 2, pl.ds(r, 64), :])

    @pl.loop(4, 10, unroll=3)
    def _(z):
        flag = in_grid(z)
        for r in range(0, 128, 64):
            c = crow(a1, z, r, 64)
            t = nb1(a1, z, r, c) + crow(s1, z, r, 64)
            b1[z, pl.ds(PAD + r, 64), :] = flag * ((1.0 / 3.0) * c + NINTH * t)

    @pl.loop(5, 9, unroll=4)
    def _(z):
        for r in range(0, 128, 64):
            c = crow(b1, z, r, 64)
            t = nb1(b1, z, r, c) + crow(s1, z, r, 64)
            e1[z - 5, pl.ds(r, 64), :] = (1.0 / 3.0) * c + NINTH * t

    e1_lo = remote(
        e1.at[pl.ds(0, 2)], e1h.at[1], e1s.at[0], e1r.at[1], gz=jnp.maximum(d - 1, 0)
    )
    e1_hi = remote(
        e1.at[pl.ds(2, 2)], e1h.at[0], e1s.at[1], e1r.at[0], gz=jnp.minimum(d + 1, gz - 1)
    )

    @pl.when(has_lo)
    def _():
        e1_lo.start()

    @pl.when(has_hi)
    def _():
        e1_hi.start()

    def f_wait(*which):
        @pl.when(has_lo)
        def _():
            for far in which:
                f_copy(1, far, False).wait_recv()

        @pl.when(has_hi)
        def _():
            for far in which:
                f_copy(0, far, False).wait_recv()

    def correct(z, ref, k):
        e = ref[k]
        for ph in range(4):
            a[z, ph, pl.ds(PAD, 128), :] = N81 * a[z, ph, pl.ds(PAD, 128), :] + e

    def sweep0(src, dst, first, last):
        @pl.loop(first + 4, last + 5)
        def _(z):
            for r in range(0, 128, CH):
                c = center(src, z, r, CH)
                nb = nbxy0(src, z, r, CH, c)
                for ph in range(4):
                    t = nb[ph] + (rows(src, z - 1, ph, r, CH) + rows(src, z + 1, ph, r, CH))
                    t = t + rows(f, z, ph, r, CH)
                    dst[z, ph, pl.ds(PAD + r, CH), :] = (1.0 / 3.0) * c[ph] + NINTH * t

    def below(first):
        return jnp.where(has_lo, first, 0)

    def above(last):
        return jnp.where(has_hi, last, 7)

    f_wait(0, 1)
    w_plane(4, True, True)
    w_plane(11, True, True)

    @pl.when(has_hi)
    def _():
        w_plane(12, True, True)

    def products(z, carry):
        plain, edges = carry
        for r in range(0, 128, CH):
            c, src, up = center(a, z, r, CH), center(f, z, r, CH), center(a, z + 1, r, CH)
            for ph in range(4):
                plain = plain + fold(c[ph] * (src[ph] - (3.0 * N81) * c[ph]))
            e = c[0] * c[1] + c[2] * c[3] + (c[0] * c[2] + c[1] * c[3])
            e = e + (c[1] * from_right(c[0]) + c[3] * from_right(c[2]))
            e = e + (c[2] * rows(a, z, 0, r, CH, 1) + c[3] * rows(a, z, 1, r, CH, 1))
            for ph in range(4):
                e = e + c[ph] * up[ph]
            edges = edges + fold(e)
        return plain, edges

    zero = jnp.zeros((8, 128), F32)
    plain, edges = lax.fori_loop(4, 12, products, (zero, zero))
    coarse = zero
    for j in range(4):
        coarse = coarse + fold(s1[5 + j, pl.ds(PAD, 128), :] * e1[j])
    part = (2.0 * N81) * (plain + N81 * edges) + 2.0 * coarse
    prods[d] = part.sum(axis=0, keepdims=True)

    @pl.loop(1, gz)
    def _(o):
        remote(prods.at[d], prods.at[d], ps.at[o], pr.at[d], gz=lax.rem(d + o, gz)).start()


    @pl.loop(0, 8)
    def _(z):
        correct(z + 4, e1, z // 2)

    sweep0(a, b, 1, 6)
    sweep0(b, a, 2, 5)

    f_wait(2, 3)

    @pl.loop(below(-3) + 4, 4)
    def _(z):
        w_plane(z, True, True)

    @pl.loop(12, above(10) + 5)
    def _(z):
        w_plane(z, True, True)

    @pl.when(has_lo)
    def _():
        e1_hi.wait_recv()
        for z in range(-3, 0):
            correct(z + 4, e1h.at[0], (z + 4) // 2)

    @pl.when(has_hi)
    def _():
        e1_lo.wait_recv()
        for z in range(8, 11):
            correct(z + 4, e1h.at[1], (z - 8) // 2)

    sweep0(a, b, below(-2), 0)
    sweep0(a, b, 7, above(9))
    sweep0(b, a, below(-1), 1)
    sweep0(b, a, 6, above(8))

    def final(z, squares):
        for r in range(0, 128, CH):
            c = center(a, z, r, CH)
            nb = nbxy0(a, z, r, CH, c)
            for ph in range(4):
                t = nb[ph] + (rows(a, z - 1, ph, r, CH) + rows(a, z + 1, ph, r, CH))
                left = (rows(f, z, ph, r, CH) - 6.0 * c[ph]) + t
                squares = squares + fold(left * left)
        return squares

    sums[d] = lax.fori_loop(4, 12, final, zero).sum(axis=0, keepdims=True)

    @pl.loop(1, gz)
    def _(o):
        remote(sums.at[d], sums.at[d], ss.at[o], sr.at[d], gz=lax.rem(d + o, gz)).start()

    @pl.loop(1, gz)
    def _(o):
        peer = lax.rem(d + o, gz)
        remote(prods.at[peer], prods.at[peer], ps.at[o], pr.at[peer], gz=peer).wait_recv()

    total = prods[0]
    for e in range(1, gz):
        total = total + prods[e]
    ens[me] = pweight[0, 0] * total

    @pl.loop(1, pairs)
    def _(o):
        remote(ens.at[me], ens.at[me], es.at[o], er.at[me], pair=lax.rem(me + o, pairs)).start()

    px[...] = selection((256, 256), lambda i, j: i == (j & 1) * 128 + (j >> 1))

    @pl.loop(0, 8)
    def _(z):
        for yp in range(2):
            x = jnp.concatenate(
                [a[z + 4, 2 * yp, pl.ds(PAD, 128), :], a[z + 4, 2 * yp + 1, pl.ds(PAD, 128), :]], axis=1
            )
            y = split_dot(x, px[...])
            for half in range(2):
                tmp[z % 2, half, pl.ds(yp, 128, stride=2), :] = y[:, 128 * half:128 * half + 128]
        for half in range(2):
            pot[0, z, :, pl.ds(128 * half, 128)] = tmp[z % 2, half]

    @pl.loop(1, gz)
    def _(o):
        peer = lax.rem(d + o, gz)
        remote(sums.at[peer], sums.at[peer], ss.at[o], sr.at[peer], gz=peer).wait_recv()

    total = sums[0]
    for e in range(1, gz):
        total = total + sums[e]
    cells = 1.0 / (gz * 8 * 256 * 256)
    res_out[...] = jnp.sqrt(jnp.sum(total, axis=1, keepdims=True) * cells)

    @pl.loop(1, pairs)
    def _(o):
        peer = lax.rem(me + o, pairs)
        remote(ens.at[peer], ens.at[peer], es.at[o], er.at[peer], pair=peer).wait_recv()

    energy = ens[0]
    for e in range(1, pairs):
        energy = energy + ens[e]
    en_out[...] = jnp.sum(energy, axis=1, keepdims=True) * (-0.5 * cells)

    for cond, side in ((has_lo, 0), (has_hi, 1)):
        @pl.when(cond)
        def _():
            (g0_lo, g0_hi)[side].wait_send()
            (g1_lo, g1_hi)[side].wait_send()
            (e1_lo, e1_hi)[side].wait_send()

    index_copy.wait_send()
    on_chip(sent)
    for far in range(4):
        crossing(far, sent, True)
    crossing(0, sent, False)
    crossing(3, sent, False)
    for far in (2, 3):
        for side, first, second, step in relays:
            @pl.when(first)
            def _():
                to_relay(side, far, step).wait_send()

            @pl.when(second)
            def _():
                hand_on(side, far).wait_send()

    for i in range(2):
        @pl.when(h1_sends[i])
        def _():
            h1_copy(i).wait_send()

    for i, step in enumerate((-2, -1, 1, 2)):
        @pl.when(inside(step))
        def _():
            h2_copy(i).wait_send()

    @pl.loop(1, gz)
    def _(o):
        t3_copy(o).wait_send()
        remote(sums.at[d], sums.at[d], ss.at[o], sr.at[d], gz=lax.rem(d + o, gz)).wait_send()
        remote(prods.at[d], prods.at[d], ps.at[o], pr.at[d], gz=lax.rem(d + o, gz)).wait_send()

    @pl.loop(1, pairs)
    def _(o):
        remote(ens.at[me], ens.at[me], es.at[o], er.at[me], pair=lax.rem(me + o, pairs)).wait_send()


def solution(mesh):
    gz, pairs = mesh.shape["gz"], mesh.shape["pair"]
    dma, vmem = pltpu.SemaphoreType.DMA, pltpu.VMEM
    field = vmem((16, 4, 144, 128), F32)
    level1, level2, level3 = vmem((14, 144, 128), F32), vmem((7, 80, 128), F32), vmem((4, 48, 128), F32)

    def per_device(orbitals, pair_index, pair_weight):
        potential, norm, energy = pl.pallas_call(
            functools.partial(kernel, gz, pairs),
            out_shape=(
                jax.ShapeDtypeStruct((1, 8, 256, 256), F32),
                jax.ShapeDtypeStruct((1, 1), F32),
                jax.ShapeDtypeStruct((1, 1), F32),
            ),
            in_specs=[
                pl.BlockSpec(memory_space=pltpu.HBM),
                pl.BlockSpec(memory_space=pltpu.HBM),
                pl.BlockSpec(memory_space=pl.ANY),
            ],
            out_specs=(
                pl.BlockSpec(memory_space=pltpu.VMEM),
                pl.BlockSpec(memory_space=pltpu.VMEM),
                pl.BlockSpec(memory_space=pltpu.VMEM),
            ),
            scratch_shapes=[
                *[vmem((8, 256, 256), BF16)] * 8,
                vmem((256, 256), BF16),
                vmem((15, 128, 128), BF16),
                vmem((2, 2, 256, 128), F32),
                pltpu.SMEM((1, 2), jnp.int32),
                pltpu.SMEM((1, 1), F32),
                pltpu.SMEM((1, 2), jnp.int32),
                vmem((4, 4, 128, 128), F32),
                vmem((2, 4, 128, 128), F32),
                field, field, field,
                vmem((2, 128, 128), F32), vmem((2, 128, 128), F32),
                level1, level1, level1,
                vmem((6, 128, 128), F32),
                vmem((2, 64, 128), F32), vmem((2, 64, 128), F32),
                vmem((6, 128, 128), F32),
                vmem((4, 128, 128), F32), vmem((2, 2, 128, 128), F32),
                level2, level2, level2,
                vmem((5, 64, 128), F32),
                vmem((5, 64, 128), F32),
                vmem((gz, 40, 128), F32),
                vmem((4, 32, 128), F32),
                level3, level3,
                vmem((gz, 1, 128), F32), vmem((gz, 1, 128), F32),
                vmem((pairs, 1, 128), F32),
                dma((2,)),
                dma((8,)),
                dma((1,)), dma((1,)),
                dma((2,)), dma((2,)), dma((2,)),
                dma((2, 4)), dma((2, 4)),
                dma((2,)), dma((2,)),
                dma((2,)), dma((2,)),
                dma((2,)), dma((2,)),
                dma((2,)), dma((2,)),
                dma((4,)), dma((4,)),
                dma((gz,)), dma((gz,)),
                dma((gz,)), dma((gz,)),
                dma((gz,)), dma((gz,)),
                dma((pairs,)), dma((pairs,)),
            ],
            compiler_params=pltpu.CompilerParams(
                collective_id=0, has_side_effects=True, vmem_limit_bytes=48 * 1024 * 1024
            ),
            name="vcycle",
        )(pltpu.with_memory_space_constraint(pair_index, pltpu.HBM), pair_weight.reshape(1, 1), orbitals)
        return potential, norm.reshape(1), energy.reshape(1)

    return jax.shard_map(
        per_device,
        mesh=mesh,
        in_specs=(P(None, "gz", None, None), P("pair", None), P("pair")),
        out_specs=(P("pair", "gz", None, None), P("pair"), P()),
        check_vma=False,
    )
```

```python
import functools

import jax
import jax.numpy as jnp
from jax import lax
from jax.experimental import pallas as pl
from jax.experimental.pallas import tpu as pltpu
from jax.sharding import PartitionSpec as P

MESH = pl.DeviceIdType.MESH
F32, BF16 = jnp.float32, jnp.bfloat16
PAD = 8
EARLY = True
CH = 32
NINTH = 1.0 / 9.0
N81 = 1.0 / 81.0


def lane_iota(shape):
    return lax.broadcasted_iota(jnp.int32, shape, len(shape) - 1)


def roll(x, shift):
    return pltpu.roll(x, shift % x.shape[-1], x.ndim - 1)


def from_left(x, width=128):
    return jnp.where(lane_iota(x.shape) % width == 0, 0.0, roll(x, 1))


def from_right(x, width=128):
    return jnp.where(lane_iota(x.shape) % width == width - 1, 0.0, roll(x, -1))


def split_dot(x, m):
    hi = x.astype(BF16)
    rest = x - hi.astype(F32)
    mid = rest.astype(BF16)
    low = (rest - mid.astype(F32)).astype(BF16)
    dot = functools.partial(jnp.dot, preferred_element_type=F32)
    return dot(hi, m) + dot(mid, m) + dot(low, m)


def selection(shape, test):
    a = lax.broadcasted_iota(jnp.int32, shape, 0)
    b = lax.broadcasted_iota(jnp.int32, shape, 1)
    return jnp.where(test(a, b), 1.0, 0.0).astype(BF16)


def fold(x):
    return x.reshape(x.shape[0] // 8, 8, x.shape[1]).sum(axis=0)


def rows(ref, z, ph, r, n, dr=0):
    return ref[z, ph, pl.ds(PAD + r + dr, n), :]


def nbxy0(ref, z, r, n, c):
    out = []
    for yp in range(2):
        for xp in range(2):
            side = c[2 * yp + 1 - xp]
            x = side + (from_right(side) if xp else from_left(side))
            other = 2 * (1 - yp) + xp
            y = c[other] + rows(ref, z, other, r, n, 1 if yp else -1)
            out.append(x + y)
    return out


def phase_sums(ref, z, r, n, c):
    total = (c[0] + c[1]) + (c[2] + c[3])
    shifts = from_left(c[1] + c[3]) + from_right(c[0] + c[2])
    shifts = shifts + (rows(ref, z, 2, r, n, -1) + rows(ref, z, 3, r, n, -1))
    shifts = shifts + (rows(ref, z, 0, r, n, 1) + rows(ref, z, 1, r, n, 1))
    return total, shifts


def center(ref, z, r, n):
    return [rows(ref, z, ph, r, n) for ph in range(4)]


def crow(ref, z, r, n, dr=0):
    return ref[z, pl.ds(PAD + r + dr, n), :]


def nbxy(ref, z, r, n, c, width):
    y = crow(ref, z, r, n, -1) + crow(ref, z, r, n, 1)
    return y + (from_left(c, width) + from_right(c, width))


def kernel(
    gz, pairs,
    index_in, weight_in, orbitals, pot, res_out, en_out,
    orb0, orb1, orb2, orb3, orb4, orb5, orb6, orb7, px, mats, tmp, pidx, pweight, pidx2, fx, relay, f, a, b, g0, g0o, s1, a1, b1, t1, g1, g1o, pe1, e1, e1h,
    s2, a2, b2, t2, pe2, t3, s3, a3, b3, kept, prods, sums, ens,
    scalar_sem, orb_sem, ixs, ixr, ys, yr, yf, fs, fr, g0s, g0r, h1s, h1r, g1s, g1r, e1s, e1r, h2s, h2r, t3s, t3p, t3r, ps, pr, ss, sr, es, er,
):
    d = lax.axis_index("gz")
    me = lax.axis_index("pair")
    has_lo, has_hi = d > 0, d < gz - 1
    flo, fhi = has_lo.astype(F32), has_hi.astype(F32)

    def remote(src, dst, s_sem, r_sem, **to):
        return pltpu.make_async_remote_copy(
            src_ref=src, dst_ref=dst, send_sem=s_sem, recv_sem=r_sem, device_id=to, device_id_type=MESH
        )

    orb = (orb0, orb1, orb2, orb3, orb4, orb5, orb6, orb7)

    def orb_copy(z):
        return pltpu.make_async_copy(orbitals.at[:, z], orb[z], orb_sem.at[z])

    index_load = pltpu.make_async_copy(index_in, pidx, scalar_sem.at[0])
    weight_load = pltpu.make_async_copy(weight_in, pweight, scalar_sem.at[1])
    index_load.start()
    weight_load.start()
    for z in range(8):
        orb_copy(z).start()
    barrier = pltpu.get_barrier_semaphore()

    @pl.loop(1, gz)
    def _(o):
        pl.semaphore_signal(barrier, inc=1, device_id={"gz": lax.rem(d + o, gz)}, device_id_type=MESH)

    @pl.loop(1, pairs)
    def _(o):
        pl.semaphore_signal(barrier, inc=1, device_id={"pair": lax.rem(me + o, pairs)}, device_id_type=MESH)

    other = lax.rem(me + pairs // 2, pairs)
    even = lax.rem(d, 2) == 0
    across = jnp.where(even, d - 1, d + 1)
    has_across = jnp.logical_and(across >= 0, across < gz)

    @pl.when(has_across)
    def _():
        pl.semaphore_signal(barrier, inc=1, device_id={"gz": across, "pair": other}, device_id_type=MESH)

    turn = lax.rem(d, 4)
    straight = jnp.logical_or(turn == 1, turn == 2)
    diagonal = jnp.logical_not(straight)
    partner = jnp.where(turn == 0, d + 3, d - 3)

    @pl.when(diagonal)
    def _():
        pl.semaphore_signal(barrier, inc=1, device_id={"gz": partner, "pair": other}, device_id_type=MESH)

    px[...] = selection((256, 256), lambda i, j: j == (i & 1) * 128 + (i >> 1))
    pad0 = jnp.zeros((4, PAD, 128), F32)
    square = (128, 128)
    mats[0] = selection(square, lambda i, j: (i >> 1) == j)
    mats[1] = selection(square, lambda i, j: (i >> 1) + 64 == j)
    for half in range(2):
        mats[2 + half] = selection(square, lambda i, j: i == (j >> 1) + 64 * half)
    for p in range(5):
        block = lax.rem(d + p - 2 + gz, 4) * 32
        mats[4 + p] = selection(square, lambda i, j: ((i & 63) >> 1) + block == j)
        mats[9 + p] = selection(square, lambda i, j: i == ((j & 63) >> 1) + block)
    mats[14] = selection(square, lambda i, j: ((i & 63) >> 1) == (j & 31))

    @pl.loop(0, 16)
    def _(z):
        for ref in (f, a, b):
            ref[z, :, pl.ds(0, PAD), :] = pad0
            ref[z, :, pl.ds(PAD + 128, PAD), :] = pad0

    def clear_outside(first):
        @pl.loop(first, first + 4)
        def _(z):
            for ref in (f, a, b):
                for ph in range(4):
                    ref[z, ph, pl.ds(PAD, 128), :] = jnp.zeros((128, 128), F32)

        @pl.when(first == 0)
        def _():
            @pl.loop(0, 5)
            def _(z):
                s1[z, pl.ds(PAD, 128), :] = jnp.zeros((128, 128), F32)

        @pl.when(first > 0)
        def _():
            @pl.loop(9, 14)
            def _(z):
                s1[z, pl.ds(PAD, 128), :] = jnp.zeros((128, 128), F32)

    @pl.when(d == 0)
    def _():
        clear_outside(0)
        g0[0] = jnp.zeros((128, 128), F32)
        g1[0] = jnp.zeros((64, 128), F32)

    @pl.when(d == gz - 1)
    def _():
        clear_outside(12)
        g0[1] = jnp.zeros((128, 128), F32)
        g1[1] = jnp.zeros((64, 128), F32)

    @pl.loop(0, 14)
    def _(z):
        s1[z, pl.ds(0, PAD), :] = jnp.zeros((PAD, 128), F32)
        s1[z, pl.ds(PAD + 128, PAD), :] = jnp.zeros((PAD, 128), F32)
        a1[z] = jnp.zeros((144, 128), F32)
        b1[z] = jnp.zeros((144, 128), F32)

    @pl.loop(0, 7)
    def _(p):
        s2[p, pl.ds(0, PAD), :] = jnp.zeros((PAD, 128), F32)
        s2[p, pl.ds(PAD + 64, PAD), :] = jnp.zeros((PAD, 128), F32)
        a2[p] = jnp.zeros((80, 128), F32)
        b2[p] = jnp.zeros((80, 128), F32)
        at = d + p - 3

        @pl.when(jnp.logical_or(jnp.logical_or(at < 0, at >= gz), jnp.logical_or(p == 0, p == 6)))
        def _():
            s2[p, pl.ds(PAD, 64), :] = jnp.zeros((64, 128), F32)

    for q in range(4):
        a3[q] = jnp.zeros((48, 128), F32)
        b3[q] = jnp.zeros((48, 128), F32)

    def density(z, which, slot, put):
        left = jnp.dot(orb[z][which[0, 0]], px[...], preferred_element_type=F32)
        right = jnp.dot(orb[z][which[0, 1]], px[...], preferred_element_type=F32)
        both = left * right
        tmp[slot, 0] = both[:, :128]
        tmp[slot, 1] = both[:, 128:]
        for yp in range(2):
            for xp in range(2):
                put(2 * yp + xp, tmp[slot, xp, pl.ds(yp, 128, stride=2), :])

    index_load.wait()
    weight_load.wait()
    def w_plane(z, lo, hi):
        for r in range(0, 128, CH):
            c = center(f, z, r, CH)
            nb = nbxy0(f, z, r, CH, c)
            for ph in range(4):
                t = 12.0 * c[ph] + nb[ph]
                if lo:
                    t = t + rows(f, z - 1, ph, r, CH)
                if hi:
                    t = t + rows(f, z + 1, ph, r, CH)
                a[z, ph, pl.ds(PAD + r, CH), :] = t

    for i, z in enumerate(range(8)):
        orb_copy(z).wait()

        def put(ph, value):
            f[z + 4, ph, pl.ds(PAD, 128), :] = value

        density(z, pidx, i % 2, put)
        if z:
            w_plane(z + 3, z > 1, True)

    w_plane(11, True, False)

    pl.semaphore_wait(barrier, gz - 1 + pairs - 1 + has_across.astype(jnp.int32) + diagonal.astype(jnp.int32))

    index_copy = remote(pidx, pidx2, ixs.at[0], ixr.at[0], pair=other)
    index_copy.start()

    for side, z in ((0, 4), (1, 11)):
        for r in range(0, 128, CH):
            total, shifts = phase_sums(f, z, r, CH, center(f, z, r, CH))
            w = center(a, z, r, CH)
            g0o[side, pl.ds(r, CH), :] = (0.5 * N81) * (
                shifts - 3.0 * total + ((w[0] + w[1]) + (w[2] + w[3]))
            )

    def exchange(out, landed, s_sems, r_sems):
        lo = remote(out.at[0], landed.at[1], s_sems.at[0], r_sems.at[1], gz=jnp.maximum(d - 1, 0))
        hi = remote(out.at[1], landed.at[0], s_sems.at[1], r_sems.at[0], gz=jnp.minimum(d + 1, gz - 1))
        return lo, hi

    g0_lo, g0_hi = exchange(g0o, g0, g0s, g0r)

    @pl.when(has_lo)
    def _():
        g0_lo.start()

    @pl.when(has_hi)
    def _():
        g0_hi.start()

    def f_copy(side, far, of_other):
        k = far if side == 0 else 3 - far
        here = k if side == 0 else 4 + k
        there = 12 + k if side == 0 else k
        to = jnp.maximum(d - 1, 0) if side == 0 else jnp.minimum(d + 1, gz - 1)
        landed = f.at[there, :, pl.ds(PAD, 128), :]
        if of_other:
            return remote(fx.at[k], landed, fs.at[side, far], fr.at[1 - side, far], gz=to, pair=other)
        return remote(
            f.at[4 + here, :, pl.ds(PAD, 128), :], landed, fs.at[side, far], fr.at[1 - side, far], gz=to, pair=me
        )

    def on_chip(act):
        for side, cond in ((0, jnp.logical_not(even)), (1, even)):
            @pl.when(cond)
            def _():
                for far in range(4):
                    act(side, far, False)

    def crossing(far, act, of_other, only=True):
        kind = {
            (0, False): diagonal, (3, False): straight,
            (0, True): straight, (1, True): True, (2, True): straight,
        }.get((far, of_other))
        if kind is None:
            return
        for side, cond in ((0, jnp.logical_and(even, has_lo)), (1, jnp.logical_and(jnp.logical_not(even), has_hi))):
            @pl.when(jnp.logical_and(cond, jnp.logical_and(kind, only)))
            def _():
                act(side, far, of_other)

    relays = ((0, jnp.logical_and(turn == 0, has_lo), jnp.logical_and(turn == 0, d < gz - 4), -4),
              (1, jnp.logical_and(turn == 3, has_hi), jnp.logical_and(turn == 3, d >= 4), 4))

    def to_relay(side, far, step):
        k = far if side == 0 else 3 - far
        return remote(
            fx.at[k], relay.at[far - 2], ys.at[far - 2], yr.at[far - 2], gz=jnp.clip(d + step, 0, gz - 1), pair=me
        )

    def hand_on(side, far):
        there = 12 + far if side == 0 else 3 - far
        return remote(
            relay.at[far - 2], f.at[there, :, pl.ds(PAD, 128), :], yf.at[far - 2], fr.at[1 - side, far],
            gz=jnp.clip(partner, 0, gz - 1), pair=other,
        )

    def begin(side, far, of_other):
        f_copy(side, far, of_other).start()

    def sent(side, far, of_other):
        f_copy(side, far, of_other).wait_send()

    crossing(0, begin, False)
    on_chip(begin)

    for ph in range(4):
        a[3, ph, pl.ds(PAD, 128), :] = flo * f[4, ph, pl.ds(PAD, 128), :]
        a[12, ph, pl.ds(PAD, 128), :] = fhi * f[11, ph, pl.ds(PAD, 128), :]

    @pl.loop(0, 4)
    def _(j):
        for r in range(0, 128, CH):
            out = None
            for dz in range(2):
                z = 4 + 2 * j + dz
                c = center(a, z, r, CH)
                total, shifts = phase_sums(a, z, r, CH, c)
                below, above, src = center(a, z - 1, r, CH), center(a, z + 1, r, CH), center(f, z, r, CH)
                zs = ((below[0] + below[1]) + (below[2] + below[3])) + (
                    (above[0] + above[1]) + (above[2] + above[3])
                )
                q = ((src[0] + src[1]) + (src[2] + src[3])) + N81 * (zs - 4.0 * total + shifts)
                out = q if out is None else out + q
            s1[5 + j, pl.ds(PAD + r, CH), :] = 0.5 * out
            b1[5 + j, pl.ds(PAD + r, CH), :] = 0.5 * out

    def ypair(ref, slot, n):
        return ref[slot, pl.ds(0, n, stride=2), :] + ref[slot, pl.ds(1, n, stride=2), :]

    def inside(step):
        at = d + step
        return jnp.logical_and(at >= 0, at < gz)

    flag2 = {p: inside(p - 3).astype(F32) for p in range(1, 6)}
    m_first, m_second = mats[0], mats[1]
    low_half = lane_iota((64, 128)) < 64

    def nb2(ref, p, c):
        z = roll(c + jnp.where(low_half, crow(ref, p + 1, 0, 64), crow(ref, p - 1, 0, 64)), 64)
        return nbxy(ref, p, 0, 64, c, 64) + z

    b1[4, pl.ds(PAD, 128), :] = flo * g0o[0]
    b1[9, pl.ds(PAD, 128), :] = fhi * g0o[1]

    @pl.loop(3, 11, unroll=4)
    def _(z):
        flag = jnp.where(z < 5, flo, jnp.where(z > 8, fhi, 1.0))
        for r in range(0, 128, 64):
            c = crow(b1, z, r, 64)
            nb = nbxy(b1, z, r, 64, c, 128) + (crow(b1, z - 1, r, 64) + crow(b1, z + 1, r, 64))
            a1[z, pl.ds(PAD + r, 64), :] = flag * (12.0 * c + nb)

    @pl.loop(0, 6, unroll=2)
    def _(j):
        for r in range(0, 128, 64):
            out = None
            for dz in range(2):
                z = 1 + 2 * j + dz
                c = crow(a1, z, r, 64)
                nb = nbxy(a1, z, r, 64, c, 128) + (crow(a1, z - 1, r, 64) + crow(a1, z + 1, r, 64))
                q = crow(b1, z, r, 64) + N81 * (nb - 6.0 * c)
                out = q if out is None else out + q
            t1[j, pl.ds(r, 64), :] = 0.5 * out

    for p in range(3):
        b2[2 + p, pl.ds(PAD, 64), :] = flag2[2 + p] * (
            split_dot(ypair(t1, 2 * p, 64), m_first) + split_dot(ypair(t1, 2 * p + 1, 64), m_second)
        )
    for p in range(1, 6):
        c = crow(b2, p, 0, 64)
        a2[p, pl.ds(PAD, 64), :] = flag2[p] * (12.0 * c + nb2(b2, p, c))
    for p in range(1, 6):
        w = crow(a2, p, 0, 64)
        t2[p - 1] = crow(b2, p, 0, 64) + N81 * (nb2(a2, p, w) - 6.0 * w)
    tile = None
    for p in range(1, 5):
        part = split_dot(ypair(t2, p, 32), mats[4 + p])
        tile = part if tile is None else tile + part
    t3[d, pl.ds(0, 32), :] = 0.5 * tile
    part = split_dot(ypair(t2, 0, 32), mats[14])
    block8 = lane_iota((8, 128)) // 32
    row = part[0:8]
    for k in range(1, 4):
        row = jnp.where(block8 == k, part[8 * k:8 * k + 8], row)
    t3[d, pl.ds(32, 8), :] = 0.5 * row

    beside = jnp.where(even, d + 1, d - 1)

    def t3_copy(o):
        return remote(t3.at[d], t3.at[d], t3s.at[o], t3r.at[d], gz=lax.rem(d + 2 * o, gz))

    def t3_pass(o):
        e = lax.rem(d + 2 * o, gz)
        return remote(t3.at[e], t3.at[e], t3p.at[o], t3r.at[e], gz=beside)

    @pl.loop(1, gz // 2)
    def _(o):
        t3_copy(o).start()

    t3_pass(0).start()

    index_copy.wait_recv()
    for far in range(4):
        for side, cond in ((0, even), (1, jnp.logical_not(even))):
            k = far if side == 0 else 3 - far
            if far in (0, 3):
                cond = jnp.logical_and(cond, straight if far == 0 else diagonal)

            def put_other(ph, value):
                fx[k, ph] = value

            @pl.when(cond)
            def _():
                density(k + 4 * side, pidx2, far % 2, put_other)

        crossing(far, begin, True, True if EARLY else straight)
        if far >= 2:
            for side, cond, _, step in relays:
                @pl.when(cond)
                def _():
                    to_relay(side, far, step).start()

    @pl.when(has_lo)
    def _():
        g0_hi.wait_recv()
        s1[5, pl.ds(PAD, 128), :] += g0[0]

    @pl.when(has_hi)
    def _():
        g0_lo.wait_recv()
        s1[8, pl.ds(PAD, 128), :] += g0[1]

    def w1_plane(z, lo, hi):
        for r in range(0, 128, 64):
            c = crow(s1, z, r, 64)
            t = 12.0 * c + nbxy(s1, z, r, 64, c, 128)
            if lo:
                t = t + crow(s1, z - 1, r, 64)
            if hi:
                t = t + crow(s1, z + 1, r, 64)
            a1[z, pl.ds(PAD + r, 64), :] = t

    for z in range(5, 9):
        w1_plane(z, z > 5, z < 8)
    a1[4, pl.ds(PAD, 128), :] = flo * crow(s1, 5, 0, 128)
    a1[9, pl.ds(PAD, 128), :] = fhi * crow(s1, 8, 0, 128)
    for slot, z in ((0, 5), (3, 8)):
        for r in range(0, 128, 64):
            c = crow(s1, z, r, 64)
            t1[slot, pl.ds(r, 64), :] = (0.5 * N81) * (
                nbxy(s1, z, r, 64, c, 128) - 5.0 * c + crow(a1, z, r, 64)
            )
    for slot in (1, 2):
        for r in range(0, 128, 64):
            out = None
            for z in (3 + 2 * slot, 4 + 2 * slot):
                c = crow(a1, z, r, 64)
                nb = nbxy(a1, z, r, 64, c, 128) + (crow(a1, z - 1, r, 64) + crow(a1, z + 1, r, 64))
                q = crow(s1, z, r, 64) + N81 * (nb - 6.0 * c)
                out = q if out is None else out + q
            t1[slot, pl.ds(r, 64), :] = 0.5 * out

    g1o[0] = split_dot(ypair(t1, 0, 64), m_second)
    g1o[1] = split_dot(ypair(t1, 3, 64), m_first)
    g1_lo, g1_hi = exchange(g1o, g1, g1s, g1r)

    @pl.when(has_lo)
    def _():
        g1_lo.start()

    @pl.when(has_hi)
    def _():
        g1_hi.start()

    s2[3, pl.ds(PAD, 64), :] = split_dot(ypair(t1, 1, 64), m_first) + split_dot(ypair(t1, 2, 64), m_second)

    def h1_copy(i):
        here, there, step = ((5, 9, -1), (6, 2, 1))[i]
        to = jnp.clip(d + step, 0, gz - 1)
        return remote(
            s1.at[pl.ds(here, 3), pl.ds(PAD, 128), :], s1.at[pl.ds(there, 3), pl.ds(PAD, 128), :],
            h1s.at[i], h1r.at[i], gz=to,
        )

    h1_sends, h1_recvs = [has_lo, has_hi], [has_hi, has_lo]

    def h1_start():
        for i in range(2):
            @pl.when(h1_sends[i])
            def _():
                h1_copy(i).start()

    h1_start()

    @pl.loop(1, gz // 2)
    def _(o):
        e = lax.rem(d + 2 * o, gz)
        remote(t3.at[e], t3.at[e], t3s.at[o], t3r.at[e], gz=e).wait_recv()
        t3_pass(o).start()

    @pl.when(has_lo)
    def _():
        g1_hi.wait_recv()
        s2[3, pl.ds(PAD, 64), :] += g1[0]

    @pl.when(has_hi)
    def _():
        g1_lo.wait_recv()
        s2[3, pl.ds(PAD, 64), :] += g1[1]

    def h2_copy(i):
        step = (-2, -1, 1, 2)[i]
        to = jnp.clip(d + step, 0, gz - 1)
        return remote(
            s2.at[3, pl.ds(PAD, 64), :], s2.at[3 - step, pl.ds(PAD, 64), :], h2s.at[i], h2r.at[i], gz=to
        )

    for i, step in enumerate((-2, -1, 1, 2)):
        @pl.when(inside(step))
        def _():
            h2_copy(i).start()

    crossing(3, begin, False)


    @pl.loop(0, gz // 2)
    def _(o):
        e = lax.rem(beside + 2 * o, gz)
        remote(t3.at[e], t3.at[e], t3p.at[o], t3r.at[e], gz=beside).wait_recv()

    if not EARLY:
        crossing(1, begin, True, diagonal)
    for far in (2, 3):
        for side, _, cond, step in relays:
            @pl.when(cond)
            def _():
                to_relay(side, far, step).wait_recv()
                hand_on(side, far).start()

    lane32 = lane_iota((32, 128))
    for q in range(4):
        total = None
        for e in range(max(4 * q - 2, 0), min(4 * q + 6, gz)):
            low, high = max(e - 1 - 4 * q, 0), min(e + 2 - 4 * q, 3)
            parts = []
            if low <= high:
                x = t3[e, pl.ds(0, 32), :]
                if (low, high) != (0, 3):
                    x = jnp.where(jnp.logical_and(lane32 >= 32 * low, lane32 < 32 * high + 32), x, 0.0)
                parts.append(x)
            block = e - 2 - 4 * q
            if 0 <= block < 4:
                x = t3[e, pl.ds(32, 8), :]
                pieces = [jnp.where(block8 == block, roll(x, 32 * (block - k)), 0.0) for k in range(4)]
                parts.append(jnp.concatenate(pieces, axis=0))
            for x in parts:
                total = x if total is None else total + x
        s3[q] = total * NINTH
        a3[q, pl.ds(PAD, 32), :] = total * NINTH

    def sweep3(src, dst):
        v = [crow(src, q, 0, 32) for q in range(4)]
        for q in range(4):
            after = v[q + 1] if q < 3 else jnp.zeros_like(v[0])
            before = v[q - 1] if q > 0 else jnp.zeros_like(v[0])
            nz = roll(jnp.where(lane32 < 32, after, v[q]), -32)
            nz = nz + roll(jnp.where(lane32 >= 96, before, v[q]), 32)
            nb = nbxy(src, q, 0, 32, v[q], 32) + nz
            dst[q, pl.ds(PAD, 32), :] = (1.0 / 3.0) * v[q] + (NINTH * nb + s3[q])

    @pl.loop(0, 3)
    def _(i):
        sweep3(a3, b3)
        sweep3(b3, a3)

    sweep3(a3, b3)

    def f_wait(*which):
        @pl.when(has_lo)
        def _():
            for far in which:
                f_copy(1, far, False).wait_recv()

        @pl.when(has_hi)
        def _():
            for far in which:
                f_copy(0, far, False).wait_recv()

    f_wait(0, 1)
    w_plane(4, True, True)
    w_plane(11, True, True)

    @pl.when(has_hi)
    def _():
        w_plane(12, True, True)

    def products(z, carry):
        plain, edges = carry
        for r in range(0, 128, CH):
            c, src, up = center(a, z, r, CH), center(f, z, r, CH), center(a, z + 1, r, CH)
            for ph in range(4):
                plain = plain + fold(c[ph] * (src[ph] - (3.0 * N81) * c[ph]))
            e = c[0] * c[1] + c[2] * c[3] + (c[0] * c[2] + c[1] * c[3])
            e = e + (c[1] * from_right(c[0]) + c[3] * from_right(c[2]))
            e = e + (c[2] * rows(a, z, 0, r, CH, 1) + c[3] * rows(a, z, 1, r, CH, 1))
            for ph in range(4):
                e = e + c[ph] * up[ph]
            edges = edges + fold(e)
        return plain, edges

    zero = jnp.zeros((8, 128), F32)
    plain, edges = lax.fori_loop(4, 12, products, (zero, zero))
    kept[0] = plain
    kept[1] = edges

    for i, step in enumerate((-2, -1, 1, 2)):
        @pl.when(inside(-step))
        def _():
            h2_copy(i).wait_recv()

    for p in range(1, 6):
        at = d + p - 3
        q = jnp.clip(at // 4, 0, 3)
        e = split_dot(b3[q, pl.ds(PAD, 32), :], mats[8 + p])
        pe2[p - 1, pl.ds(0, 32, stride=2), :] = e
        pe2[p - 1, pl.ds(1, 32, stride=2), :] = e
    for p in range(1, 6):
        c = crow(s2, p, 0, 64)
        w = 12.0 * c + nb2(s2, p, c)
        a2[p, pl.ds(PAD, 64), :] = flag2[p] * (N81 * w + pe2[p - 1])

    def sweep2(src, dst, p):
        c = crow(src, p, 0, 64)
        dst[p, pl.ds(PAD, 64), :] = flag2[p] * (
            (1.0 / 3.0) * c + NINTH * (nb2(src, p, c) + crow(s2, p, 0, 64))
        )

    for p in range(2, 5):
        sweep2(a2, b2, p)
    for p in range(2, 5):
        sweep2(b2, a2, p)

    for i in range(2):
        @pl.when(h1_recvs[i])
        def _():
            h1_copy(i).wait_recv()

    for j in range(1, 5):
        e = split_dot(a2[2 + j // 2, pl.ds(PAD, 64), :], mats[2 + j % 2])
        pe1[j, pl.ds(0, 64, stride=2), :] = e
        pe1[j, pl.ds(1, 64, stride=2), :] = e

    def in_grid(z):
        return jnp.where(z < 5, flo, jnp.where(z > 8, fhi, 1.0))

    def nb1(ref, z, r, c):
        return nbxy(ref, z, r, 64, c, 128) + (crow(ref, z - 1, r, 64) + crow(ref, z + 1, r, 64))

    @pl.loop(3, 11, unroll=4)
    def _(z):
        flag = in_grid(z)
        for r in range(0, 128, 64):
            c = crow(s1, z, r, 64)
            w = 12.0 * c + nb1(s1, z, r, c)
            a1[z, pl.ds(PAD + r, 64), :] = flag * (N81 * w + pe1[(z - 1) // 2, pl.ds(r, 64), :])

    @pl.loop(4, 10, unroll=3)
    def _(z):
        flag = in_grid(z)
        for r in range(0, 128, 64):
            c = crow(a1, z, r, 64)
            t = nb1(a1, z, r, c) + crow(s1, z, r, 64)
            b1[z, pl.ds(PAD + r, 64), :] = flag * ((1.0 / 3.0) * c + NINTH * t)

    @pl.loop(5, 9, unroll=4)
    def _(z):
        for r in range(0, 128, 64):
            c = crow(b1, z, r, 64)
            t = nb1(b1, z, r, c) + crow(s1, z, r, 64)
            e1[z - 5, pl.ds(r, 64), :] = (1.0 / 3.0) * c + NINTH * t

    e1_lo = remote(
        e1.at[pl.ds(0, 2)], e1h.at[1], e1s.at[0], e1r.at[1], gz=jnp.maximum(d - 1, 0)
    )
    e1_hi = remote(
        e1.at[pl.ds(2, 2)], e1h.at[0], e1s.at[1], e1r.at[0], gz=jnp.minimum(d + 1, gz - 1)
    )

    @pl.when(has_lo)
    def _():
        e1_lo.start()

    @pl.when(has_hi)
    def _():
        e1_hi.start()

    def correct(z, ref, k):
        e = ref[k]
        for ph in range(4):
            a[z, ph, pl.ds(PAD, 128), :] = N81 * a[z, ph, pl.ds(PAD, 128), :] + e

    def sweep0(src, dst, first, last):
        @pl.loop(first + 4, last + 5)
        def _(z):
            for r in range(0, 128, CH):
                c = center(src, z, r, CH)
                nb = nbxy0(src, z, r, CH, c)
                for ph in range(4):
                    t = nb[ph] + (rows(src, z - 1, ph, r, CH) + rows(src, z + 1, ph, r, CH))
                    t = t + rows(f, z, ph, r, CH)
                    dst[z, ph, pl.ds(PAD + r, CH), :] = (1.0 / 3.0) * c[ph] + NINTH * t

    def below(first):
        return jnp.where(has_lo, first, 0)

    def above(last):
        return jnp.where(has_hi, last, 7)

    plain, edges = kept[0], kept[1]
    coarse = zero
    for j in range(4):
        coarse = coarse + fold(s1[5 + j, pl.ds(PAD, 128), :] * e1[j])
    part = (2.0 * N81) * (plain + N81 * edges) + 2.0 * coarse
    prods[d] = part.sum(axis=0, keepdims=True)

    @pl.loop(1, gz)
    def _(o):
        remote(prods.at[d], prods.at[d], ps.at[o], pr.at[d], gz=lax.rem(d + o, gz)).start()


    @pl.loop(0, 8)
    def _(z):
        correct(z + 4, e1, z // 2)

    sweep0(a, b, 1, 6)
    sweep0(b, a, 2, 5)

    f_wait(2, 3)

    @pl.loop(below(-3) + 4, 4)
    def _(z):
        w_plane(z, True, True)

    @pl.loop(12, above(10) + 5)
    def _(z):
        w_plane(z, True, True)

    @pl.when(has_lo)
    def _():
        e1_hi.wait_recv()
        for z in range(-3, 0):
            correct(z + 4, e1h.at[0], (z + 4) // 2)

    @pl.when(has_hi)
    def _():
        e1_lo.wait_recv()
        for z in range(8, 11):
            correct(z + 4, e1h.at[1], (z - 8) // 2)

    sweep0(a, b, below(-2), 0)
    sweep0(a, b, 7, above(9))
    sweep0(b, a, below(-1), 1)
    sweep0(b, a, 6, above(8))

    def final(z, squares):
        for r in range(0, 128, CH):
            c = center(a, z, r, CH)
            nb = nbxy0(a, z, r, CH, c)
            for ph in range(4):
                t = nb[ph] + (rows(a, z - 1, ph, r, CH) + rows(a, z + 1, ph, r, CH))
                left = (rows(f, z, ph, r, CH) - 6.0 * c[ph]) + t
                squares = squares + fold(left * left)
        return squares

    sums[d] = lax.fori_loop(4, 12, final, zero).sum(axis=0, keepdims=True)

    @pl.loop(1, gz)
    def _(o):
        remote(sums.at[d], sums.at[d], ss.at[o], sr.at[d], gz=lax.rem(d + o, gz)).start()

    @pl.loop(1, gz)
    def _(o):
        peer = lax.rem(d + o, gz)
        remote(prods.at[peer], prods.at[peer], ps.at[o], pr.at[peer], gz=peer).wait_recv()

    total = prods[0]
    for e in range(1, gz):
        total = total + prods[e]
    ens[me] = pweight[0, 0] * total

    @pl.loop(1, pairs)
    def _(o):
        remote(ens.at[me], ens.at[me], es.at[o], er.at[me], pair=lax.rem(me + o, pairs)).start()

    px[...] = selection((256, 256), lambda i, j: i == (j & 1) * 128 + (j >> 1))

    @pl.loop(0, 8)
    def _(z):
        for yp in range(2):
            x = jnp.concatenate(
                [a[z + 4, 2 * yp, pl.ds(PAD, 128), :], a[z + 4, 2 * yp + 1, pl.ds(PAD, 128), :]], axis=1
            )
            y = split_dot(x, px[...])
            for half in range(2):
                tmp[z % 2, half, pl.ds(yp, 128, stride=2), :] = y[:, 128 * half:128 * half + 128]
        for half in range(2):
            pot[0, z, :, pl.ds(128 * half, 128)] = tmp[z % 2, half]

    @pl.loop(1, gz)
    def _(o):
        peer = lax.rem(d + o, gz)
        remote(sums.at[peer], sums.at[peer], ss.at[o], sr.at[peer], gz=peer).wait_recv()

    total = sums[0]
    for e in range(1, gz):
        total = total + sums[e]
    cells = 1.0 / (gz * 8 * 256 * 256)
    res_out[...] = jnp.sqrt(jnp.sum(total, axis=1, keepdims=True) * cells)

    @pl.loop(1, pairs)
    def _(o):
        peer = lax.rem(me + o, pairs)
        remote(ens.at[peer], ens.at[peer], es.at[o], er.at[peer], pair=peer).wait_recv()

    energy = ens[0]
    for e in range(1, pairs):
        energy = energy + ens[e]
    en_out[...] = jnp.sum(energy, axis=1, keepdims=True) * (-0.5 * cells)

    for cond, side in ((has_lo, 0), (has_hi, 1)):
        @pl.when(cond)
        def _():
            (g0_lo, g0_hi)[side].wait_send()
            (g1_lo, g1_hi)[side].wait_send()
            (e1_lo, e1_hi)[side].wait_send()

    index_copy.wait_send()
    on_chip(sent)
    for far in range(4):
        crossing(far, sent, True)
    crossing(0, sent, False)
    crossing(3, sent, False)
    for far in (2, 3):
        for side, first, second, step in relays:
            @pl.when(first)
            def _():
                to_relay(side, far, step).wait_send()

            @pl.when(second)
            def _():
                hand_on(side, far).wait_send()

    for i in range(2):
        @pl.when(h1_sends[i])
        def _():
            h1_copy(i).wait_send()

    for i, step in enumerate((-2, -1, 1, 2)):
        @pl.when(inside(step))
        def _():
            h2_copy(i).wait_send()

    @pl.loop(1, gz)
    def _(o):
        remote(sums.at[d], sums.at[d], ss.at[o], sr.at[d], gz=lax.rem(d + o, gz)).wait_send()
        remote(prods.at[d], prods.at[d], ps.at[o], pr.at[d], gz=lax.rem(d + o, gz)).wait_send()

    @pl.loop(1, gz // 2)
    def _(o):
        t3_copy(o).wait_send()

    @pl.loop(0, gz // 2)
    def _(o):
        t3_pass(o).wait_send()

    @pl.loop(1, pairs)
    def _(o):
        remote(ens.at[me], ens.at[me], es.at[o], er.at[me], pair=lax.rem(me + o, pairs)).wait_send()


def solution(mesh):
    gz, pairs = mesh.shape["gz"], mesh.shape["pair"]
    dma, vmem = pltpu.SemaphoreType.DMA, pltpu.VMEM
    field = vmem((16, 4, 144, 128), F32)
    level1, level2, level3 = vmem((14, 144, 128), F32), vmem((7, 80, 128), F32), vmem((4, 48, 128), F32)

    def per_device(orbitals, pair_index, pair_weight):
        potential, norm, energy = pl.pallas_call(
            functools.partial(kernel, gz, pairs),
            out_shape=(
                jax.ShapeDtypeStruct((1, 8, 256, 256), F32),
                jax.ShapeDtypeStruct((1, 1), F32),
                jax.ShapeDtypeStruct((1, 1), F32),
            ),
            in_specs=[
                pl.BlockSpec(memory_space=pltpu.HBM),
                pl.BlockSpec(memory_space=pltpu.HBM),
                pl.BlockSpec(memory_space=pl.ANY),
            ],
            out_specs=(
                pl.BlockSpec(memory_space=pltpu.VMEM),
                pl.BlockSpec(memory_space=pltpu.VMEM),
                pl.BlockSpec(memory_space=pltpu.VMEM),
            ),
            scratch_shapes=[
                *[vmem((8, 256, 256), BF16)] * 8,
                vmem((256, 256), BF16),
                vmem((15, 128, 128), BF16),
                vmem((2, 2, 256, 128), F32),
                pltpu.SMEM((1, 2), jnp.int32),
                pltpu.SMEM((1, 1), F32),
                pltpu.SMEM((1, 2), jnp.int32),
                vmem((4, 4, 128, 128), F32),
                vmem((2, 4, 128, 128), F32),
                field, field, field,
                vmem((2, 128, 128), F32), vmem((2, 128, 128), F32),
                level1, level1, level1,
                vmem((6, 128, 128), F32),
                vmem((2, 64, 128), F32), vmem((2, 64, 128), F32),
                vmem((6, 128, 128), F32),
                vmem((4, 128, 128), F32), vmem((2, 2, 128, 128), F32),
                level2, level2, level2,
                vmem((5, 64, 128), F32),
                vmem((5, 64, 128), F32),
                vmem((gz, 40, 128), F32),
                vmem((4, 32, 128), F32),
                level3, level3,
                vmem((2, 8, 128), F32),
                vmem((gz, 1, 128), F32), vmem((gz, 1, 128), F32),
                vmem((pairs, 1, 128), F32),
                dma((2,)),
                dma((8,)),
                dma((1,)), dma((1,)),
                dma((2,)), dma((2,)), dma((2,)),
                dma((2, 4)), dma((2, 4)),
                dma((2,)), dma((2,)),
                dma((2,)), dma((2,)),
                dma((2,)), dma((2,)),
                dma((2,)), dma((2,)),
                dma((4,)), dma((4,)),
                dma((gz,)), dma((gz,)), dma((gz,)),
                dma((gz,)), dma((gz,)),
                dma((gz,)), dma((gz,)),
                dma((pairs,)), dma((pairs,)),
            ],
            compiler_params=pltpu.CompilerParams(
                collective_id=0, has_side_effects=True, vmem_limit_bytes=48 * 1024 * 1024
            ),
            name="vcycle",
        )(pltpu.with_memory_space_constraint(pair_index, pltpu.HBM), pair_weight.reshape(1, 1), orbitals)
        return potential, norm.reshape(1), energy.reshape(1)

    return jax.shard_map(
        per_device,
        mesh=mesh,
        in_specs=(P(None, "gz", None, None), P("pair", None), P("pair")),
        out_specs=(P("pair", "gz", None, None), P("pair"), P()),
        check_vma=False,
    )
```

```python
import functools

import jax
import jax.numpy as jnp
from jax import lax
from jax.experimental import pallas as pl
from jax.experimental.pallas import tpu as pltpu
from jax.sharding import PartitionSpec as P

MESH = pl.DeviceIdType.MESH
F32, BF16 = jnp.float32, jnp.bfloat16
PAD = 8
EARLY = True
CH = 32
NINTH = 1.0 / 9.0
N81 = 1.0 / 81.0


def lane_iota(shape):
    return lax.broadcasted_iota(jnp.int32, shape, len(shape) - 1)


def roll(x, shift):
    return pltpu.roll(x, shift % x.shape[-1], x.ndim - 1)


def from_left(x, width=128):
    return jnp.where(lane_iota(x.shape) % width == 0, 0.0, roll(x, 1))


def from_right(x, width=128):
    return jnp.where(lane_iota(x.shape) % width == width - 1, 0.0, roll(x, -1))


def split_dot(x, m):
    hi = x.astype(BF16)
    rest = x - hi.astype(F32)
    mid = rest.astype(BF16)
    low = (rest - mid.astype(F32)).astype(BF16)
    dot = functools.partial(jnp.dot, preferred_element_type=F32)
    return dot(hi, m) + dot(mid, m) + dot(low, m)


def selection(shape, test):
    a = lax.broadcasted_iota(jnp.int32, shape, 0)
    b = lax.broadcasted_iota(jnp.int32, shape, 1)
    return jnp.where(test(a, b), 1.0, 0.0).astype(BF16)


def fold(x):
    return x.reshape(x.shape[0] // 8, 8, x.shape[1]).sum(axis=0)


def rows(ref, z, ph, r, n, dr=0):
    return ref[z, ph, pl.ds(PAD + r + dr, n), :]


def nbxy0(ref, z, r, n, c):
    out = []
    for yp in range(2):
        for xp in range(2):
            side = c[2 * yp + 1 - xp]
            x = side + (from_right(side) if xp else from_left(side))
            other = 2 * (1 - yp) + xp
            y = c[other] + rows(ref, z, other, r, n, 1 if yp else -1)
            out.append(x + y)
    return out


def phase_sums(ref, z, r, n, c):
    total = (c[0] + c[1]) + (c[2] + c[3])
    shifts = from_left(c[1] + c[3]) + from_right(c[0] + c[2])
    shifts = shifts + (rows(ref, z, 2, r, n, -1) + rows(ref, z, 3, r, n, -1))
    shifts = shifts + (rows(ref, z, 0, r, n, 1) + rows(ref, z, 1, r, n, 1))
    return total, shifts


def center(ref, z, r, n):
    return [rows(ref, z, ph, r, n) for ph in range(4)]


def crow(ref, z, r, n, dr=0):
    return ref[z, pl.ds(PAD + r + dr, n), :]


def nbxy(ref, z, r, n, c, width):
    y = crow(ref, z, r, n, -1) + crow(ref, z, r, n, 1)
    return y + (from_left(c, width) + from_right(c, width))


def kernel(
    gz, pairs,
    index_in, weight_in, orbitals, pot, stats,
    orb0, orb1, orb2, orb3, orb4, orb5, orb6, orb7, px, mats, tmp, pidx, pweight, pidx2, fx, relay, f, a, b, g0, g0o, s1, a1, b1, t1, g1, g1o, pe1, e1, e1h,
    s2, a2, b2, t2, pe2, t3, s3, a3, b3, kept, prods, sums, ens,
    scalar_sem, orb_sem, ixs, ixr, ys, yr, yf, fs, fr, g0s, g0r, h1s, h1r, g1s, g1r, e1s, e1r, h2s, h2r, t3s, t3p, t3r, ps, pr, ss, sr, es, er,
):
    d = lax.axis_index("gz")
    me = lax.axis_index("pair")
    has_lo, has_hi = d > 0, d < gz - 1
    flo, fhi = has_lo.astype(F32), has_hi.astype(F32)

    def remote(src, dst, s_sem, r_sem, **to):
        return pltpu.make_async_remote_copy(
            src_ref=src, dst_ref=dst, send_sem=s_sem, recv_sem=r_sem, device_id=to, device_id_type=MESH
        )

    orb = (orb0, orb1, orb2, orb3, orb4, orb5, orb6, orb7)

    def orb_copy(z):
        return pltpu.make_async_copy(orbitals.at[:, z], orb[z], orb_sem.at[z])

    index_load = pltpu.make_async_copy(index_in, pidx, scalar_sem.at[0])
    weight_load = pltpu.make_async_copy(weight_in, pweight, scalar_sem.at[1])
    index_load.start()
    weight_load.start()
    for z in range(8):
        orb_copy(z).start()
    barrier = pltpu.get_barrier_semaphore()

    @pl.loop(1, gz)
    def _(o):
        pl.semaphore_signal(barrier, inc=1, device_id={"gz": lax.rem(d + o, gz)}, device_id_type=MESH)

    @pl.loop(1, pairs)
    def _(o):
        pl.semaphore_signal(barrier, inc=1, device_id={"pair": lax.rem(me + o, pairs)}, device_id_type=MESH)

    other = lax.rem(me + pairs // 2, pairs)
    even = lax.rem(d, 2) == 0
    across = jnp.where(even, d - 1, d + 1)
    has_across = jnp.logical_and(across >= 0, across < gz)

    @pl.when(has_across)
    def _():
        pl.semaphore_signal(barrier, inc=1, device_id={"gz": across, "pair": other}, device_id_type=MESH)

    turn = lax.rem(d, 4)
    straight = jnp.logical_or(turn == 1, turn == 2)
    diagonal = jnp.logical_not(straight)
    partner = jnp.where(turn == 0, d + 3, d - 3)

    @pl.when(diagonal)
    def _():
        pl.semaphore_signal(barrier, inc=1, device_id={"gz": partner, "pair": other}, device_id_type=MESH)

    px[...] = selection((256, 256), lambda i, j: j == (i & 1) * 128 + (i >> 1))
    pad0 = jnp.zeros((4, PAD, 128), F32)
    square = (128, 128)
    mats[0] = selection(square, lambda i, j: (i >> 1) == j)
    mats[1] = selection(square, lambda i, j: (i >> 1) + 64 == j)
    for half in range(2):
        mats[2 + half] = selection(square, lambda i, j: i == (j >> 1) + 64 * half)
    for p in range(5):
        block = lax.rem(d + p - 2 + gz, 4) * 32
        mats[4 + p] = selection(square, lambda i, j: ((i & 63) >> 1) + block == j)
        mats[9 + p] = selection(square, lambda i, j: i == ((j & 63) >> 1) + block)
    mats[14] = selection(square, lambda i, j: ((i & 63) >> 1) == (j & 31))

    @pl.loop(0, 16)
    def _(z):
        for ref in (f, a, b):
            ref[z, :, pl.ds(0, PAD), :] = pad0
            ref[z, :, pl.ds(PAD + 128, PAD), :] = pad0

    def clear_outside(first):
        @pl.loop(first, first + 4)
        def _(z):
            for ref in (f, a, b):
                for ph in range(4):
                    ref[z, ph, pl.ds(PAD, 128), :] = jnp.zeros((128, 128), F32)

        @pl.when(first == 0)
        def _():
            @pl.loop(0, 5)
            def _(z):
                s1[z, pl.ds(PAD, 128), :] = jnp.zeros((128, 128), F32)

        @pl.when(first > 0)
        def _():
            @pl.loop(9, 14)
            def _(z):
                s1[z, pl.ds(PAD, 128), :] = jnp.zeros((128, 128), F32)

    @pl.when(d == 0)
    def _():
        clear_outside(0)
        g0[0] = jnp.zeros((128, 128), F32)
        g1[0] = jnp.zeros((64, 128), F32)

    @pl.when(d == gz - 1)
    def _():
        clear_outside(12)
        g0[1] = jnp.zeros((128, 128), F32)
        g1[1] = jnp.zeros((64, 128), F32)

    @pl.loop(0, 14)
    def _(z):
        s1[z, pl.ds(0, PAD), :] = jnp.zeros((PAD, 128), F32)
        s1[z, pl.ds(PAD + 128, PAD), :] = jnp.zeros((PAD, 128), F32)
        a1[z] = jnp.zeros((144, 128), F32)
        b1[z] = jnp.zeros((144, 128), F32)

    @pl.loop(0, 7)
    def _(p):
        s2[p, pl.ds(0, PAD), :] = jnp.zeros((PAD, 128), F32)
        s2[p, pl.ds(PAD + 64, PAD), :] = jnp.zeros((PAD, 128), F32)
        a2[p] = jnp.zeros((80, 128), F32)
        b2[p] = jnp.zeros((80, 128), F32)
        at = d + p - 3

        @pl.when(jnp.logical_or(jnp.logical_or(at < 0, at >= gz), jnp.logical_or(p == 0, p == 6)))
        def _():
            s2[p, pl.ds(PAD, 64), :] = jnp.zeros((64, 128), F32)

    for q in range(4):
        a3[q] = jnp.zeros((48, 128), F32)
        b3[q] = jnp.zeros((48, 128), F32)

    def density(z, which, slot, put):
        left = jnp.dot(orb[z][which[0, 0]], px[...], preferred_element_type=F32)
        right = jnp.dot(orb[z][which[0, 1]], px[...], preferred_element_type=F32)
        both = left * right
        tmp[slot, 0] = both[:, :128]
        tmp[slot, 1] = both[:, 128:]
        for yp in range(2):
            for xp in range(2):
                put(2 * yp + xp, tmp[slot, xp, pl.ds(yp, 128, stride=2), :])

    index_load.wait()
    weight_load.wait()
    def w_plane(z, lo, hi):
        for r in range(0, 128, CH):
            c = center(f, z, r, CH)
            nb = nbxy0(f, z, r, CH, c)
            for ph in range(4):
                t = 12.0 * c[ph] + nb[ph]
                if lo:
                    t = t + rows(f, z - 1, ph, r, CH)
                if hi:
                    t = t + rows(f, z + 1, ph, r, CH)
                a[z, ph, pl.ds(PAD + r, CH), :] = t

    for i, z in enumerate(range(8)):
        orb_copy(z).wait()

        def put(ph, value):
            f[z + 4, ph, pl.ds(PAD, 128), :] = value

        density(z, pidx, i % 2, put)
        if z:
            w_plane(z + 3, z > 1, True)

    w_plane(11, True, False)

    pl.semaphore_wait(barrier, gz - 1 + pairs - 1 + has_across.astype(jnp.int32) + diagonal.astype(jnp.int32))

    index_copy = remote(pidx, pidx2, ixs.at[0], ixr.at[0], pair=other)
    index_copy.start()

    for side, z in ((0, 4), (1, 11)):
        for r in range(0, 128, CH):
            total, shifts = phase_sums(f, z, r, CH, center(f, z, r, CH))
            w = center(a, z, r, CH)
            g0o[side, pl.ds(r, CH), :] = (0.5 * N81) * (
                shifts - 3.0 * total + ((w[0] + w[1]) + (w[2] + w[3]))
            )

    def exchange(out, landed, s_sems, r_sems):
        lo = remote(out.at[0], landed.at[1], s_sems.at[0], r_sems.at[1], gz=jnp.maximum(d - 1, 0))
        hi = remote(out.at[1], landed.at[0], s_sems.at[1], r_sems.at[0], gz=jnp.minimum(d + 1, gz - 1))
        return lo, hi

    g0_lo, g0_hi = exchange(g0o, g0, g0s, g0r)

    @pl.when(has_lo)
    def _():
        g0_lo.start()

    @pl.when(has_hi)
    def _():
        g0_hi.start()

    def f_copy(side, far, of_other):
        k = far if side == 0 else 3 - far
        here = k if side == 0 else 4 + k
        there = 12 + k if side == 0 else k
        to = jnp.maximum(d - 1, 0) if side == 0 else jnp.minimum(d + 1, gz - 1)
        landed = f.at[there, :, pl.ds(PAD, 128), :]
        if of_other:
            return remote(fx.at[k], landed, fs.at[side, far], fr.at[1 - side, far], gz=to, pair=other)
        return remote(
            f.at[4 + here, :, pl.ds(PAD, 128), :], landed, fs.at[side, far], fr.at[1 - side, far], gz=to, pair=me
        )

    def on_chip(act):
        for side, cond in ((0, jnp.logical_not(even)), (1, even)):
            @pl.when(cond)
            def _():
                for far in range(4):
                    act(side, far, False)

    def crossing(far, act, of_other, only=True):
        kind = {
            (0, False): diagonal, (3, False): straight,
            (0, True): straight, (1, True): True, (2, True): straight,
        }.get((far, of_other))
        if kind is None:
            return
        for side, cond in ((0, jnp.logical_and(even, has_lo)), (1, jnp.logical_and(jnp.logical_not(even), has_hi))):
            @pl.when(jnp.logical_and(cond, jnp.logical_and(kind, only)))
            def _():
                act(side, far, of_other)

    relays = ((0, jnp.logical_and(turn == 0, has_lo), jnp.logical_and(turn == 0, d < gz - 4), -4),
              (1, jnp.logical_and(turn == 3, has_hi), jnp.logical_and(turn == 3, d >= 4), 4))

    def to_relay(side, far, step):
        k = far if side == 0 else 3 - far
        return remote(
            fx.at[k], relay.at[far - 2], ys.at[far - 2], yr.at[far - 2], gz=jnp.clip(d + step, 0, gz - 1), pair=me
        )

    def hand_on(side, far):
        there = 12 + far if side == 0 else 3 - far
        return remote(
            relay.at[far - 2], f.at[there, :, pl.ds(PAD, 128), :], yf.at[far - 2], fr.at[1 - side, far],
            gz=jnp.clip(partner, 0, gz - 1), pair=other,
        )

    def begin(side, far, of_other):
        f_copy(side, far, of_other).start()

    def sent(side, far, of_other):
        f_copy(side, far, of_other).wait_send()

    crossing(0, begin, False)
    on_chip(begin)

    for ph in range(4):
        a[3, ph, pl.ds(PAD, 128), :] = flo * f[4, ph, pl.ds(PAD, 128), :]
        a[12, ph, pl.ds(PAD, 128), :] = fhi * f[11, ph, pl.ds(PAD, 128), :]

    @pl.loop(0, 4)
    def _(j):
        for r in range(0, 128, CH):
            out = None
            for dz in range(2):
                z = 4 + 2 * j + dz
                c = center(a, z, r, CH)
                total, shifts = phase_sums(a, z, r, CH, c)
                below, above, src = center(a, z - 1, r, CH), center(a, z + 1, r, CH), center(f, z, r, CH)
                zs = ((below[0] + below[1]) + (below[2] + below[3])) + (
                    (above[0] + above[1]) + (above[2] + above[3])
                )
                q = ((src[0] + src[1]) + (src[2] + src[3])) + N81 * (zs - 4.0 * total + shifts)
                out = q if out is None else out + q
            s1[5 + j, pl.ds(PAD + r, CH), :] = 0.5 * out
            b1[5 + j, pl.ds(PAD + r, CH), :] = 0.5 * out

    def ypair(ref, slot, n):
        return ref[slot, pl.ds(0, n, stride=2), :] + ref[slot, pl.ds(1, n, stride=2), :]

    def inside(step):
        at = d + step
        return jnp.logical_and(at >= 0, at < gz)

    flag2 = {p: inside(p - 3).astype(F32) for p in range(1, 6)}
    m_first, m_second = mats[0], mats[1]
    low_half = lane_iota((64, 128)) < 64

    def nb2(ref, p, c):
        z = roll(c + jnp.where(low_half, crow(ref, p + 1, 0, 64), crow(ref, p - 1, 0, 64)), 64)
        return nbxy(ref, p, 0, 64, c, 64) + z

    b1[4, pl.ds(PAD, 128), :] = flo * g0o[0]
    b1[9, pl.ds(PAD, 128), :] = fhi * g0o[1]

    @pl.loop(3, 11, unroll=4)
    def _(z):
        flag = jnp.where(z < 5, flo, jnp.where(z > 8, fhi, 1.0))
        for r in range(0, 128, 64):
            c = crow(b1, z, r, 64)
            nb = nbxy(b1, z, r, 64, c, 128) + (crow(b1, z - 1, r, 64) + crow(b1, z + 1, r, 64))
            a1[z, pl.ds(PAD + r, 64), :] = flag * (12.0 * c + nb)

    @pl.loop(0, 6, unroll=2)
    def _(j):
        for r in range(0, 128, 64):
            out = None
            for dz in range(2):
                z = 1 + 2 * j + dz
                c = crow(a1, z, r, 64)
                nb = nbxy(a1, z, r, 64, c, 128) + (crow(a1, z - 1, r, 64) + crow(a1, z + 1, r, 64))
                q = crow(b1, z, r, 64) + N81 * (nb - 6.0 * c)
                out = q if out is None else out + q
            t1[j, pl.ds(r, 64), :] = 0.5 * out

    for p in range(3):
        b2[2 + p, pl.ds(PAD, 64), :] = flag2[2 + p] * (
            split_dot(ypair(t1, 2 * p, 64), m_first) + split_dot(ypair(t1, 2 * p + 1, 64), m_second)
        )
    for p in range(1, 6):
        c = crow(b2, p, 0, 64)
        a2[p, pl.ds(PAD, 64), :] = flag2[p] * (12.0 * c + nb2(b2, p, c))
    for p in range(1, 6):
        w = crow(a2, p, 0, 64)
        t2[p - 1] = crow(b2, p, 0, 64) + N81 * (nb2(a2, p, w) - 6.0 * w)
    tile = None
    for p in range(1, 5):
        part = split_dot(ypair(t2, p, 32), mats[4 + p])
        tile = part if tile is None else tile + part
    t3[d, pl.ds(0, 32), :] = 0.5 * tile
    part = split_dot(ypair(t2, 0, 32), mats[14])
    block8 = lane_iota((8, 128)) // 32
    row = part[0:8]
    for k in range(1, 4):
        row = jnp.where(block8 == k, part[8 * k:8 * k + 8], row)
    t3[d, pl.ds(32, 8), :] = 0.5 * row

    beside = jnp.where(even, d + 1, d - 1)

    def t3_copy(o):
        return remote(t3.at[d], t3.at[d], t3s.at[o], t3r.at[d], gz=lax.rem(d + 2 * o, gz))

    def t3_pass(o):
        e = lax.rem(d + 2 * o, gz)
        return remote(t3.at[e], t3.at[e], t3p.at[o], t3r.at[e], gz=beside)

    @pl.loop(1, gz // 2)
    def _(o):
        t3_copy(o).start()

    t3_pass(0).start()

    index_copy.wait_recv()
    for far in range(4):
        for side, cond in ((0, even), (1, jnp.logical_not(even))):
            k = far if side == 0 else 3 - far
            if far in (0, 3):
                cond = jnp.logical_and(cond, straight if far == 0 else diagonal)

            def put_other(ph, value):
                fx[k, ph] = value

            @pl.when(cond)
            def _():
                density(k + 4 * side, pidx2, far % 2, put_other)

        crossing(far, begin, True, True if EARLY else straight)
        if far >= 2:
            for side, cond, _, step in relays:
                @pl.when(cond)
                def _():
                    to_relay(side, far, step).start()

    @pl.when(has_lo)
    def _():
        g0_hi.wait_recv()
        s1[5, pl.ds(PAD, 128), :] += g0[0]

    @pl.when(has_hi)
    def _():
        g0_lo.wait_recv()
        s1[8, pl.ds(PAD, 128), :] += g0[1]

    def w1_plane(z, lo, hi):
        for r in range(0, 128, 64):
            c = crow(s1, z, r, 64)
            t = 12.0 * c + nbxy(s1, z, r, 64, c, 128)
            if lo:
                t = t + crow(s1, z - 1, r, 64)
            if hi:
                t = t + crow(s1, z + 1, r, 64)
            a1[z, pl.ds(PAD + r, 64), :] = t

    for z in range(5, 9):
        w1_plane(z, z > 5, z < 8)
    a1[4, pl.ds(PAD, 128), :] = flo * crow(s1, 5, 0, 128)
    a1[9, pl.ds(PAD, 128), :] = fhi * crow(s1, 8, 0, 128)
    for slot, z in ((0, 5), (3, 8)):
        for r in range(0, 128, 64):
            c = crow(s1, z, r, 64)
            t1[slot, pl.ds(r, 64), :] = (0.5 * N81) * (
                nbxy(s1, z, r, 64, c, 128) - 5.0 * c + crow(a1, z, r, 64)
            )
    for slot in (1, 2):
        for r in range(0, 128, 64):
            out = None
            for z in (3 + 2 * slot, 4 + 2 * slot):
                c = crow(a1, z, r, 64)
                nb = nbxy(a1, z, r, 64, c, 128) + (crow(a1, z - 1, r, 64) + crow(a1, z + 1, r, 64))
                q = crow(s1, z, r, 64) + N81 * (nb - 6.0 * c)
                out = q if out is None else out + q
            t1[slot, pl.ds(r, 64), :] = 0.5 * out

    g1o[0] = split_dot(ypair(t1, 0, 64), m_second)
    g1o[1] = split_dot(ypair(t1, 3, 64), m_first)
    g1_lo, g1_hi = exchange(g1o, g1, g1s, g1r)

    @pl.when(has_lo)
    def _():
        g1_lo.start()

    @pl.when(has_hi)
    def _():
        g1_hi.start()

    s2[3, pl.ds(PAD, 64), :] = split_dot(ypair(t1, 1, 64), m_first) + split_dot(ypair(t1, 2, 64), m_second)

    def h1_copy(i):
        here, there, step = ((5, 9, -1), (6, 2, 1))[i]
        to = jnp.clip(d + step, 0, gz - 1)
        return remote(
            s1.at[pl.ds(here, 3), pl.ds(PAD, 128), :], s1.at[pl.ds(there, 3), pl.ds(PAD, 128), :],
            h1s.at[i], h1r.at[i], gz=to,
        )

    h1_sends, h1_recvs = [has_lo, has_hi], [has_hi, has_lo]

    def h1_start():
        for i in range(2):
            @pl.when(h1_sends[i])
            def _():
                h1_copy(i).start()

    h1_start()

    @pl.loop(1, gz // 2)
    def _(o):
        e = lax.rem(d + 2 * o, gz)
        remote(t3.at[e], t3.at[e], t3s.at[o], t3r.at[e], gz=e).wait_recv()
        t3_pass(o).start()

    @pl.when(has_lo)
    def _():
        g1_hi.wait_recv()
        s2[3, pl.ds(PAD, 64), :] += g1[0]

    @pl.when(has_hi)
    def _():
        g1_lo.wait_recv()
        s2[3, pl.ds(PAD, 64), :] += g1[1]

    def h2_copy(i):
        step = (-2, -1, 1, 2)[i]
        to = jnp.clip(d + step, 0, gz - 1)
        return remote(
            s2.at[3, pl.ds(PAD, 64), :], s2.at[3 - step, pl.ds(PAD, 64), :], h2s.at[i], h2r.at[i], gz=to
        )

    for i, step in enumerate((-2, -1, 1, 2)):
        @pl.when(inside(step))
        def _():
            h2_copy(i).start()

    crossing(3, begin, False)


    @pl.loop(0, gz // 2)
    def _(o):
        e = lax.rem(beside + 2 * o, gz)
        remote(t3.at[e], t3.at[e], t3p.at[o], t3r.at[e], gz=beside).wait_recv()

    if not EARLY:
        crossing(1, begin, True, diagonal)
    for far in (2, 3):
        for side, _, cond, step in relays:
            @pl.when(cond)
            def _():
                to_relay(side, far, step).wait_recv()
                hand_on(side, far).start()

    lane32 = lane_iota((32, 128))
    for q in range(4):
        total = None
        for e in range(max(4 * q - 2, 0), min(4 * q + 6, gz)):
            low, high = max(e - 1 - 4 * q, 0), min(e + 2 - 4 * q, 3)
            parts = []
            if low <= high:
                x = t3[e, pl.ds(0, 32), :]
                if (low, high) != (0, 3):
                    x = jnp.where(jnp.logical_and(lane32 >= 32 * low, lane32 < 32 * high + 32), x, 0.0)
                parts.append(x)
            block = e - 2 - 4 * q
            if 0 <= block < 4:
                x = t3[e, pl.ds(32, 8), :]
                pieces = [jnp.where(block8 == block, roll(x, 32 * (block - k)), 0.0) for k in range(4)]
                parts.append(jnp.concatenate(pieces, axis=0))
            for x in parts:
                total = x if total is None else total + x
        s3[q] = total * NINTH
        a3[q, pl.ds(PAD, 32), :] = total * NINTH

    def sweep3(src, dst):
        v = [crow(src, q, 0, 32) for q in range(4)]
        for q in range(4):
            after = v[q + 1] if q < 3 else jnp.zeros_like(v[0])
            before = v[q - 1] if q > 0 else jnp.zeros_like(v[0])
            nz = roll(jnp.where(lane32 < 32, after, v[q]), -32)
            nz = nz + roll(jnp.where(lane32 >= 96, before, v[q]), 32)
            nb = nbxy(src, q, 0, 32, v[q], 32) + nz
            dst[q, pl.ds(PAD, 32), :] = (1.0 / 3.0) * v[q] + (NINTH * nb + s3[q])

    @pl.loop(0, 3)
    def _(i):
        sweep3(a3, b3)
        sweep3(b3, a3)

    sweep3(a3, b3)

    def f_wait(*which):
        @pl.when(has_lo)
        def _():
            for far in which:
                f_copy(1, far, False).wait_recv()

        @pl.when(has_hi)
        def _():
            for far in which:
                f_copy(0, far, False).wait_recv()

    f_wait(0, 1)
    w_plane(4, True, True)
    w_plane(11, True, True)

    @pl.when(has_lo)
    def _():
        w_plane(3, True, True)

    @pl.when(has_hi)
    def _():
        w_plane(12, True, True)

    def products(z, carry):
        plain, edges = carry
        for r in range(0, 128, CH):
            c, src, up = center(a, z, r, CH), center(f, z, r, CH), center(a, z + 1, r, CH)
            for ph in range(4):
                plain = plain + fold(c[ph] * (src[ph] - (3.0 * N81) * c[ph]))
            e = c[0] * c[1] + c[2] * c[3] + (c[0] * c[2] + c[1] * c[3])
            e = e + (c[1] * from_right(c[0]) + c[3] * from_right(c[2]))
            e = e + (c[2] * rows(a, z, 0, r, CH, 1) + c[3] * rows(a, z, 1, r, CH, 1))
            for ph in range(4):
                e = e + c[ph] * up[ph]
            edges = edges + fold(e)
        return plain, edges

    zero = jnp.zeros((8, 128), F32)
    plain, edges = lax.fori_loop(4, 12, products, (zero, zero))
    kept[0] = plain
    kept[1] = edges

    for i, step in enumerate((-2, -1, 1, 2)):
        @pl.when(inside(-step))
        def _():
            h2_copy(i).wait_recv()

    for p in range(1, 6):
        at = d + p - 3
        q = jnp.clip(at // 4, 0, 3)
        e = split_dot(b3[q, pl.ds(PAD, 32), :], mats[8 + p])
        pe2[p - 1, pl.ds(0, 32, stride=2), :] = e
        pe2[p - 1, pl.ds(1, 32, stride=2), :] = e
    for p in range(1, 6):
        c = crow(s2, p, 0, 64)
        w = 12.0 * c + nb2(s2, p, c)
        a2[p, pl.ds(PAD, 64), :] = flag2[p] * (N81 * w + pe2[p - 1])

    def sweep2(src, dst, p):
        c = crow(src, p, 0, 64)
        dst[p, pl.ds(PAD, 64), :] = flag2[p] * (
            (1.0 / 3.0) * c + NINTH * (nb2(src, p, c) + crow(s2, p, 0, 64))
        )

    for p in range(2, 5):
        sweep2(a2, b2, p)
    for p in range(2, 5):
        sweep2(b2, a2, p)

    for i in range(2):
        @pl.when(h1_recvs[i])
        def _():
            h1_copy(i).wait_recv()

    for j in range(1, 5):
        e = split_dot(a2[2 + j // 2, pl.ds(PAD, 64), :], mats[2 + j % 2])
        pe1[j, pl.ds(0, 64, stride=2), :] = e
        pe1[j, pl.ds(1, 64, stride=2), :] = e

    def in_grid(z):
        return jnp.where(z < 5, flo, jnp.where(z > 8, fhi, 1.0))

    def nb1(ref, z, r, c):
        return nbxy(ref, z, r, 64, c, 128) + (crow(ref, z - 1, r, 64) + crow(ref, z + 1, r, 64))

    @pl.loop(3, 11, unroll=4)
    def _(z):
        flag = in_grid(z)
        for r in range(0, 128, 64):
            c = crow(s1, z, r, 64)
            w = 12.0 * c + nb1(s1, z, r, c)
            a1[z, pl.ds(PAD + r, 64), :] = flag * (N81 * w + pe1[(z - 1) // 2, pl.ds(r, 64), :])

    @pl.loop(4, 10, unroll=3)
    def _(z):
        flag = in_grid(z)
        for r in range(0, 128, 64):
            c = crow(a1, z, r, 64)
            t = nb1(a1, z, r, c) + crow(s1, z, r, 64)
            b1[z, pl.ds(PAD + r, 64), :] = flag * ((1.0 / 3.0) * c + NINTH * t)

    @pl.loop(5, 9, unroll=4)
    def _(z):
        for r in range(0, 128, 64):
            c = crow(b1, z, r, 64)
            t = nb1(b1, z, r, c) + crow(s1, z, r, 64)
            e1[z - 5, pl.ds(r, 64), :] = (1.0 / 3.0) * c + NINTH * t

    e1_lo = remote(
        e1.at[pl.ds(0, 2)], e1h.at[1], e1s.at[0], e1r.at[1], gz=jnp.maximum(d - 1, 0)
    )
    e1_hi = remote(
        e1.at[pl.ds(2, 2)], e1h.at[0], e1s.at[1], e1r.at[0], gz=jnp.minimum(d + 1, gz - 1)
    )

    @pl.when(has_lo)
    def _():
        e1_lo.start()

    @pl.when(has_hi)
    def _():
        e1_hi.start()

    def correct(z, ref, k):
        e = ref[k]
        for ph in range(4):
            a[z, ph, pl.ds(PAD, 128), :] = N81 * a[z, ph, pl.ds(PAD, 128), :] + e

    def sweep0(src, dst, first, last):
        @pl.loop(first + 4, last + 5)
        def _(z):
            for r in range(0, 128, CH):
                c = center(src, z, r, CH)
                nb = nbxy0(src, z, r, CH, c)
                for ph in range(4):
                    t = nb[ph] + (rows(src, z - 1, ph, r, CH) + rows(src, z + 1, ph, r, CH))
                    t = t + rows(f, z, ph, r, CH)
                    dst[z, ph, pl.ds(PAD + r, CH), :] = (1.0 / 3.0) * c[ph] + NINTH * t

    def below(first):
        return jnp.where(has_lo, first, 0)

    def above(last):
        return jnp.where(has_hi, last, 7)

    plain, edges = kept[0], kept[1]
    coarse = zero
    for j in range(4):
        coarse = coarse + fold(s1[5 + j, pl.ds(PAD, 128), :] * e1[j])
    part = (2.0 * N81) * (plain + N81 * edges) + 2.0 * coarse
    prods[d] = part.sum(axis=0, keepdims=True)

    @pl.loop(1, gz)
    def _(o):
        remote(prods.at[d], prods.at[d], ps.at[o], pr.at[d], gz=lax.rem(d + o, gz)).start()


    @pl.loop(0, 8)
    def _(z):
        correct(z + 4, e1, z // 2)

    sweep0(a, b, 1, 6)
    sweep0(b, a, 2, 5)

    def final(z, squares):
        for r in range(0, 128, CH):
            c = center(a, z, r, CH)
            nb = nbxy0(a, z, r, CH, c)
            for ph in range(4):
                t = nb[ph] + (rows(a, z - 1, ph, r, CH) + rows(a, z + 1, ph, r, CH))
                left = (rows(f, z, ph, r, CH) - 6.0 * c[ph]) + t
                squares = squares + fold(left * left)
        return squares

    kept[0] = lax.fori_loop(7, 9, final, zero)

    f_wait(2, 3)

    @pl.loop(jnp.where(has_lo, 1, 3), 3)
    def _(z):
        w_plane(z, True, True)

    @pl.loop(13, jnp.where(has_hi, 15, 13))
    def _(z):
        w_plane(z, True, True)

    @pl.when(has_lo)
    def _():
        e1_hi.wait_recv()
        for z in range(-3, 0):
            correct(z + 4, e1h.at[0], (z + 4) // 2)

    @pl.when(has_hi)
    def _():
        e1_lo.wait_recv()
        for z in range(8, 11):
            correct(z + 4, e1h.at[1], (z - 8) // 2)

    sweep0(a, b, below(-2), 0)
    sweep0(a, b, 7, above(9))
    sweep0(b, a, below(-1), 1)
    sweep0(b, a, 6, above(8))

    squares = lax.fori_loop(4, 7, final, kept[0])
    sums[d] = lax.fori_loop(9, 12, final, squares).sum(axis=0, keepdims=True)

    @pl.loop(1, gz)
    def _(o):
        remote(sums.at[d], sums.at[d], ss.at[o], sr.at[d], gz=lax.rem(d + o, gz)).start()

    @pl.loop(1, gz)
    def _(o):
        peer = lax.rem(d + o, gz)
        remote(prods.at[peer], prods.at[peer], ps.at[o], pr.at[peer], gz=peer).wait_recv()

    total = prods[0]
    for e in range(1, gz):
        total = total + prods[e]
    ens[me] = pweight[0, 0] * total

    @pl.loop(1, pairs)
    def _(o):
        remote(ens.at[me], ens.at[me], es.at[o], er.at[me], pair=lax.rem(me + o, pairs)).start()

    px[...] = selection((256, 256), lambda i, j: i == (j & 1) * 128 + (j >> 1))

    @pl.loop(0, 8)
    def _(z):
        for yp in range(2):
            x = jnp.concatenate(
                [a[z + 4, 2 * yp, pl.ds(PAD, 128), :], a[z + 4, 2 * yp + 1, pl.ds(PAD, 128), :]], axis=1
            )
            y = split_dot(x, px[...])
            for half in range(2):
                tmp[z % 2, half, pl.ds(yp, 128, stride=2), :] = y[:, 128 * half:128 * half + 128]
        for half in range(2):
            pot[0, z, :, pl.ds(128 * half, 128)] = tmp[z % 2, half]

    @pl.loop(1, gz)
    def _(o):
        peer = lax.rem(d + o, gz)
        remote(sums.at[peer], sums.at[peer], ss.at[o], sr.at[peer], gz=peer).wait_recv()

    total = sums[0]
    for e in range(1, gz):
        total = total + sums[e]
    cells = 1.0 / (gz * 8 * 256 * 256)
    stats[0:1, :] = jnp.zeros((1, 128), F32) + jnp.sqrt(jnp.sum(total, axis=1, keepdims=True) * cells)

    @pl.loop(1, pairs)
    def _(o):
        peer = lax.rem(me + o, pairs)
        remote(ens.at[peer], ens.at[peer], es.at[o], er.at[peer], pair=peer).wait_recv()

    energy = ens[0]
    for e in range(1, pairs):
        energy = energy + ens[e]
    stats[1:2, :] = jnp.zeros((1, 128), F32) + jnp.sum(energy, axis=1, keepdims=True) * (-0.5 * cells)

    for cond, side in ((has_lo, 0), (has_hi, 1)):
        @pl.when(cond)
        def _():
            (g0_lo, g0_hi)[side].wait_send()
            (g1_lo, g1_hi)[side].wait_send()
            (e1_lo, e1_hi)[side].wait_send()

    index_copy.wait_send()
    on_chip(sent)
    for far in range(4):
        crossing(far, sent, True)
    crossing(0, sent, False)
    crossing(3, sent, False)
    for far in (2, 3):
        for side, first, second, step in relays:
            @pl.when(first)
            def _():
                to_relay(side, far, step).wait_send()

            @pl.when(second)
            def _():
                hand_on(side, far).wait_send()

    for i in range(2):
        @pl.when(h1_sends[i])
        def _():
            h1_copy(i).wait_send()

    for i, step in enumerate((-2, -1, 1, 2)):
        @pl.when(inside(step))
        def _():
            h2_copy(i).wait_send()

    @pl.loop(1, gz)
    def _(o):
        remote(sums.at[d], sums.at[d], ss.at[o], sr.at[d], gz=lax.rem(d + o, gz)).wait_send()
        remote(prods.at[d], prods.at[d], ps.at[o], pr.at[d], gz=lax.rem(d + o, gz)).wait_send()

    @pl.loop(1, gz // 2)
    def _(o):
        t3_copy(o).wait_send()

    @pl.loop(0, gz // 2)
    def _(o):
        t3_pass(o).wait_send()

    @pl.loop(1, pairs)
    def _(o):
        remote(ens.at[me], ens.at[me], es.at[o], er.at[me], pair=lax.rem(me + o, pairs)).wait_send()


def solution(mesh):
    gz, pairs = mesh.shape["gz"], mesh.shape["pair"]
    dma, vmem = pltpu.SemaphoreType.DMA, pltpu.VMEM
    field = vmem((16, 4, 144, 128), F32)
    level1, level2, level3 = vmem((14, 144, 128), F32), vmem((7, 80, 128), F32), vmem((4, 48, 128), F32)

    def per_device(orbitals, pair_index, pair_weight):
        potential, stats = pl.pallas_call(
            functools.partial(kernel, gz, pairs),
            out_shape=(
                jax.ShapeDtypeStruct((1, 8, 256, 256), F32),
                jax.ShapeDtypeStruct((2, 128), F32),
            ),
            in_specs=[
                pl.BlockSpec(memory_space=pltpu.HBM),
                pl.BlockSpec(memory_space=pltpu.HBM),
                pl.BlockSpec(memory_space=pl.ANY),
            ],
            out_specs=(
                pl.BlockSpec(memory_space=pltpu.VMEM),
                pl.BlockSpec(memory_space=pltpu.VMEM),
            ),
            scratch_shapes=[
                *[vmem((8, 256, 256), BF16)] * 8,
                vmem((256, 256), BF16),
                vmem((15, 128, 128), BF16),
                vmem((2, 2, 256, 128), F32),
                pltpu.SMEM((1, 2), jnp.int32),
                pltpu.SMEM((1, 1), F32),
                pltpu.SMEM((1, 2), jnp.int32),
                vmem((4, 4, 128, 128), F32),
                vmem((2, 4, 128, 128), F32),
                field, field, field,
                vmem((2, 128, 128), F32), vmem((2, 128, 128), F32),
                level1, level1, level1,
                vmem((6, 128, 128), F32),
                vmem((2, 64, 128), F32), vmem((2, 64, 128), F32),
                vmem((6, 128, 128), F32),
                vmem((4, 128, 128), F32), vmem((2, 2, 128, 128), F32),
                level2, level2, level2,
                vmem((5, 64, 128), F32),
                vmem((5, 64, 128), F32),
                vmem((gz, 40, 128), F32),
                vmem((4, 32, 128), F32),
                level3, level3,
                vmem((2, 8, 128), F32),
                vmem((gz, 1, 128), F32), vmem((gz, 1, 128), F32),
                vmem((pairs, 1, 128), F32),
                dma((2,)),
                dma((8,)),
                dma((1,)), dma((1,)),
                dma((2,)), dma((2,)), dma((2,)),
                dma((2, 4)), dma((2, 4)),
                dma((2,)), dma((2,)),
                dma((2,)), dma((2,)),
                dma((2,)), dma((2,)),
                dma((2,)), dma((2,)),
                dma((4,)), dma((4,)),
                dma((gz,)), dma((gz,)), dma((gz,)),
                dma((gz,)), dma((gz,)),
                dma((gz,)), dma((gz,)),
                dma((pairs,)), dma((pairs,)),
            ],
            compiler_params=pltpu.CompilerParams(
                collective_id=0, has_side_effects=True, vmem_limit_bytes=48 * 1024 * 1024
            ),
            name="vcycle",
        )(pltpu.with_memory_space_constraint(pair_index, pltpu.HBM), pair_weight.reshape(1, 1), orbitals)
        return potential, stats[0, :1], stats[1, :1]

    return jax.shard_map(
        per_device,
        mesh=mesh,
        in_specs=(P(None, "gz", None, None), P("pair", None), P("pair")),
        out_specs=(P("pair", "gz", None, None), P("pair"), P()),
        check_vma=False,
    )
```

```python
import functools

import jax
import jax.numpy as jnp
from jax import lax
from jax.experimental import pallas as pl
from jax.experimental.pallas import tpu as pltpu
from jax.sharding import PartitionSpec as P

MESH = pl.DeviceIdType.MESH
F32, BF16 = jnp.float32, jnp.bfloat16
PAD = 8
EARLY = True
CH = 32
NINTH = 1.0 / 9.0
N81 = 1.0 / 81.0


def lane_iota(shape):
    return lax.broadcasted_iota(jnp.int32, shape, len(shape) - 1)


def roll(x, shift):
    return pltpu.roll(x, shift % x.shape[-1], x.ndim - 1)


def from_left(x, width=128):
    return jnp.where(lane_iota(x.shape) % width == 0, 0.0, roll(x, 1))


def from_right(x, width=128):
    return jnp.where(lane_iota(x.shape) % width == width - 1, 0.0, roll(x, -1))


def split_dot(x, m):
    hi = x.astype(BF16)
    rest = x - hi.astype(F32)
    mid = rest.astype(BF16)
    low = (rest - mid.astype(F32)).astype(BF16)
    dot = functools.partial(jnp.dot, preferred_element_type=F32)
    return dot(hi, m) + dot(mid, m) + dot(low, m)


def selection(shape, test):
    a = lax.broadcasted_iota(jnp.int32, shape, 0)
    b = lax.broadcasted_iota(jnp.int32, shape, 1)
    return jnp.where(test(a, b), 1.0, 0.0).astype(BF16)


def fold(x):
    return x.reshape(x.shape[0] // 8, 8, x.shape[1]).sum(axis=0)


def rows(ref, z, ph, r, n, dr=0):
    return ref[z, ph, pl.ds(PAD + r + dr, n), :]


def nbxy0(ref, z, r, n, c):
    out = []
    for yp in range(2):
        for xp in range(2):
            side = c[2 * yp + 1 - xp]
            x = side + (from_right(side) if xp else from_left(side))
            other = 2 * (1 - yp) + xp
            y = c[other] + rows(ref, z, other, r, n, 1 if yp else -1)
            out.append(x + y)
    return out


def phase_sums(ref, z, r, n, c):
    total = (c[0] + c[1]) + (c[2] + c[3])
    shifts = from_left(c[1] + c[3]) + from_right(c[0] + c[2])
    shifts = shifts + (rows(ref, z, 2, r, n, -1) + rows(ref, z, 3, r, n, -1))
    shifts = shifts + (rows(ref, z, 0, r, n, 1) + rows(ref, z, 1, r, n, 1))
    return total, shifts


def center(ref, z, r, n):
    return [rows(ref, z, ph, r, n) for ph in range(4)]


def crow(ref, z, r, n, dr=0):
    return ref[z, pl.ds(PAD + r + dr, n), :]


def nbxy(ref, z, r, n, c, width):
    y = crow(ref, z, r, n, -1) + crow(ref, z, r, n, 1)
    return y + (from_left(c, width) + from_right(c, width))


def kernel(
    gz, pairs,
    index_in, weight_in, orbitals, pot, stats,
    orb0, orb1, orb2, orb3, orb4, orb5, orb6, orb7, px, mats, tmp, pidx, pweight, pidx2, fx, relay, f, a, b, g0, g0o, s1, a1, b1, t1, g1, g1o, pe1, e1, e1h,
    s2, a2, b2, t2, pe2, t3, s3, a3, b3, kept, prods, sums, ens,
    scalar_sem, orb_sem, ixs, ixr, ys, yr, yf, fs, fr, g0s, g0r, h1s, h1r, g1s, g1r, e1s, e1r, h2s, h2r, t3s, t3p, t3r, ps, pr, ss, sr, es, er,
):
    d = lax.axis_index("gz")
    me = lax.axis_index("pair")
    has_lo, has_hi = d > 0, d < gz - 1
    flo, fhi = has_lo.astype(F32), has_hi.astype(F32)

    def remote(src, dst, s_sem, r_sem, **to):
        return pltpu.make_async_remote_copy(
            src_ref=src, dst_ref=dst, send_sem=s_sem, recv_sem=r_sem, device_id=to, device_id_type=MESH
        )

    orb = (orb0, orb1, orb2, orb3, orb4, orb5, orb6, orb7)

    def orb_copy(z):
        return pltpu.make_async_copy(orbitals.at[:, z], orb[z], orb_sem.at[z])

    index_load = pltpu.make_async_copy(index_in, pidx, scalar_sem.at[0])
    weight_load = pltpu.make_async_copy(weight_in, pweight, scalar_sem.at[1])
    index_load.start()
    weight_load.start()
    for z in range(8):
        orb_copy(z).start()
    barrier = pltpu.get_barrier_semaphore()

    @pl.loop(1, gz)
    def _(o):
        pl.semaphore_signal(barrier, inc=1, device_id={"gz": lax.rem(d + o, gz)}, device_id_type=MESH)

    @pl.loop(1, pairs)
    def _(o):
        pl.semaphore_signal(barrier, inc=1, device_id={"pair": lax.rem(me + o, pairs)}, device_id_type=MESH)

    other = lax.rem(me + pairs // 2, pairs)
    even = lax.rem(d, 2) == 0
    across = jnp.where(even, d - 1, d + 1)
    has_across = jnp.logical_and(across >= 0, across < gz)

    @pl.when(has_across)
    def _():
        pl.semaphore_signal(barrier, inc=1, device_id={"gz": across, "pair": other}, device_id_type=MESH)

    turn = lax.rem(d, 4)
    straight = jnp.logical_or(turn == 1, turn == 2)
    diagonal = jnp.logical_not(straight)
    partner = jnp.where(turn == 0, d + 3, d - 3)

    @pl.when(diagonal)
    def _():
        pl.semaphore_signal(barrier, inc=1, device_id={"gz": partner, "pair": other}, device_id_type=MESH)

    px[...] = selection((256, 256), lambda i, j: j == (i & 1) * 128 + (i >> 1))
    pad0 = jnp.zeros((4, PAD, 128), F32)
    square = (128, 128)
    mats[0] = selection(square, lambda i, j: (i >> 1) == j)
    mats[1] = selection(square, lambda i, j: (i >> 1) + 64 == j)
    for half in range(2):
        mats[2 + half] = selection(square, lambda i, j: i == (j >> 1) + 64 * half)
    for p in range(5):
        block = lax.rem(d + p - 2 + gz, 4) * 32
        mats[4 + p] = selection(square, lambda i, j: ((i & 63) >> 1) + block == j)
        mats[9 + p] = selection(square, lambda i, j: i == ((j & 63) >> 1) + block)
    mats[14] = selection(square, lambda i, j: ((i & 63) >> 1) == (j & 31))

    @pl.loop(0, 16)
    def _(z):
        for ref in (f, a, b):
            ref[z, :, pl.ds(0, PAD), :] = pad0
            ref[z, :, pl.ds(PAD + 128, PAD), :] = pad0

    def clear_outside(first):
        @pl.loop(first, first + 4)
        def _(z):
            for ref in (f, a, b):
                for ph in range(4):
                    ref[z, ph, pl.ds(PAD, 128), :] = jnp.zeros((128, 128), F32)

        @pl.when(first == 0)
        def _():
            @pl.loop(0, 5)
            def _(z):
                s1[z, pl.ds(PAD, 128), :] = jnp.zeros((128, 128), F32)

        @pl.when(first > 0)
        def _():
            @pl.loop(9, 14)
            def _(z):
                s1[z, pl.ds(PAD, 128), :] = jnp.zeros((128, 128), F32)

    @pl.when(d == 0)
    def _():
        clear_outside(0)
        g0[0] = jnp.zeros((128, 128), F32)
        g1[0] = jnp.zeros((64, 128), F32)

    @pl.when(d == gz - 1)
    def _():
        clear_outside(12)
        g0[1] = jnp.zeros((128, 128), F32)
        g1[1] = jnp.zeros((64, 128), F32)

    @pl.loop(0, 14)
    def _(z):
        s1[z, pl.ds(0, PAD), :] = jnp.zeros((PAD, 128), F32)
        s1[z, pl.ds(PAD + 128, PAD), :] = jnp.zeros((PAD, 128), F32)
        a1[z] = jnp.zeros((144, 128), F32)
        b1[z] = jnp.zeros((144, 128), F32)

    @pl.loop(0, 7)
    def _(p):
        s2[p, pl.ds(0, PAD), :] = jnp.zeros((PAD, 128), F32)
        s2[p, pl.ds(PAD + 64, PAD), :] = jnp.zeros((PAD, 128), F32)
        a2[p] = jnp.zeros((80, 128), F32)
        b2[p] = jnp.zeros((80, 128), F32)
        at = d + p - 3

        @pl.when(jnp.logical_or(jnp.logical_or(at < 0, at >= gz), jnp.logical_or(p == 0, p == 6)))
        def _():
            s2[p, pl.ds(PAD, 64), :] = jnp.zeros((64, 128), F32)

    for q in range(4):
        a3[q] = jnp.zeros((48, 128), F32)
        b3[q] = jnp.zeros((48, 128), F32)

    def density(z, which, slot, put):
        left = jnp.dot(orb[z][which[0, 0]], px[...], preferred_element_type=F32)
        right = jnp.dot(orb[z][which[0, 1]], px[...], preferred_element_type=F32)
        both = left * right
        tmp[slot, 0] = both[:, :128]
        tmp[slot, 1] = both[:, 128:]
        for yp in range(2):
            for xp in range(2):
                put(2 * yp + xp, tmp[slot, xp, pl.ds(yp, 128, stride=2), :])

    index_load.wait()
    weight_load.wait()
    def w_plane(z, lo, hi):
        for r in range(0, 128, CH):
            c = center(f, z, r, CH)
            nb = nbxy0(f, z, r, CH, c)
            for ph in range(4):
                t = 12.0 * c[ph] + nb[ph]
                if lo:
                    t = t + rows(f, z - 1, ph, r, CH)
                if hi:
                    t = t + rows(f, z + 1, ph, r, CH)
                a[z, ph, pl.ds(PAD + r, CH), :] = t

    for i, z in enumerate(range(8)):
        orb_copy(z).wait()

        def put(ph, value):
            f[z + 4, ph, pl.ds(PAD, 128), :] = value

        density(z, pidx, i % 2, put)
        if z:
            w_plane(z + 3, z > 1, True)

    w_plane(11, True, False)

    pl.semaphore_wait(barrier, gz - 1 + pairs - 1 + has_across.astype(jnp.int32) + diagonal.astype(jnp.int32))

    index_copy = remote(pidx, pidx2, ixs.at[0], ixr.at[0], pair=other)
    index_copy.start()

    for side, z in ((0, 4), (1, 11)):
        for r in range(0, 128, CH):
            total, shifts = phase_sums(f, z, r, CH, center(f, z, r, CH))
            w = center(a, z, r, CH)
            g0o[side, pl.ds(r, CH), :] = (0.5 * N81) * (
                shifts - 3.0 * total + ((w[0] + w[1]) + (w[2] + w[3]))
            )

    def exchange(out, landed, s_sems, r_sems):
        lo = remote(out.at[0], landed.at[1], s_sems.at[0], r_sems.at[1], gz=jnp.maximum(d - 1, 0))
        hi = remote(out.at[1], landed.at[0], s_sems.at[1], r_sems.at[0], gz=jnp.minimum(d + 1, gz - 1))
        return lo, hi

    g0_lo, g0_hi = exchange(g0o, g0, g0s, g0r)

    @pl.when(has_lo)
    def _():
        g0_lo.start()

    @pl.when(has_hi)
    def _():
        g0_hi.start()

    def f_copy(side, far, of_other):
        k = far if side == 0 else 3 - far
        here = k if side == 0 else 4 + k
        there = 12 + k if side == 0 else k
        to = jnp.maximum(d - 1, 0) if side == 0 else jnp.minimum(d + 1, gz - 1)
        landed = f.at[there, :, pl.ds(PAD, 128), :]
        if of_other:
            return remote(fx.at[k], landed, fs.at[side, far], fr.at[1 - side, far], gz=to, pair=other)
        return remote(
            f.at[4 + here, :, pl.ds(PAD, 128), :], landed, fs.at[side, far], fr.at[1 - side, far], gz=to, pair=me
        )

    def on_chip(act):
        for side, cond in ((0, jnp.logical_not(even)), (1, even)):
            @pl.when(cond)
            def _():
                for far in range(4):
                    act(side, far, False)

    def crossing(far, act, of_other, only=True):
        kind = {
            (0, False): diagonal, (3, False): straight,
            (0, True): straight, (1, True): True, (2, True): straight,
        }.get((far, of_other))
        if kind is None:
            return
        for side, cond in ((0, jnp.logical_and(even, has_lo)), (1, jnp.logical_and(jnp.logical_not(even), has_hi))):
            @pl.when(jnp.logical_and(cond, jnp.logical_and(kind, only)))
            def _():
                act(side, far, of_other)

    relays = ((0, jnp.logical_and(turn == 0, has_lo), jnp.logical_and(turn == 0, d < gz - 4), -4),
              (1, jnp.logical_and(turn == 3, has_hi), jnp.logical_and(turn == 3, d >= 4), 4))

    def to_relay(side, far, step):
        k = far if side == 0 else 3 - far
        return remote(
            fx.at[k], relay.at[far - 2], ys.at[far - 2], yr.at[far - 2], gz=jnp.clip(d + step, 0, gz - 1), pair=me
        )

    def hand_on(side, far):
        there = 12 + far if side == 0 else 3 - far
        return remote(
            relay.at[far - 2], f.at[there, :, pl.ds(PAD, 128), :], yf.at[far - 2], fr.at[1 - side, far],
            gz=jnp.clip(partner, 0, gz - 1), pair=other,
        )

    def begin(side, far, of_other):
        f_copy(side, far, of_other).start()

    def sent(side, far, of_other):
        f_copy(side, far, of_other).wait_send()

    crossing(0, begin, False)
    on_chip(begin)

    for ph in range(4):
        a[3, ph, pl.ds(PAD, 128), :] = flo * f[4, ph, pl.ds(PAD, 128), :]
        a[12, ph, pl.ds(PAD, 128), :] = fhi * f[11, ph, pl.ds(PAD, 128), :]

    @pl.loop(0, 4)
    def _(j):
        for r in range(0, 128, CH):
            out = None
            for dz in range(2):
                z = 4 + 2 * j + dz
                c = center(a, z, r, CH)
                total, shifts = phase_sums(a, z, r, CH, c)
                below, above, src = center(a, z - 1, r, CH), center(a, z + 1, r, CH), center(f, z, r, CH)
                zs = ((below[0] + below[1]) + (below[2] + below[3])) + (
                    (above[0] + above[1]) + (above[2] + above[3])
                )
                q = ((src[0] + src[1]) + (src[2] + src[3])) + N81 * (zs - 4.0 * total + shifts)
                out = q if out is None else out + q
            s1[5 + j, pl.ds(PAD + r, CH), :] = 0.5 * out
            b1[5 + j, pl.ds(PAD + r, CH), :] = 0.5 * out

    def ypair(ref, slot, n):
        return ref[slot, pl.ds(0, n, stride=2), :] + ref[slot, pl.ds(1, n, stride=2), :]

    def inside(step):
        at = d + step
        return jnp.logical_and(at >= 0, at < gz)

    flag2 = {p: inside(p - 3).astype(F32) for p in range(1, 6)}
    m_first, m_second = mats[0], mats[1]
    low_half = lane_iota((64, 128)) < 64

    def nb2(ref, p, c):
        z = roll(c + jnp.where(low_half, crow(ref, p + 1, 0, 64), crow(ref, p - 1, 0, 64)), 64)
        return nbxy(ref, p, 0, 64, c, 64) + z

    b1[4, pl.ds(PAD, 128), :] = flo * g0o[0]
    b1[9, pl.ds(PAD, 128), :] = fhi * g0o[1]

    @pl.loop(3, 11, unroll=8)
    def _(z):
        flag = jnp.where(z < 5, flo, jnp.where(z > 8, fhi, 1.0))
        for r in range(0, 128, 64):
            c = crow(b1, z, r, 64)
            nb = nbxy(b1, z, r, 64, c, 128) + (crow(b1, z - 1, r, 64) + crow(b1, z + 1, r, 64))
            a1[z, pl.ds(PAD + r, 64), :] = flag * (12.0 * c + nb)

    @pl.loop(0, 6, unroll=3)
    def _(j):
        for r in range(0, 128, 64):
            out = None
            for dz in range(2):
                z = 1 + 2 * j + dz
                c = crow(a1, z, r, 64)
                nb = nbxy(a1, z, r, 64, c, 128) + (crow(a1, z - 1, r, 64) + crow(a1, z + 1, r, 64))
                q = crow(b1, z, r, 64) + N81 * (nb - 6.0 * c)
                out = q if out is None else out + q
            t1[j, pl.ds(r, 64), :] = 0.5 * out

    for p in range(3):
        b2[2 + p, pl.ds(PAD, 64), :] = flag2[2 + p] * (
            split_dot(ypair(t1, 2 * p, 64), m_first) + split_dot(ypair(t1, 2 * p + 1, 64), m_second)
        )
    for p in range(1, 6):
        c = crow(b2, p, 0, 64)
        a2[p, pl.ds(PAD, 64), :] = flag2[p] * (12.0 * c + nb2(b2, p, c))
    for p in range(1, 6):
        w = crow(a2, p, 0, 64)
        t2[p - 1] = crow(b2, p, 0, 64) + N81 * (nb2(a2, p, w) - 6.0 * w)
    tile = None
    for p in range(1, 5):
        part = split_dot(ypair(t2, p, 32), mats[4 + p])
        tile = part if tile is None else tile + part
    t3[d, pl.ds(0, 32), :] = 0.5 * tile
    part = split_dot(ypair(t2, 0, 32), mats[14])
    block8 = lane_iota((8, 128)) // 32
    row = part[0:8]
    for k in range(1, 4):
        row = jnp.where(block8 == k, part[8 * k:8 * k + 8], row)
    t3[d, pl.ds(32, 8), :] = 0.5 * row

    beside = jnp.where(even, d + 1, d - 1)

    def t3_copy(o):
        return remote(t3.at[d], t3.at[d], t3s.at[o], t3r.at[d], gz=lax.rem(d + 2 * o, gz))

    def t3_pass(o):
        e = lax.rem(d + 2 * o, gz)
        return remote(t3.at[e], t3.at[e], t3p.at[o], t3r.at[e], gz=beside)

    @pl.loop(1, gz // 2)
    def _(o):
        t3_copy(o).start()

    t3_pass(0).start()

    index_copy.wait_recv()
    for far in range(4):
        for side, cond in ((0, even), (1, jnp.logical_not(even))):
            k = far if side == 0 else 3 - far
            if far in (0, 3):
                cond = jnp.logical_and(cond, straight if far == 0 else diagonal)

            def put_other(ph, value):
                fx[k, ph] = value

            @pl.when(cond)
            def _():
                density(k + 4 * side, pidx2, far % 2, put_other)

        crossing(far, begin, True, True if EARLY else straight)
        if far >= 2:
            for side, cond, _, step in relays:
                @pl.when(cond)
                def _():
                    to_relay(side, far, step).start()

    @pl.when(has_lo)
    def _():
        g0_hi.wait_recv()
        s1[5, pl.ds(PAD, 128), :] += g0[0]

    @pl.when(has_hi)
    def _():
        g0_lo.wait_recv()
        s1[8, pl.ds(PAD, 128), :] += g0[1]

    def w1_plane(z, lo, hi):
        for r in range(0, 128, 64):
            c = crow(s1, z, r, 64)
            t = 12.0 * c + nbxy(s1, z, r, 64, c, 128)
            if lo:
                t = t + crow(s1, z - 1, r, 64)
            if hi:
                t = t + crow(s1, z + 1, r, 64)
            a1[z, pl.ds(PAD + r, 64), :] = t

    for z in range(5, 9):
        w1_plane(z, z > 5, z < 8)
    a1[4, pl.ds(PAD, 128), :] = flo * crow(s1, 5, 0, 128)
    a1[9, pl.ds(PAD, 128), :] = fhi * crow(s1, 8, 0, 128)
    for slot, z in ((0, 5), (3, 8)):
        for r in range(0, 128, 64):
            c = crow(s1, z, r, 64)
            t1[slot, pl.ds(r, 64), :] = (0.5 * N81) * (
                nbxy(s1, z, r, 64, c, 128) - 5.0 * c + crow(a1, z, r, 64)
            )
    for slot in (1, 2):
        for r in range(0, 128, 64):
            out = None
            for z in (3 + 2 * slot, 4 + 2 * slot):
                c = crow(a1, z, r, 64)
                nb = nbxy(a1, z, r, 64, c, 128) + (crow(a1, z - 1, r, 64) + crow(a1, z + 1, r, 64))
                q = crow(s1, z, r, 64) + N81 * (nb - 6.0 * c)
                out = q if out is None else out + q
            t1[slot, pl.ds(r, 64), :] = 0.5 * out

    g1o[0] = split_dot(ypair(t1, 0, 64), m_second)
    g1o[1] = split_dot(ypair(t1, 3, 64), m_first)
    g1_lo, g1_hi = exchange(g1o, g1, g1s, g1r)

    @pl.when(has_lo)
    def _():
        g1_lo.start()

    @pl.when(has_hi)
    def _():
        g1_hi.start()

    s2[3, pl.ds(PAD, 64), :] = split_dot(ypair(t1, 1, 64), m_first) + split_dot(ypair(t1, 2, 64), m_second)

    def h1_copy(i):
        here, there, step = ((5, 9, -1), (6, 2, 1))[i]
        to = jnp.clip(d + step, 0, gz - 1)
        return remote(
            s1.at[pl.ds(here, 3), pl.ds(PAD, 128), :], s1.at[pl.ds(there, 3), pl.ds(PAD, 128), :],
            h1s.at[i], h1r.at[i], gz=to,
        )

    h1_sends, h1_recvs = [has_lo, has_hi], [has_hi, has_lo]

    def h1_start():
        for i in range(2):
            @pl.when(h1_sends[i])
            def _():
                h1_copy(i).start()

    h1_start()

    @pl.loop(1, gz // 2)
    def _(o):
        e = lax.rem(d + 2 * o, gz)
        remote(t3.at[e], t3.at[e], t3s.at[o], t3r.at[e], gz=e).wait_recv()
        t3_pass(o).start()

    @pl.when(has_lo)
    def _():
        g1_hi.wait_recv()
        s2[3, pl.ds(PAD, 64), :] += g1[0]

    @pl.when(has_hi)
    def _():
        g1_lo.wait_recv()
        s2[3, pl.ds(PAD, 64), :] += g1[1]

    def h2_copy(i):
        step = (-2, -1, 1, 2)[i]
        to = jnp.clip(d + step, 0, gz - 1)
        return remote(
            s2.at[3, pl.ds(PAD, 64), :], s2.at[3 - step, pl.ds(PAD, 64), :], h2s.at[i], h2r.at[i], gz=to
        )

    for i, step in enumerate((-2, -1, 1, 2)):
        @pl.when(inside(step))
        def _():
            h2_copy(i).start()

    crossing(3, begin, False)


    @pl.loop(0, gz // 2)
    def _(o):
        e = lax.rem(beside + 2 * o, gz)
        remote(t3.at[e], t3.at[e], t3p.at[o], t3r.at[e], gz=beside).wait_recv()

    if not EARLY:
        crossing(1, begin, True, diagonal)
    for far in (2, 3):
        for side, _, cond, step in relays:
            @pl.when(cond)
            def _():
                to_relay(side, far, step).wait_recv()
                hand_on(side, far).start()

    lane32 = lane_iota((32, 128))
    for q in range(4):
        total = None
        for e in range(max(4 * q - 2, 0), min(4 * q + 6, gz)):
            low, high = max(e - 1 - 4 * q, 0), min(e + 2 - 4 * q, 3)
            parts = []
            if low <= high:
                x = t3[e, pl.ds(0, 32), :]
                if (low, high) != (0, 3):
                    x = jnp.where(jnp.logical_and(lane32 >= 32 * low, lane32 < 32 * high + 32), x, 0.0)
                parts.append(x)
            block = e - 2 - 4 * q
            if 0 <= block < 4:
                x = t3[e, pl.ds(32, 8), :]
                pieces = [jnp.where(block8 == block, roll(x, 32 * (block - k)), 0.0) for k in range(4)]
                parts.append(jnp.concatenate(pieces, axis=0))
            for x in parts:
                total = x if total is None else total + x
        s3[q] = total * NINTH
        a3[q, pl.ds(PAD, 32), :] = total * NINTH

    def sweep3(src, dst):
        v = [crow(src, q, 0, 32) for q in range(4)]
        for q in range(4):
            after = v[q + 1] if q < 3 else jnp.zeros_like(v[0])
            before = v[q - 1] if q > 0 else jnp.zeros_like(v[0])
            nz = roll(jnp.where(lane32 < 32, after, v[q]), -32)
            nz = nz + roll(jnp.where(lane32 >= 96, before, v[q]), 32)
            nb = nbxy(src, q, 0, 32, v[q], 32) + nz
            dst[q, pl.ds(PAD, 32), :] = (1.0 / 3.0) * v[q] + (NINTH * nb + s3[q])

    @pl.loop(0, 3)
    def _(i):
        sweep3(a3, b3)
        sweep3(b3, a3)

    sweep3(a3, b3)

    def f_wait(*which):
        @pl.when(has_lo)
        def _():
            for far in which:
                f_copy(1, far, False).wait_recv()

        @pl.when(has_hi)
        def _():
            for far in which:
                f_copy(0, far, False).wait_recv()

    f_wait(0, 1)
    w_plane(4, True, True)
    w_plane(11, True, True)

    @pl.when(has_lo)
    def _():
        w_plane(3, True, True)

    @pl.when(has_hi)
    def _():
        w_plane(12, True, True)

    def products(z, carry):
        plain, edges = carry
        for r in range(0, 128, CH):
            c, src, up = center(a, z, r, CH), center(f, z, r, CH), center(a, z + 1, r, CH)
            for ph in range(4):
                plain = plain + fold(c[ph] * (src[ph] - (3.0 * N81) * c[ph]))
            e = c[0] * c[1] + c[2] * c[3] + (c[0] * c[2] + c[1] * c[3])
            e = e + (c[1] * from_right(c[0]) + c[3] * from_right(c[2]))
            e = e + (c[2] * rows(a, z, 0, r, CH, 1) + c[3] * rows(a, z, 1, r, CH, 1))
            for ph in range(4):
                e = e + c[ph] * up[ph]
            edges = edges + fold(e)
        return plain, edges

    zero = jnp.zeros((8, 128), F32)
    plain, edges = lax.fori_loop(4, 12, products, (zero, zero))
    kept[0] = plain
    kept[1] = edges

    for i, step in enumerate((-2, -1, 1, 2)):
        @pl.when(inside(-step))
        def _():
            h2_copy(i).wait_recv()

    for p in range(1, 6):
        at = d + p - 3
        q = jnp.clip(at // 4, 0, 3)
        e = split_dot(b3[q, pl.ds(PAD, 32), :], mats[8 + p])
        pe2[p - 1, pl.ds(0, 32, stride=2), :] = e
        pe2[p - 1, pl.ds(1, 32, stride=2), :] = e
    for p in range(1, 6):
        c = crow(s2, p, 0, 64)
        w = 12.0 * c + nb2(s2, p, c)
        a2[p, pl.ds(PAD, 64), :] = flag2[p] * (N81 * w + pe2[p - 1])

    def sweep2(src, dst, p):
        c = crow(src, p, 0, 64)
        dst[p, pl.ds(PAD, 64), :] = flag2[p] * (
            (1.0 / 3.0) * c + NINTH * (nb2(src, p, c) + crow(s2, p, 0, 64))
        )

    for p in range(2, 5):
        sweep2(a2, b2, p)
    for p in range(2, 5):
        sweep2(b2, a2, p)

    for i in range(2):
        @pl.when(h1_recvs[i])
        def _():
            h1_copy(i).wait_recv()

    for j in range(1, 5):
        e = split_dot(a2[2 + j // 2, pl.ds(PAD, 64), :], mats[2 + j % 2])
        pe1[j, pl.ds(0, 64, stride=2), :] = e
        pe1[j, pl.ds(1, 64, stride=2), :] = e

    def in_grid(z):
        return jnp.where(z < 5, flo, jnp.where(z > 8, fhi, 1.0))

    def nb1(ref, z, r, c):
        return nbxy(ref, z, r, 64, c, 128) + (crow(ref, z - 1, r, 64) + crow(ref, z + 1, r, 64))

    @pl.loop(3, 11, unroll=8)
    def _(z):
        flag = in_grid(z)
        for r in range(0, 128, 64):
            c = crow(s1, z, r, 64)
            w = 12.0 * c + nb1(s1, z, r, c)
            a1[z, pl.ds(PAD + r, 64), :] = flag * (N81 * w + pe1[(z - 1) // 2, pl.ds(r, 64), :])

    @pl.loop(4, 10, unroll=6)
    def _(z):
        flag = in_grid(z)
        for r in range(0, 128, 64):
            c = crow(a1, z, r, 64)
            t = nb1(a1, z, r, c) + crow(s1, z, r, 64)
            b1[z, pl.ds(PAD + r, 64), :] = flag * ((1.0 / 3.0) * c + NINTH * t)

    @pl.loop(5, 9, unroll=4)
    def _(z):
        for r in range(0, 128, 64):
            c = crow(b1, z, r, 64)
            t = nb1(b1, z, r, c) + crow(s1, z, r, 64)
            e1[z - 5, pl.ds(r, 64), :] = (1.0 / 3.0) * c + NINTH * t

    e1_lo = remote(
        e1.at[pl.ds(0, 2)], e1h.at[1], e1s.at[0], e1r.at[1], gz=jnp.maximum(d - 1, 0)
    )
    e1_hi = remote(
        e1.at[pl.ds(2, 2)], e1h.at[0], e1s.at[1], e1r.at[0], gz=jnp.minimum(d + 1, gz - 1)
    )

    @pl.when(has_lo)
    def _():
        e1_lo.start()

    @pl.when(has_hi)
    def _():
        e1_hi.start()

    def correct(z, ref, k):
        e = ref[k]
        for ph in range(4):
            a[z, ph, pl.ds(PAD, 128), :] = N81 * a[z, ph, pl.ds(PAD, 128), :] + e

    def sweep0(src, dst, first, last):
        @pl.loop(first + 4, last + 5)
        def _(z):
            for r in range(0, 128, CH):
                c = center(src, z, r, CH)
                nb = nbxy0(src, z, r, CH, c)
                for ph in range(4):
                    t = nb[ph] + (rows(src, z - 1, ph, r, CH) + rows(src, z + 1, ph, r, CH))
                    t = t + rows(f, z, ph, r, CH)
                    dst[z, ph, pl.ds(PAD + r, CH), :] = (1.0 / 3.0) * c[ph] + NINTH * t

    def below(first):
        return jnp.where(has_lo, first, 0)

    def above(last):
        return jnp.where(has_hi, last, 7)

    plain, edges = kept[0], kept[1]
    coarse = zero
    for j in range(4):
        coarse = coarse + fold(s1[5 + j, pl.ds(PAD, 128), :] * e1[j])
    part = (2.0 * N81) * (plain + N81 * edges) + 2.0 * coarse
    prods[d] = part.sum(axis=0, keepdims=True)

    @pl.loop(1, gz)
    def _(o):
        remote(prods.at[d], prods.at[d], ps.at[o], pr.at[d], gz=lax.rem(d + o, gz)).start()


    @pl.loop(0, 8)
    def _(z):
        correct(z + 4, e1, z // 2)

    sweep0(a, b, 1, 6)
    sweep0(b, a, 2, 5)

    def final(z, squares):
        for r in range(0, 128, CH):
            c = center(a, z, r, CH)
            nb = nbxy0(a, z, r, CH, c)
            for ph in range(4):
                t = nb[ph] + (rows(a, z - 1, ph, r, CH) + rows(a, z + 1, ph, r, CH))
                left = (rows(f, z, ph, r, CH) - 6.0 * c[ph]) + t
                squares = squares + fold(left * left)
        return squares

    kept[0] = lax.fori_loop(7, 9, final, zero)

    f_wait(2, 3)

    @pl.loop(jnp.where(has_lo, 1, 3), 3)
    def _(z):
        w_plane(z, True, True)

    @pl.loop(13, jnp.where(has_hi, 15, 13))
    def _(z):
        w_plane(z, True, True)

    @pl.when(has_lo)
    def _():
        e1_hi.wait_recv()
        for z in range(-3, 0):
            correct(z + 4, e1h.at[0], (z + 4) // 2)

    @pl.when(has_hi)
    def _():
        e1_lo.wait_recv()
        for z in range(8, 11):
            correct(z + 4, e1h.at[1], (z - 8) // 2)

    sweep0(a, b, below(-2), 0)
    sweep0(a, b, 7, above(9))
    sweep0(b, a, below(-1), 1)
    sweep0(b, a, 6, above(8))

    squares = lax.fori_loop(4, 7, final, kept[0])
    sums[d] = lax.fori_loop(9, 12, final, squares).sum(axis=0, keepdims=True)

    @pl.loop(1, gz)
    def _(o):
        remote(sums.at[d], sums.at[d], ss.at[o], sr.at[d], gz=lax.rem(d + o, gz)).start()

    @pl.loop(1, gz)
    def _(o):
        peer = lax.rem(d + o, gz)
        remote(prods.at[peer], prods.at[peer], ps.at[o], pr.at[peer], gz=peer).wait_recv()

    total = prods[0]
    for e in range(1, gz):
        total = total + prods[e]
    ens[me] = pweight[0, 0] * total

    @pl.loop(1, pairs)
    def _(o):
        remote(ens.at[me], ens.at[me], es.at[o], er.at[me], pair=lax.rem(me + o, pairs)).start()

    px[...] = selection((256, 256), lambda i, j: i == (j & 1) * 128 + (j >> 1))

    @pl.loop(0, 8)
    def _(z):
        for yp in range(2):
            x = jnp.concatenate(
                [a[z + 4, 2 * yp, pl.ds(PAD, 128), :], a[z + 4, 2 * yp + 1, pl.ds(PAD, 128), :]], axis=1
            )
            y = split_dot(x, px[...])
            for half in range(2):
                tmp[z % 2, half, pl.ds(yp, 128, stride=2), :] = y[:, 128 * half:128 * half + 128]
        for half in range(2):
            pot[0, z, :, pl.ds(128 * half, 128)] = tmp[z % 2, half]

    for cond, side in ((has_lo, 0), (has_hi, 1)):
        @pl.when(cond)
        def _():
            (g0_lo, g0_hi)[side].wait_send()
            (g1_lo, g1_hi)[side].wait_send()
            (e1_lo, e1_hi)[side].wait_send()

    index_copy.wait_send()
    on_chip(sent)
    for far in range(4):
        crossing(far, sent, True)
    crossing(0, sent, False)
    crossing(3, sent, False)
    for far in (2, 3):
        for side, first, second, step in relays:
            @pl.when(first)
            def _():
                to_relay(side, far, step).wait_send()

            @pl.when(second)
            def _():
                hand_on(side, far).wait_send()

    for i in range(2):
        @pl.when(h1_sends[i])
        def _():
            h1_copy(i).wait_send()

    for i, step in enumerate((-2, -1, 1, 2)):
        @pl.when(inside(step))
        def _():
            h2_copy(i).wait_send()

    @pl.loop(1, gz // 2)
    def _(o):
        t3_copy(o).wait_send()

    @pl.loop(0, gz // 2)
    def _(o):
        t3_pass(o).wait_send()

    @pl.loop(1, gz)
    def _(o):
        peer = lax.rem(d + o, gz)
        remote(sums.at[peer], sums.at[peer], ss.at[o], sr.at[peer], gz=peer).wait_recv()

    total = sums[0]
    for e in range(1, gz):
        total = total + sums[e]
    cells = 1.0 / (gz * 8 * 256 * 256)
    stats[0:1, :] = jnp.zeros((1, 128), F32) + jnp.sqrt(jnp.sum(total, axis=1, keepdims=True) * cells)

    @pl.loop(1, pairs)
    def _(o):
        peer = lax.rem(me + o, pairs)
        remote(ens.at[peer], ens.at[peer], es.at[o], er.at[peer], pair=peer).wait_recv()

    energy = ens[0]
    for e in range(1, pairs):
        energy = energy + ens[e]
    stats[1:2, :] = jnp.zeros((1, 128), F32) + jnp.sum(energy, axis=1, keepdims=True) * (-0.5 * cells)

    @pl.loop(1, gz)
    def _(o):
        remote(sums.at[d], sums.at[d], ss.at[o], sr.at[d], gz=lax.rem(d + o, gz)).wait_send()
        remote(prods.at[d], prods.at[d], ps.at[o], pr.at[d], gz=lax.rem(d + o, gz)).wait_send()

    @pl.loop(1, pairs)
    def _(o):
        remote(ens.at[me], ens.at[me], es.at[o], er.at[me], pair=lax.rem(me + o, pairs)).wait_send()


def solution(mesh):
    gz, pairs = mesh.shape["gz"], mesh.shape["pair"]
    dma, vmem = pltpu.SemaphoreType.DMA, pltpu.VMEM
    field = vmem((16, 4, 144, 128), F32)
    level1, level2, level3 = vmem((14, 144, 128), F32), vmem((7, 80, 128), F32), vmem((4, 48, 128), F32)

    def per_device(orbitals, pair_index, pair_weight):
        potential, stats = pl.pallas_call(
            functools.partial(kernel, gz, pairs),
            out_shape=(
                jax.ShapeDtypeStruct((1, 8, 256, 256), F32),
                jax.ShapeDtypeStruct((2, 128), F32),
            ),
            in_specs=[
                pl.BlockSpec(memory_space=pltpu.HBM),
                pl.BlockSpec(memory_space=pltpu.HBM),
                pl.BlockSpec(memory_space=pl.ANY),
            ],
            out_specs=(
                pl.BlockSpec(memory_space=pltpu.VMEM),
                pl.BlockSpec(memory_space=pltpu.VMEM),
            ),
            scratch_shapes=[
                *[vmem((8, 256, 256), BF16)] * 8,
                vmem((256, 256), BF16),
                vmem((15, 128, 128), BF16),
                vmem((2, 2, 256, 128), F32),
                pltpu.SMEM((1, 2), jnp.int32),
                pltpu.SMEM((1, 1), F32),
                pltpu.SMEM((1, 2), jnp.int32),
                vmem((4, 4, 128, 128), F32),
                vmem((2, 4, 128, 128), F32),
                field, field, field,
                vmem((2, 128, 128), F32), vmem((2, 128, 128), F32),
                level1, level1, level1,
                vmem((6, 128, 128), F32),
                vmem((2, 64, 128), F32), vmem((2, 64, 128), F32),
                vmem((6, 128, 128), F32),
                vmem((4, 128, 128), F32), vmem((2, 2, 128, 128), F32),
                level2, level2, level2,
                vmem((5, 64, 128), F32),
                vmem((5, 64, 128), F32),
                vmem((gz, 40, 128), F32),
                vmem((4, 32, 128), F32),
                level3, level3,
                vmem((2, 8, 128), F32),
                vmem((gz, 1, 128), F32), vmem((gz, 1, 128), F32),
                vmem((pairs, 1, 128), F32),
                dma((2,)),
                dma((8,)),
                dma((1,)), dma((1,)),
                dma((2,)), dma((2,)), dma((2,)),
                dma((2, 4)), dma((2, 4)),
                dma((2,)), dma((2,)),
                dma((2,)), dma((2,)),
                dma((2,)), dma((2,)),
                dma((2,)), dma((2,)),
                dma((4,)), dma((4,)),
                dma((gz,)), dma((gz,)), dma((gz,)),
                dma((gz,)), dma((gz,)),
                dma((gz,)), dma((gz,)),
                dma((pairs,)), dma((pairs,)),
            ],
            compiler_params=pltpu.CompilerParams(
                collective_id=0, has_side_effects=True, vmem_limit_bytes=48 * 1024 * 1024
            ),
            name="vcycle",
        )(pltpu.with_memory_space_constraint(pair_index, pltpu.HBM), pair_weight.reshape(1, 1), orbitals)
        return potential, stats[0, :1], stats[1, :1]

    return jax.shard_map(
        per_device,
        mesh=mesh,
        in_specs=(P(None, "gz", None, None), P("pair", None), P("pair")),
        out_specs=(P("pair", "gz", None, None), P("pair"), P()),
        check_vma=False,
    )
```
